32 devices in a mesh: dom: 8 (over y, x, core), col: 4 (over z).
Axes of the slice: x: 2, y: 2, z: 4, core: 2. Of those that a mesh axis runs over, the one named last changes fastest.
Arguments:
- features: bfloat16 [65536, 1024], P('dom', 'col')
- weight: bfloat16 [1024, 1024], P(None, 'col'), may hold values from -0.1875 to 0.1875
- out_bias: bfloat16 [1024], P('col'), may hold values from -3 to 3
- local_index: int32 [8, 64, 4], P('dom'), may hold values from 0 to 63
- local_count: int32 [8, 64], P('dom'), may hold values from 1 to 4, as said below
- local_vals: bfloat16 [8, 64, 4, 128, 128], P('dom'), may hold values from -0.1875 to 0.1875
- halo_index: int32 [8, 64, 4], P('dom'), may hold values from 0 to 31
- halo_count: int32 [8, 64], P('dom'), may hold values from 0 to 4, as said below
- halo_vals: bfloat16 [8, 64, 4, 128, 128], P('dom'), may hold values from -0.1875 to 0.1875
- send_rows: int32 [8, 8, 512], P('dom'), may hold values from 0 to 8191
- send_count: int32 [8, 8], P('dom'), may hold values from 0 to 512, as said below
Outputs:
- normalized: bfloat16 [65536, 1024], P('dom', 'col')
- channel_stats: float32 [2, 1024], P(None, 'col')
The draws below stay inside these ranges and needn't reach their ends.
Inputs may be any that keep to these rules, and one draw needn't show every extreme that they name: `local_index`: slots k >= local_count of a row tile are not used. `local_count`: every partition has a row tile with all 4 slots used. `halo_index`: slots k >= halo_count of a row tile are not used. `halo_count`: every partition has a row tile with all 4 slots used. `send_rows`: slots s >= send_count[q, p] are not used. send_count[p, p] is 0; every partition fills all 512 slots to some other partition.
All inputs are finite; a program needn't handle non-finite values.
Results may differ from the reference program's by a relative error of at most 0.0075.
Values may be sent and summed in bfloat16 or wider, within the bound.
No kernel may reach another device: no remote copies, remote signals or barrier semaphores. Data moves between devices by JAX's collectives and lax.ppermute only.
A program may use at most 192 MiB of HBM per device.

```python
import jax
import jax.numpy as jnp
from jax import lax

F = 1024
ROWS_DEV = 8192
TILE = 128
LOCAL_SLOTS = 4
HALO_SLOTS = 4
HALO_PEER = 512
NODES = 65536
LOCAL_TILES = 64
HALO_TILES = 32
N_DOM = 8


def draw_features(key, part):
    key_base = jax.random.fold_in(key, 0)
    rising = 1.0 + 2.0 * jnp.arange(NODES, dtype=jnp.float32) / NODES
    values = jax.random.normal(key_base, (NODES, F), jnp.float32) * rising[:, None]
    return values.astype(jnp.bfloat16)


def slot_counts(key, highest, lowest):
    key_base, key_heavy, key_place = jax.random.split(key, 3)
    counts = jax.random.randint(key_base, (N_DOM, LOCAL_TILES), lowest, highest + 1)
    heavier = jax.random.randint(key_heavy, (N_DOM, 1), 0, highest)
    counts = jnp.minimum(counts + heavier, highest)
    placed = jax.random.randint(key_place, (N_DOM, 1), 0, LOCAL_TILES)
    tile_ids = jnp.arange(LOCAL_TILES)[None, :]
    return jnp.where(tile_ids == placed, highest, counts).astype(jnp.int32)


def draw_local_count(key, part):
    return slot_counts(jax.random.fold_in(key, 11), LOCAL_SLOTS, 1)


def draw_halo_count(key, part):
    return slot_counts(jax.random.fold_in(key, 23), HALO_SLOTS, 0)


def draw_send_count(key, part):
    key_base, key_target = jax.random.split(jax.random.fold_in(key, 37))
    counts = jax.random.randint(key_base, (N_DOM, N_DOM), HALO_PEER // 4, HALO_PEER + 1)
    offset = jax.random.randint(key_target, (N_DOM, 1), 1, N_DOM)
    sources = jnp.arange(N_DOM)[:, None]
    targets = jnp.arange(N_DOM)[None, :]
    counts = jnp.where(targets == (sources + offset) % N_DOM, HALO_PEER, counts)
    return jnp.where(targets == sources, 0, counts).astype(jnp.int32)


def touch_ends(entries, key, low, high):
    longest = entries.shape.index(max(entries.shape))
    spots = []
    for shift in (0, 1):
        where = [jax.random.randint(jax.random.fold_in(key, axis), (), 0, length) for axis, length in enumerate(entries.shape)]
        where[longest] = (where[longest] + shift) % entries.shape[longest]
        spots.append(tuple(where))
    return entries.at[spots[0]].set(low).at[spots[1]].set(high)


def block_levels(stream_key, shape, cuts, least, high):
    level = 1.0
    for dim, shards_of in cuts:
        draws = jax.random.uniform(jax.random.fold_in(jax.random.fold_in(stream_key, 6), dim), (shards_of,), jnp.float32, least / len(cuts), high / len(cuts))
        level = level * jnp.repeat(jnp.exp(draws), shape[dim] // shards_of).reshape((-1,) + (1,) * (len(shape) - 1 - dim))
    return level


def bell_draw(stream_key, dims, deviation, reach, cuts=(), kind=jnp.bfloat16):
    entries = deviation * jax.random.normal(stream_key, dims, jnp.float32)
    if cuts:
        entries = entries * block_levels(stream_key, dims, cuts, -0.22, 0.18)
    return jnp.clip(entries, -reach, reach).astype(kind)


def setup_inputs(seed: int = 0) -> dict:
    arg_keys = jax.random.split(jax.random.key(seed), 12)
    features = draw_features(jax.random.fold_in(arg_keys[11], 71), 0)
    weight = bell_draw(arg_keys[1], (F, F), F ** -0.5, 0.1875, ((1, 4),))
    out_bias = bell_draw(arg_keys[2], (F,), 0.5, 3.0, ((0, 4),))
    local_index = touch_ends(jax.random.randint(arg_keys[3], (N_DOM, LOCAL_TILES, LOCAL_SLOTS), 0, LOCAL_TILES), jax.random.fold_in(arg_keys[3], 1), 0, LOCAL_TILES - 1).astype(jnp.int32)
    local_count = draw_local_count(jax.random.fold_in(arg_keys[11], 71), 0)
    local_vals = bell_draw(arg_keys[5], (N_DOM, LOCAL_TILES, LOCAL_SLOTS, TILE, TILE), (TILE * (LOCAL_SLOTS + HALO_SLOTS)) ** -0.5, 0.1875, ((0, 8),))
    halo_index = touch_ends(jax.random.randint(arg_keys[6], (N_DOM, LOCAL_TILES, HALO_SLOTS), 0, HALO_TILES), jax.random.fold_in(arg_keys[6], 1), 0, HALO_TILES - 1).astype(jnp.int32)
    halo_count = draw_halo_count(jax.random.fold_in(arg_keys[11], 71), 0)
    halo_vals = bell_draw(arg_keys[8], (N_DOM, LOCAL_TILES, HALO_SLOTS, TILE, TILE), (TILE * (LOCAL_SLOTS + HALO_SLOTS)) ** -0.5, 0.1875, ((0, 8),))
    send_rows = touch_ends(jax.random.randint(arg_keys[9], (N_DOM, N_DOM, HALO_PEER), 0, ROWS_DEV), jax.random.fold_in(arg_keys[9], 1), 0, ROWS_DEV - 1).astype(jnp.int32)
    send_count = draw_send_count(jax.random.fold_in(arg_keys[11], 71), 0)
    return {"features": features, "weight": weight, "out_bias": out_bias, "local_index": local_index, "local_count": local_count, "local_vals": local_vals, "halo_index": halo_index, "halo_count": halo_count, "halo_vals": halo_vals, "send_rows": send_rows, "send_count": send_count}


epsilon = 1e-06

def tile_product(sources, tile_index, tile_count, tile_vals, slot_total):
    gathered = sources[tile_index]
    keep_mask = jnp.arange(slot_total)[None, :] < tile_count[:, None]
    masked = jnp.where(keep_mask[:, :, None, None], tile_vals, jnp.zeros_like(tile_vals))
    return jnp.einsum('tkij,tkjc->tic', masked.astype(jnp.float32), gathered.astype(jnp.float32))

def reference(features, weight, out_bias, local_index, local_count, local_vals, halo_index, halo_count, halo_vals, send_rows, send_count):
    blocks = features.reshape(N_DOM, ROWS_DEV, F)
    slot_ids = jnp.arange(HALO_PEER)
    sources_ids = jnp.arange(N_DOM)

    def aggregate(partition):
        chosen = blocks[sources_ids[:, None], send_rows[:, partition, :]]
        keep_mask = slot_ids[None, :] < send_count[:, partition][:, None]
        halo_tiles = jnp.where(keep_mask[:, :, None], chosen, jnp.zeros_like(chosen)).reshape(HALO_TILES, TILE, F)
        own_tiles = blocks[partition].reshape(LOCAL_TILES, TILE, F)
        summed = tile_product(own_tiles, local_index[partition], local_count[partition], local_vals[partition], LOCAL_SLOTS)
        summed = summed + tile_product(halo_tiles, halo_index[partition], halo_count[partition], halo_vals[partition], HALO_SLOTS)
        return summed.reshape(ROWS_DEV, F).astype(jnp.bfloat16)
    spread = lax.map(aggregate, jnp.arange(N_DOM)).reshape(NODES, F)
    mixed_rows = jnp.dot(spread, weight, preferred_element_type=jnp.float32) + out_bias.astype(jnp.float32)
    active = jnp.maximum(mixed_rows, 0.0)
    row_power = lax.optimization_barrier(jnp.mean(active * active, axis=1, keepdims=True))
    scaled = active * lax.rsqrt(row_power + epsilon)
    channel_mean = lax.optimization_barrier(jnp.sum(scaled, axis=0)) / NODES
    channel_var = lax.optimization_barrier(jnp.sum(scaled * scaled, axis=0)) / NODES - channel_mean * channel_mean
    return (scaled.astype(jnp.bfloat16), jnp.stack([channel_mean, channel_var]))
```

```python
import functools

import jax
import jax.numpy as jnp
from jax import lax
from jax.experimental import pallas as pl
from jax.experimental.pallas import tpu as pltpu
from jax.sharding import PartitionSpec as P

TILE = 128
EPS = 1e-06

HBM = pl.BlockSpec(memory_space=pl.ANY)


def cost(flops, nbytes):
    return pl.CostEstimate(flops=int(flops), bytes_accessed=int(nbytes), transcendentals=0)


def gather_kernel(n_dom, peer, slots, ids, rows, counts, feat, *refs):
    outs = refs[: n_dom - 1]
    table, raw, stage, sems = refs[n_dom - 1 :]
    n_rows = table.shape[0]
    parts = 8 if n_rows % (8 * 64) == 0 else 1
    part = n_rows // parts
    copies = [
        pltpu.make_async_copy(
            feat.at[pl.ds(c * part, part)], raw.at[pl.ds(c * part, part)], sems.at[c]
        )
        for c in range(parts)
    ]
    for copy in copies:
        copy.start()
    for c in range(parts):
        copies[c].wait()

        def widen(b, carry, c=c):
            at = pl.ds(pl.multiple_of(c * part + b * 64, 64), 64)
            table[at, :] = raw[at, :].astype(jnp.float32)
            return carry

        lax.fori_loop(0, part // 64, widen, 0)
    me = ids[1]
    for k in range(1, n_dom):
        q = peer(me, k)
        used = counts[q]

        def pick(b, carry, q=q):
            base = b * 16
            for j in range(16):
                r = rows[q * slots + base + j]
                stage[pl.ds(base + j, 1), :] = table[pl.ds(r, 1), :]
            return carry

        lax.fori_loop(0, (used + 15) // 16, pick, 0)
        for b in range(slots // 64):
            at = pl.ds(b * 64, 64)
            slot = b * 64 + lax.broadcasted_iota(jnp.int32, (64, stage.shape[1]), 0)
            kept = jnp.where(slot < used, stage[at, :], 0.0)
            outs[k - 1][at, :] = kept.astype(jnp.bfloat16)


def gather_rows(ids, send_rows, send_count, features, n_dom, peer):
    slots = send_rows.shape[1]
    n_rows, width = features.shape
    piece = jax.ShapeDtypeStruct((slots, width), features.dtype)
    return pl.pallas_call(
        functools.partial(gather_kernel, n_dom, peer, slots),
        out_shape=[piece] * (n_dom - 1),
        grid_spec=pltpu.PrefetchScalarGridSpec(
            num_scalar_prefetch=3,
            grid=(1,),
            in_specs=[HBM],
            out_specs=[
                pl.BlockSpec((slots, width), lambda i, *_: (0, 0), pipeline_mode=pl.Buffered(1))
            ]
            * (n_dom - 1),
            scratch_shapes=[
                pltpu.VMEM((n_rows, width), jnp.float32),
                pltpu.VMEM((n_rows, width), features.dtype),
                pltpu.VMEM((slots, width), jnp.float32),
                pltpu.SemaphoreType.DMA((8,)),
            ],
        ),
        cost_estimate=cost(4e9, 6 << 20),
        name="gather_rows",
    )(ids, send_rows.reshape(-1), send_count, features)


def tile_sum(src, index, used, vals, t, row_tile, slots):
    left, right = [], []
    for k in range(slots):
        left.append(jnp.where(k < used, vals[t, k], jnp.zeros_like(vals[t, k])))
        start = pl.multiple_of(index[row_tile * slots + k] * TILE, TILE)
        right.append(src[pl.ds(start, TILE), :])
    return jnp.dot(
        jnp.concatenate(left, axis=1),
        jnp.concatenate(right, axis=0),
        preferred_element_type=jnp.float32,
    )


def local_kernel(group, slots, index, counts, feat, vals, out):
    step = pl.program_id(0)
    for t in range(group):
        row_tile = step * group + t
        out[pl.ds(t * TILE, TILE), :] = tile_sum(
            feat, index, counts[row_tile], vals, t, row_tile, slots
        )


def local_sums(index, counts, features, vals):
    tiles, slots = vals.shape[:2]
    n_rows, width = features.shape
    group = 4 if tiles % 4 == 0 else 1
    return pl.pallas_call(
        functools.partial(local_kernel, group, slots),
        out_shape=jax.ShapeDtypeStruct((n_rows, width), jnp.float32),
        grid_spec=pltpu.PrefetchScalarGridSpec(
            num_scalar_prefetch=2,
            grid=(tiles // group,),
            in_specs=[
                pl.BlockSpec((n_rows, width), lambda i, *_: (0, 0), pipeline_mode=pl.Buffered(1)),
                pl.BlockSpec((group, slots, TILE, TILE), lambda i, *_: (i, 0, 0, 0)),
            ],
            out_specs=pl.BlockSpec((group * TILE, width), lambda i, *_: (i, 0)),
        ),
        cost_estimate=cost(4e9, 20 << 20),
        name="local_sums",
    )(index, counts, features, vals)


def halo_kernel(n_dom, n_col, peer, slots, piece_rows, per_dest, base, ids, index, counts, *refs):
    pieces = refs[: n_dom - 1]
    part, vals = refs[n_dom - 1 : n_dom + 1]
    outs = refs[n_dom + 1 : n_dom + 1 + n_col]
    halo, sems = refs[n_dom + 1 + n_col :]
    shift = pl.program_id(0)
    sub = pl.program_id(1)
    group = vals.shape[0]

    @pl.when((shift == 0) & (sub == 0))
    def _():
        me = ids[1]
        copies = []
        for k in range(1, n_dom):
            at = pl.ds(pl.multiple_of(peer(me, -k) * piece_rows, piece_rows), piece_rows)
            copies.append(pltpu.make_async_copy(pieces[k - 1], halo.at[at], sems.at[k - 1]))
        for copy in copies:
            copy.start()
        own = pl.ds(pl.multiple_of(me * piece_rows, piece_rows), piece_rows)
        halo[own, :] = jnp.zeros((piece_rows, halo.shape[1]), halo.dtype)
        for copy in copies:
            copy.wait()

    dest = lax.rem(ids[0] + shift, n_col)
    for t in range(group):
        row_tile = dest * per_dest + base + sub * group + t
        total = part[pl.ds(t * TILE, TILE), :] + tile_sum(
            halo, index, counts[row_tile], vals, t, row_tile, slots
        )
        total = total.astype(jnp.bfloat16)
        for k in range(n_col):

            @pl.when(shift == k)
            def _(k=k, t=t, total=total):
                at = pl.ds(pl.multiple_of((sub * group + t) * TILE, TILE), TILE)
                outs[k][at, :] = total


def halo_sums(ids, index, counts, pieces, part, vals, n_dom, n_col, peer, base, size):
    tiles, slots = vals.shape[:2]
    width = part.shape[1]
    piece_rows = pieces[0].shape[0]
    per_dest = tiles // n_col
    group = size
    while base % group or group > 4:
        group //= 2
    block = lambda k, i, ids, *_: (lax.rem(ids[0] + k, n_col) * per_dest + base) // group + i
    rows = size * TILE
    return pl.pallas_call(
        functools.partial(halo_kernel, n_dom, n_col, peer, slots, piece_rows, per_dest, base),
        out_shape=[jax.ShapeDtypeStruct((rows, width), jnp.bfloat16)] * n_col,
        grid_spec=pltpu.PrefetchScalarGridSpec(
            num_scalar_prefetch=3,
            grid=(n_col, size // group),
            in_specs=[HBM] * (n_dom - 1)
            + [
                pl.BlockSpec((group * TILE, width), lambda *a: (block(*a), 0)),
                pl.BlockSpec((group, slots, TILE, TILE), lambda *a: (block(*a), 0, 0, 0)),
            ],
            out_specs=[
                pl.BlockSpec((rows, width), lambda *_: (0, 0), pipeline_mode=pl.Buffered(1))
            ]
            * n_col,
            scratch_shapes=[
                pltpu.VMEM((n_dom * piece_rows, width), jnp.bfloat16),
                pltpu.SemaphoreType.DMA((n_dom - 1,)),
            ],
        ),
        cost_estimate=cost(2e9, 6 << 20),
        name="halo_sums",
    )(ids, index, counts, *pieces, part, vals)


def mix_kernel(n_col, channels, ids, *refs):
    pieces = refs[:n_col]
    weights = refs[n_col : 2 * n_col]
    bias, before = refs[2 * n_col : 2 * n_col + 2]
    outs = refs[2 * n_col + 2 : 3 * n_col + 2]
    stats = refs[3 * n_col + 2]
    held, sems = refs[3 * n_col + 3 :]
    width = pieces[0].shape[1]

    @pl.when(pl.program_id(0) == 0)
    def _():
        copies = []
        for k in range(n_col):
            for s in range(n_col):
                j = lax.rem(ids[0] + n_col - s, n_col)
                src = weights[k].at[pl.ds(pl.multiple_of(j * width, width), width)]
                dst = held.at[k, pl.ds(s * width, width)]
                copies.append(pltpu.make_async_copy(src, dst, sems.at[k * n_col + s]))
        for copy in copies:
            copy.start()
        stats[...] = before[...]
        for copy in copies:
            copy.wait()

    spread = jnp.concatenate([piece[...] for piece in pieces], axis=1)
    active, power = [], 0.0
    for k in range(n_col):
        mixed = jnp.dot(spread, held[k], preferred_element_type=jnp.float32)
        mixed = jnp.maximum(mixed + bias[pl.ds(k, 1), :], 0.0)
        power = power + jnp.sum(mixed * mixed, axis=1, keepdims=True)
        active.append(mixed)
    scale = lax.rsqrt(power * (1.0 / channels) + EPS)
    for k in range(n_col):
        scaled = active[k] * scale
        outs[k][...] = scaled.astype(outs[k].dtype)
        stats[pl.ds(2 * k, 1), :] += jnp.sum(scaled, axis=0, keepdims=True)
        stats[pl.ds(2 * k + 1, 1), :] += jnp.sum(scaled * scaled, axis=0, keepdims=True)


def mix_rows(ids, pieces, weights, bias, before):
    n_col = len(pieces)
    rows, width = pieces[0].shape
    channels = n_col * width
    block = 128
    piece = pl.BlockSpec((block, width), lambda i, *_: (i, 0))
    whole = lambda a: pl.BlockSpec(a.shape, lambda i, *_: (0, 0))
    out = pl.pallas_call(
        functools.partial(mix_kernel, n_col, channels),
        out_shape=[jax.ShapeDtypeStruct((rows, width), jnp.bfloat16)] * n_col
        + [jax.ShapeDtypeStruct(before.shape, jnp.float32)],
        grid_spec=pltpu.PrefetchScalarGridSpec(
            num_scalar_prefetch=1,
            grid=(rows // block,),
            in_specs=[piece] * n_col + [HBM] * n_col + [whole(bias), whole(before)],
            out_specs=[piece] * n_col + [whole(before)],
            scratch_shapes=[
                pltpu.VMEM((n_col, channels, width), jnp.bfloat16),
                pltpu.SemaphoreType.DMA((n_col * n_col,)),
            ],
        ),
        cost_estimate=cost(2 * rows * channels * channels, 4 << 20),
        name="mix_rows",
    )(ids, *pieces, *weights, bias, before)
    return out[:n_col], out[n_col]


def place_kernel(n_col, per_dest, base, ids, *refs):
    pieces = refs[:n_col]
    out, held, get, put = refs[-4:]
    rows = pieces[0].shape[0]
    loads, stores = [], []
    for k in range(n_col):
        dest = lax.rem(ids[0] + k, n_col)
        at = pl.ds(pl.multiple_of((dest * per_dest + base) * TILE, TILE), rows)
        loads.append(pltpu.make_async_copy(pieces[k], held.at[k], get.at[k]))
        stores.append(pltpu.make_async_copy(held.at[k], out.at[at], put.at[k]))
    for load in loads:
        load.start()
    for k in range(n_col):
        loads[k].wait()
        stores[k].start()
    for store in stores:
        store.wait()


def place_rows(ids, pieces, out, n_rows, base):
    n_col = len(pieces)
    rows, width = pieces[0].shape
    per_dest = n_rows // TILE // n_col
    extra = [] if out is None else [out]
    return pl.pallas_call(
        functools.partial(place_kernel, n_col, per_dest, base),
        out_shape=jax.ShapeDtypeStruct((n_rows, width), jnp.bfloat16),
        grid_spec=pltpu.PrefetchScalarGridSpec(
            num_scalar_prefetch=1,
            grid=(1,),
            in_specs=[HBM] * (n_col + len(extra)),
            out_specs=HBM,
            scratch_shapes=[
                pltpu.VMEM((n_col, rows, width), jnp.bfloat16),
                pltpu.SemaphoreType.DMA((n_col,)),
                pltpu.SemaphoreType.DMA((n_col,)),
            ],
        ),
        input_output_aliases={1 + n_col: 0} if extra else {},
        cost_estimate=cost(1e8, 2 << 20),
        name="place_rows",
    )(ids, *pieces, *extra)


def chunk_plan(per_dest):
    if per_dest % 8:
        return [(0, per_dest)]
    u = per_dest // 8
    return [(0, u), (u, u), (2 * u, 2 * u), (4 * u, 2 * u), (6 * u, 2 * u)]


def on_device(
    features,
    weight,
    out_bias,
    local_index,
    local_count,
    local_vals,
    halo_index,
    halo_count,
    halo_vals,
    send_rows,
    send_count,
):
    n_rows, width = features.shape
    n_dom, n_col = lax.axis_size("dom"), lax.axis_size("col")
    col, dom = lax.axis_index("col"), lax.axis_index("dom")
    ids = jnp.stack([col, dom]).astype(jnp.int32)
    channels = n_col * width

    if n_dom & (n_dom - 1) == 0:
        peer = lambda d, k: d ^ abs(k)
    else:
        peer = lambda d, k: (d + k + n_dom) % n_dom
    along_dom = lambda x, k: lax.ppermute(x, "dom", [(i, peer(i, k)) for i in range(n_dom)])
    along_col = lambda x, k: lax.ppermute(x, "col", [(i, (i + k) % n_col) for i in range(n_col)])

    bias_rows = jnp.broadcast_to(out_bias[None, :], (16, width))
    share = 2 if n_dom % 2 == 0 else 1
    half = channels // share
    odd = dom % share
    mine = lax.dynamic_slice_in_dim(weight, odd * half, half, 0)
    mine = jnp.concatenate([mine, bias_rows], axis=0)
    order = sorted(range(1, n_col), key=lambda k: min(k, n_col - k), reverse=True)
    arrived = {k: along_col(mine, k) for k in order}

    outgoing = gather_rows(ids, send_rows[0], send_count[0], features, n_dom, peer)
    halo = [None] * (n_dom - 1)
    for k in reversed(range(1, n_dom)):
        halo[k - 1] = along_dom(outgoing[k - 1], k)

    part = local_sums(
        local_index[0].reshape(-1), local_count[0], features, local_vals[0]
    )

    weights, biases = [weight], [out_bias[None, :]]
    for k in range(1, n_col):
        got = arrived[k]
        biases.append(got[half : half + 1])
        if share == 1:
            weights.append(got[:half])
            continue
        other = lax.ppermute(got, "dom", [(i, i ^ 1) for i in range(n_dom)])
        first = jnp.where(odd == 0, got[:half], other[:half])
        second = jnp.where(odd == 0, other[:half], got[:half])
        weights.append(jnp.concatenate([first, second], axis=0))
    bias = jnp.concatenate(biases, axis=0).astype(jnp.float32)

    plan = chunk_plan(n_rows // TILE // n_col)
    incoming = []
    for base, size in plan:
        sums = halo_sums(
            ids, halo_index[0].reshape(-1), halo_count[0], halo, part, halo_vals[0],
            n_dom, n_col, peer, base, size,
        )
        moved = {k: along_col(sums[k], k) for k in order}
        incoming.append([sums[0]] + [moved[k] for k in range(1, n_col)])

    stats = jnp.zeros((2 * n_col, width), jnp.float32)
    returned = []
    for pieces in incoming:
        done, stats = mix_rows(ids, pieces, weights, bias, stats)
        moved = {k: along_col(done[k], -k) for k in order}
        returned.append([done[0]] + [moved[k] for k in range(1, n_col)])

    over_dom = lax.all_gather(stats, "dom", axis=0).sum(axis=0)
    total = over_dom[:2]
    for k in range(1, n_col):
        total = total + along_col(over_dom[2 * k : 2 * k + 2], -k)

    out = None
    for (base, _), pieces in zip(plan, returned):
        out = place_rows(ids, pieces, out, n_rows, base)

    node_total = n_rows * n_dom
    mean = total[0] / node_total
    var = total[1] / node_total - mean * mean
    return (out, jnp.stack([mean, var]))


def solution(mesh):
    in_specs = (
        P("dom", "col"),
        P(None, "col"),
        P("col"),
        P("dom", None, None),
        P("dom", None),
        P("dom", None, None, None, None),
        P("dom", None, None),
        P("dom", None),
        P("dom", None, None, None, None),
        P("dom", None, None),
        P("dom", None),
    )
    out_specs = (P("dom", "col"), P(None, "col"))
    return jax.shard_map(
        on_device, mesh=mesh, in_specs=in_specs, out_specs=out_specs, check_vma=False
    )
```

```python
import functools

import jax
import jax.numpy as jnp
from jax import lax
from jax.experimental import pallas as pl
from jax.experimental.pallas import tpu as pltpu
from jax.sharding import PartitionSpec as P


TILE = 128
EPS = 1e-06

HBM = pl.BlockSpec(memory_space=pl.ANY)
VMEM = pl.BlockSpec(memory_space=pltpu.VMEM)


def cost(flops, nbytes):
    return pl.CostEstimate(flops=int(flops), bytes_accessed=int(nbytes), transcendentals=0)


def grant(mib):
    return pltpu.CompilerParams(vmem_limit_bytes=int(mib) << 20)


def gather_kernel(peers, peer, slots, ids, rows, counts, feat, *refs):
    outs = refs[: len(peers)]
    table, raw, stage, sems = refs[len(peers) :]
    n_rows = table.shape[0]
    parts = 8 if n_rows % (8 * 64) == 0 else 1
    part = n_rows // parts
    copies = [
        pltpu.make_async_copy(
            feat.at[pl.ds(c * part, part)], raw.at[pl.ds(c * part, part)], sems.at[c]
        )
        for c in range(parts)
    ]
    for copy in copies:
        copy.start()
    for c in range(parts):
        copies[c].wait()

        def widen(b, carry, c=c):
            at = pl.ds(pl.multiple_of(c * part + b * 64, 64), 64)
            table[at, :] = raw[at, :].astype(jnp.float32)
            return carry

        lax.fori_loop(0, part // 64, widen, 0)
    me = ids[1]
    for out, k in zip(outs, peers):
        q = peer(me, k)
        used = counts[q]

        def pick(b, carry, q=q):
            base = b * 16
            for j in range(16):
                r = rows[q, base + j]
                stage[pl.ds(base + j, 1), :] = table[pl.ds(r, 1), :]
            return carry

        lax.fori_loop(0, (used + 15) // 16, pick, 0)
        for b in range(slots // 64):
            at = pl.ds(b * 64, 64)
            slot = b * 64 + lax.broadcasted_iota(jnp.int32, (64, stage.shape[1]), 0)
            kept = jnp.where(slot < used, stage[at, :], 0.0)
            out[at, :] = kept.astype(jnp.bfloat16)


def gather_rows(ids, send_rows, send_count, features, peers, peer):
    slots = send_rows.shape[1]
    n_rows, width = features.shape
    piece = jax.ShapeDtypeStruct((slots, width), features.dtype)
    return pl.pallas_call(
        functools.partial(gather_kernel, peers, peer, slots),
        out_shape=[piece] * len(peers),
        grid_spec=pltpu.PrefetchScalarGridSpec(
            num_scalar_prefetch=3,
            grid=(1,),
            in_specs=[HBM],
            out_specs=[
                pl.BlockSpec((slots, width), lambda i, *_: (0, 0), pipeline_mode=pl.Buffered(1))
            ]
            * len(peers),
            scratch_shapes=[
                pltpu.VMEM((n_rows, width), jnp.float32),
                pltpu.VMEM((n_rows, width), features.dtype),
                pltpu.VMEM((slots, width), jnp.float32),
                pltpu.SemaphoreType.DMA((8,)),
            ],
        ),
        compiler_params=grant(18 + len(peers)),
        cost_estimate=cost(4e9, 6 << 20),
        name="gather_rows",
    )(ids, send_rows, send_count, features)


def tile_sum(src, index, used, vals, t, row_tile, slots):
    left, right = [], []
    for k in range(slots):
        left.append(jnp.where(k < used, vals[t, k], jnp.zeros_like(vals[t, k])))
        start = pl.multiple_of(index[row_tile * slots + k] * TILE, TILE)
        right.append(src[pl.ds(start, TILE), :])
    return jnp.dot(
        jnp.concatenate(left, axis=1),
        jnp.concatenate(right, axis=0),
        preferred_element_type=jnp.float32,
    )


def local_kernel(group, slots, index, counts, feat, vals, out):
    step = pl.program_id(0)
    for t in range(group):
        row_tile = step * group + t
        out[pl.ds(t * TILE, TILE), :] = tile_sum(
            feat, index, counts[row_tile], vals, t, row_tile, slots
        )


def local_sums(index, counts, features, vals):
    tiles, slots = vals.shape[:2]
    n_rows, width = features.shape
    group = 4 if tiles % 4 == 0 else 1
    return pl.pallas_call(
        functools.partial(local_kernel, group, slots),
        out_shape=jax.ShapeDtypeStruct((n_rows, width), jnp.float32),
        grid_spec=pltpu.PrefetchScalarGridSpec(
            num_scalar_prefetch=2,
            grid=(tiles // group,),
            in_specs=[
                pl.BlockSpec((n_rows, width), lambda i, *_: (0, 0), pipeline_mode=pl.Buffered(1)),
                pl.BlockSpec((group, slots, TILE, TILE), lambda i, *_: (i, 0, 0, 0)),
            ],
            out_specs=pl.BlockSpec((group * TILE, width), lambda i, *_: (i, 0)),
        ),
        cost_estimate=cost(4e9, 20 << 20),
        compiler_params=grant(14),
        name="local_sums",
    )(index, counts, features, vals)


def halo_kernel(n_dom, n_col, peer, slots, piece_rows, per_dest, base, ids, index, counts, *refs):
    pieces = refs[: n_dom - 1]
    part, vals = refs[n_dom - 1 : n_dom + 1]
    outs = refs[n_dom + 1 : n_dom + 1 + n_col]
    (halo,) = refs[n_dom + 1 + n_col :]
    shift = pl.program_id(0)
    sub = pl.program_id(1)
    group = vals.shape[0]

    @pl.when((shift == 0) & (sub == 0))
    def _():
        me = ids[1]
        for k in range(1, n_dom):
            at = pl.ds(pl.multiple_of(peer(me, -k) * piece_rows, piece_rows), piece_rows)
            halo[at, :] = pieces[k - 1][...]
        own = pl.ds(pl.multiple_of(me * piece_rows, piece_rows), piece_rows)
        halo[own, :] = jnp.zeros((piece_rows, halo.shape[1]), halo.dtype)

    dest = lax.rem(ids[0] + shift, n_col)
    for t in range(group):
        row_tile = dest * per_dest + base + sub * group + t
        total = part[pl.ds(t * TILE, TILE), :] + tile_sum(
            halo, index, counts[row_tile], vals, t, row_tile, slots
        )
        total = total.astype(jnp.bfloat16)
        for k in range(n_col):

            @pl.when(shift == k)
            def _(k=k, t=t, total=total):
                at = pl.ds(pl.multiple_of((sub * group + t) * TILE, TILE), TILE)
                outs[k][at, :] = total


def halo_sums(ids, index, counts, pieces, part, vals, n_dom, n_col, peer, base, size):
    tiles, slots = vals.shape[:2]
    width = part.shape[1]
    piece_rows = pieces[0].shape[0]
    per_dest = tiles // n_col
    group = size
    while base % group or group > 4:
        group //= 2
    block = lambda k, i, ids, *_: (lax.rem(ids[0] + k, n_col) * per_dest + base) // group + i
    rows = size * TILE
    return pl.pallas_call(
        functools.partial(halo_kernel, n_dom, n_col, peer, slots, piece_rows, per_dest, base),
        out_shape=[jax.ShapeDtypeStruct((rows, width), jnp.bfloat16)] * n_col,
        grid_spec=pltpu.PrefetchScalarGridSpec(
            num_scalar_prefetch=3,
            grid=(n_col, size // group),
            in_specs=[VMEM] * (n_dom - 1)
            + [
                pl.BlockSpec((group * TILE, width), lambda *a: (block(*a), 0)),
                pl.BlockSpec((group, slots, TILE, TILE), lambda *a: (block(*a), 0, 0, 0)),
            ],
            out_specs=[
                pl.BlockSpec((rows, width), lambda *_: (0, 0), pipeline_mode=pl.Buffered(1))
            ]
            * n_col,
            scratch_shapes=[
                pltpu.VMEM((n_dom * piece_rows, width), jnp.bfloat16),
            ],
        ),
        cost_estimate=cost(2e9, 6 << 20),
        compiler_params=grant(8 + n_dom),
        name="halo_sums",
    )(ids, index, counts, *pieces, part, vals)


def mix_kernel(n_col, channels, ids, *refs):
    pieces = refs[:n_col]
    weights = refs[n_col : 2 * n_col]
    bias, before = refs[2 * n_col : 2 * n_col + 2]
    outs = refs[2 * n_col + 2 : 3 * n_col + 2]
    stats = refs[3 * n_col + 2]
    held, sems = refs[3 * n_col + 3 :]
    width = pieces[0].shape[1]

    @pl.when(pl.program_id(0) == 0)
    def _():
        copies = []
        for k in range(n_col):
            for s in range(n_col):
                j = lax.rem(ids[0] + n_col - s, n_col)
                src = weights[k].at[pl.ds(pl.multiple_of(j * width, width), width)]
                dst = held.at[k, pl.ds(s * width, width)]
                copies.append(pltpu.make_async_copy(src, dst, sems.at[k * n_col + s]))
        for copy in copies:
            copy.start()
        stats[...] = before[...]
        for copy in copies:
            copy.wait()

    spread = jnp.concatenate([piece[...] for piece in pieces], axis=1)
    active, power = [], 0.0
    for k in range(n_col):
        mixed = jnp.dot(spread, held[k], preferred_element_type=jnp.float32)
        mixed = jnp.maximum(mixed + bias[pl.ds(k, 1), :], 0.0)
        power = power + jnp.sum(mixed * mixed, axis=1, keepdims=True)
        active.append(mixed)
    scale = lax.rsqrt(power * (1.0 / channels) + EPS)
    for k in range(n_col):
        scaled = active[k] * scale
        outs[k][...] = scaled.astype(outs[k].dtype)
        stats[pl.ds(2 * k, 1), :] += jnp.sum(scaled, axis=0, keepdims=True)
        stats[pl.ds(2 * k + 1, 1), :] += jnp.sum(scaled * scaled, axis=0, keepdims=True)


def mix_rows(ids, pieces, weights, bias, before):
    n_col = len(pieces)
    rows, width = pieces[0].shape
    channels = n_col * width
    block = 128
    piece = pl.BlockSpec((block, width), lambda i, *_: (i, 0))
    whole = lambda a: pl.BlockSpec(a.shape, lambda i, *_: (0, 0))
    out = pl.pallas_call(
        functools.partial(mix_kernel, n_col, channels),
        out_shape=[jax.ShapeDtypeStruct((rows, width), jnp.bfloat16)] * n_col
        + [jax.ShapeDtypeStruct(before.shape, jnp.float32)],
        grid_spec=pltpu.PrefetchScalarGridSpec(
            num_scalar_prefetch=1,
            grid=(rows // block,),
            in_specs=[piece] * n_col + [HBM] * n_col + [whole(bias), whole(before)],
            out_specs=[piece] * n_col + [whole(before)],
            scratch_shapes=[
                pltpu.VMEM((n_col, channels, width), jnp.bfloat16),
                pltpu.SemaphoreType.DMA((n_col * n_col,)),
            ],
        ),
        cost_estimate=cost(2 * rows * channels * channels, 4 << 20),
        compiler_params=grant(12),
        name="mix_rows",
    )(ids, *pieces, *weights, bias, before)
    return out[:n_col], out[n_col]


def place_kernel(n_col, per_dest, base, nodes, ids, *refs):
    pieces = refs[:n_col]
    parts = refs[n_col : 2 * n_col] if nodes else ()
    out, put = refs[-2 - bool(nodes)], refs[-1]
    rows = pieces[0].shape[0]
    stores = []
    for k in range(n_col):
        dest = lax.rem(ids[0] + k, n_col)
        at = pl.ds(pl.multiple_of((dest * per_dest + base) * TILE, TILE), rows)
        stores.append(pltpu.make_async_copy(pieces[k], out.at[at], put.at[k]))
    for store in stores:
        store.start()
    if nodes:
        total = parts[0][...]
        for part in parts[1:]:
            total = total + part[...]
        total = total / nodes
        mean = total[0:1]
        refs[-2][pl.ds(0, 1), :] = mean
        refs[-2][pl.ds(1, 1), :] = total[1:2] - mean * mean
    for store in stores:
        store.wait()


def place_rows(ids, pieces, out, n_rows, base, parts=(), nodes=0):
    n_col = len(pieces)
    _, width = pieces[0].shape
    per_dest = n_rows // TILE // n_col
    extra = list(parts) + ([] if out is None else [out])
    out_shape = [jax.ShapeDtypeStruct((n_rows, width), jnp.bfloat16)]
    out_specs = [HBM]
    if nodes:
        out_shape.append(jax.ShapeDtypeStruct((2, width), jnp.float32))
        out_specs.append(VMEM)
    return pl.pallas_call(
        functools.partial(place_kernel, n_col, per_dest, base, nodes),
        out_shape=out_shape,
        grid_spec=pltpu.PrefetchScalarGridSpec(
            num_scalar_prefetch=1,
            grid=(1,),
            in_specs=[VMEM] * (n_col + len(parts)) + ([] if out is None else [HBM]),
            out_specs=out_specs,
            scratch_shapes=[pltpu.SemaphoreType.DMA((n_col,))],
        ),
        input_output_aliases={} if out is None else {n_col + len(extra): 0},
        cost_estimate=cost(1e8, 2 << 20),
        compiler_params=grant(8),
        name="place_rows",
    )(ids, *pieces, *extra)


def chunk_plan(per_dest):
    if per_dest % 8:
        return [(0, per_dest)]
    u = per_dest // 8
    return [(0, u), (u, u), (2 * u, 2 * u), (4 * u, 2 * u), (6 * u, 2 * u)]


def on_device(
    features,
    weight,
    out_bias,
    local_index,
    local_count,
    local_vals,
    halo_index,
    halo_count,
    halo_vals,
    send_rows,
    send_count,
):
    n_rows, width = features.shape
    n_dom, n_col = lax.axis_size("dom"), lax.axis_size("col")
    col, dom = lax.axis_index("col"), lax.axis_index("dom")
    ids = jnp.stack([col, dom]).astype(jnp.int32)
    channels = n_col * width

    if n_dom & (n_dom - 1) == 0:
        peer = lambda d, k: d ^ abs(k)
    else:
        peer = lambda d, k: (d + k + n_dom) % n_dom
    along_dom = lambda x, k: lax.ppermute(x, "dom", [(i, peer(i, k)) for i in range(n_dom)])
    along_col = lambda x, k: lax.ppermute(x, "col", [(i, (i + k) % n_col) for i in range(n_col)])

    far = list(reversed(range(1, n_dom)))
    halo = [None] * (n_dom - 1)
    for part, peers in enumerate((far[: (n_dom - 1) // 2], far[(n_dom - 1) // 2 :])):
        outgoing = gather_rows(ids, send_rows[0], send_count[0], features, peers, peer)
        for k, rows in zip(peers, outgoing):
            halo[k - 1] = along_dom(rows, k)

    bias_rows = jnp.broadcast_to(out_bias[None, :], (16, width))
    share = 2 if n_dom % 2 == 0 else 1
    half = channels // share
    odd = dom % share
    mine = lax.dynamic_slice_in_dim(weight, odd * half, half, 0)
    mine = jnp.concatenate([mine, bias_rows], axis=0)
    order = sorted(range(1, n_col), key=lambda k: min(k, n_col - k), reverse=True)
    arrived = {k: along_col(mine, k) for k in order}

    part = local_sums(
        local_index[0].reshape(-1), local_count[0], features, local_vals[0]
    )

    weights, biases = [weight], [out_bias[None, :]]
    for k in range(1, n_col):
        got = arrived[k]
        biases.append(got[half : half + 1])
        if share == 1:
            weights.append(got[:half])
            continue
        other = lax.ppermute(got, "dom", [(i, i ^ 1) for i in range(n_dom)])
        first = jnp.where(odd == 0, got[:half], other[:half])
        second = jnp.where(odd == 0, other[:half], got[:half])
        weights.append(jnp.concatenate([first, second], axis=0))
    bias = jnp.concatenate(biases, axis=0).astype(jnp.float32)

    plan = chunk_plan(n_rows // TILE // n_col)
    incoming = []
    for base, size in plan:
        sums = halo_sums(
            ids, halo_index[0].reshape(-1), halo_count[0], halo, part, halo_vals[0],
            n_dom, n_col, peer, base, size,
        )
        moved = {k: along_col(sums[k], k) for k in order}
        incoming.append([sums[0]] + [moved[k] for k in range(1, n_col)])

    stats = jnp.zeros((2 * n_col, width), jnp.float32)
    returned = []
    for pieces in incoming:
        done, stats = mix_rows(ids, pieces, weights, bias, stats)
        moved = {k: along_col(done[k], -k) for k in order}
        returned.append([done[0]] + [moved[k] for k in range(1, n_col)])

    over_dom = lax.all_gather(stats, "dom", axis=0)
    over_dom = over_dom.sum(axis=0)
    totals = [over_dom[:2]]
    for k in range(1, n_col):
        totals.append(along_col(over_dom[2 * k : 2 * k + 2], -k))

    out = None
    for g, ((base, _), pieces) in enumerate(zip(plan, returned)):
        if g < len(plan) - 1:
            (out,) = place_rows(ids, pieces, out, n_rows, base)
        else:
            out, channel_stats = place_rows(ids, pieces, out, n_rows, base, totals, n_rows * n_dom)
    return (out, channel_stats)


def solution(mesh):
    in_specs = (
        P("dom", "col"),
        P(None, "col"),
        P("col"),
        P("dom", None, None),
        P("dom", None),
        P("dom", None, None, None, None),
        P("dom", None, None),
        P("dom", None),
        P("dom", None, None, None, None),
        P("dom", None, None),
        P("dom", None),
    )
    out_specs = (P("dom", "col"), P(None, "col"))
    return jax.shard_map(
        on_device, mesh=mesh, in_specs=in_specs, out_specs=out_specs, check_vma=False
    )
```

```python
import functools

import jax
import jax.numpy as jnp
from jax import lax
from jax.experimental import pallas as pl
from jax.experimental.pallas import tpu as pltpu
from jax.sharding import PartitionSpec as P


TILE = 128
EPS = 1e-06

HBM = pl.BlockSpec(memory_space=pl.ANY)
VMEM = pl.BlockSpec(memory_space=pltpu.VMEM)
RAW = pl.BlockSpec(memory_space=pltpu.HBM)


def cost(flops, nbytes):
    return pl.CostEstimate(flops=int(flops), bytes_accessed=int(nbytes), transcendentals=0)


def in_hbm(x):
    return pltpu.with_memory_space_constraint(x, pltpu.HBM)


def grant(mib):
    return pltpu.CompilerParams(vmem_limit_bytes=int(mib) << 20)


LANES = 128
SUBLANES = 8
UNROLL = 16


def storage_order(send_rows):
    n, slots = send_rows.shape
    if n % SUBLANES or slots % LANES:
        return send_rows.reshape(-1), lambda q: q * slots, lambda b: b * UNROLL
    blocks = slots // LANES
    tiled = send_rows.reshape(n // SUBLANES, SUBLANES, blocks, LANES)
    tile = SUBLANES * LANES
    per = LANES // UNROLL

    def first(q):
        return (q >> 3) * (blocks * tile) + (q & (SUBLANES - 1)) * LANES

    def within(b):
        return lax.div(b, per) * tile + lax.rem(b, per) * UNROLL

    return tiled.transpose(0, 2, 1, 3).reshape(-1), first, within


def widen(feat, tables, raw, sems):
    n_rows = raw.shape[0]
    parts = sems.shape[0]
    part = n_rows // parts
    step = 64
    copies = [
        pltpu.make_async_copy(
            feat.at[pl.ds(c * part, part)], raw.at[pl.ds(c * part, part)], sems.at[c]
        )
        for c in range(parts)
    ]
    for copy in copies:
        copy.start()
    for c in range(parts):
        copies[c].wait()

        def one(b, carry, c=c):
            at = pl.ds(pl.multiple_of(c * part + b * step, step), step)
            for h, table in enumerate(tables):
                table[at, :] = raw[at, pl.ds(h * LANES, LANES)].astype(jnp.float32)
            return carry

        lax.fori_loop(0, part // step, one, 0)


def gather_kernel(peers, peer, first_row, within, first, halves, rows_in, counts_in, *refs):
    n_out = len(peers)
    refs = list(refs)
    if first:
        feat = refs.pop(0)
        outs, tables = refs[:n_out], refs[n_out : n_out + halves]
        raw = refs[n_out + halves]
        refs = refs[n_out + halves + 1 :]
    else:
        tables, outs = refs[:halves], refs[halves : halves + n_out]
        refs = refs[halves + n_out :]
    rows, counts, index_sems = refs[:3]
    stages = refs[3 : 3 + halves]
    load_rows = pltpu.make_async_copy(rows_in, rows, index_sems.at[0])
    load_counts = pltpu.make_async_copy(counts_in, counts, index_sems.at[1])
    load_rows.start()
    load_counts.start()
    if first:
        widen(feat, tables, raw, refs[3 + halves])
    load_rows.wait()
    load_counts.wait()
    me = lax.axis_index("dom")
    slots = stages[0].shape[0]
    for out, k in zip(outs, peers):
        q = peer(me, k)
        used = counts[q]

        begin = first_row(q)

        def pick(b, carry, begin=begin):
            base = begin + within(b)
            source = [rows[base + j] for j in range(UNROLL)]
            for table, stage in zip(tables, stages):
                got = [table[pl.ds(r, 1), :] for r in source]
                for j in range(UNROLL):
                    stage[pl.ds(b * UNROLL + j, 1), :] = got[j]
            return carry

        lax.fori_loop(0, (used + UNROLL - 1) // UNROLL, pick, 0)
        for b in range(slots // 64):
            at = pl.ds(b * 64, 64)
            slot = b * 64 + lax.broadcasted_iota(jnp.int32, (64, LANES), 0)
            for h, stage in enumerate(stages):
                kept = jnp.where(slot < used, stage[at, :], 0.0)
                out[at, pl.ds(h * LANES, LANES)] = kept.astype(out.dtype)


def gather_rows(rows, first_row, within, send_count, features, tables, peers, peer, slots):
    n_rows, width = features.shape
    halves = width // LANES
    first = not tables
    piece = jax.ShapeDtypeStruct((slots, width), features.dtype)
    table = jax.ShapeDtypeStruct((n_rows, LANES), jnp.float32)
    parts = 8 if n_rows % (8 * 64) == 0 else 1
    out = pl.pallas_call(
        functools.partial(gather_kernel, peers, peer, first_row, within, first, halves),
        out_shape=[piece] * len(peers)
        + ([table] * halves + [pltpu.VMEM(features.shape, features.dtype)]) * first,
        in_specs=[RAW, RAW] + ([RAW] if first else [VMEM] * halves),
        out_specs=[VMEM] * (len(peers) + (halves + 1) * first),
        scratch_shapes=[
            pltpu.SMEM(rows.shape, jnp.int32),
            pltpu.SMEM(send_count.shape, jnp.int32),
            pltpu.SemaphoreType.DMA((2,)),
        ]
        + [pltpu.VMEM((slots, LANES), jnp.float32)] * halves
        + (
            [pltpu.SemaphoreType.DMA((parts,))] if first else []
        ),
        compiler_params=grant(18 + len(peers) if first else 4),
        cost_estimate=cost(4e9, 6 << 20),
        name="gather_rows",
    )(in_hbm(rows), in_hbm(send_count), *([in_hbm(features)] if first else tables))
    return out[: len(peers)], out[len(peers) :]


def sum_kernel(
    n_dom, n_col, peer, slots, piece_rows, per_dest, base,
    own_index, own_counts, halo_index, halo_counts, *refs
):
    pieces = refs[: n_dom - 1]
    feat = refs[n_dom - 1]
    own_vals = refs[n_dom : n_dom + n_col]
    halo_vals = refs[n_dom + n_col : n_dom + 2 * n_col]
    outs = refs[n_dom + 2 * n_col : n_dom + 3 * n_col]
    (halo,) = refs[n_dom + 3 * n_col :]
    sub = pl.program_id(0)
    group = own_vals[0].shape[0]
    col = lax.axis_index("col")

    @pl.when(sub == 0)
    def _():
        me = lax.axis_index("dom")
        for k in range(1, n_dom):
            at = pl.ds(pl.multiple_of(peer(me, -k) * piece_rows, piece_rows), piece_rows)
            halo[at, :] = pieces[k - 1][...]
        own = pl.ds(pl.multiple_of(me * piece_rows, piece_rows), piece_rows)
        halo[own, :] = jnp.zeros((piece_rows, halo.shape[1]), halo.dtype)

    for k in range(n_col):
        dest = lax.rem(col + k, n_col)
        for t in range(group):
            row_tile = dest * per_dest + base + sub * group + t
            left, right = [], []
            for src, index, counts, vals in (
                (feat, own_index, own_counts, own_vals[k]),
                (halo, halo_index, halo_counts, halo_vals[k]),
            ):
                used = counts[row_tile]
                for s in range(slots):
                    left.append(jnp.where(s < used, vals[t, s], jnp.zeros_like(vals[t, s])))
                    at = pl.multiple_of(index[s, row_tile] * TILE, TILE)
                    right.append(src[pl.ds(at, TILE), :])
            total = jnp.dot(
                jnp.concatenate(left, axis=1),
                jnp.concatenate(right, axis=0),
                preferred_element_type=jnp.float32,
            )
            at = pl.ds(pl.multiple_of((sub * group + t) * TILE, TILE), TILE)
            outs[k][at, :] = total.astype(outs[k].dtype)


def tile_sums(tables, pieces, features, own_vals, halo_vals, n_dom, n_col, peer, base, size):
    tiles, slots = own_vals.shape[:2]
    width = features.shape[1]
    piece_rows = pieces[0].shape[0]
    per_dest = tiles // n_col
    group = min(size, 2)
    while base % group or size % group:
        group -= 1

    def vals_spec(k):
        def place(i, *_):
            dest = lax.rem(lax.axis_index("col") + k, n_col)
            return ((dest * per_dest + base) // group + i, 0, 0, 0)

        return pl.BlockSpec((group, slots, TILE, TILE), place)

    rows = size * TILE
    return pl.pallas_call(
        functools.partial(sum_kernel, n_dom, n_col, peer, slots, piece_rows, per_dest, base),
        out_shape=[jax.ShapeDtypeStruct((rows, width), jnp.bfloat16)] * n_col,
        grid_spec=pltpu.PrefetchScalarGridSpec(
            num_scalar_prefetch=4,
            grid=(size // group,),
            in_specs=[VMEM] * n_dom + [vals_spec(k) for k in range(n_col)] * 2,
            out_specs=[VMEM] * n_col,
            scratch_shapes=[pltpu.VMEM((n_dom * piece_rows, width), jnp.bfloat16)],
        ),
        compiler_params=grant(10 + n_dom),
        cost_estimate=cost(2e9, 6 << 20),
        name="tile_sums",
    )(
        *tables, *pieces, pltpu.with_memory_space_constraint(features, pltpu.VMEM),
        *([in_hbm(own_vals)] * n_col), *([in_hbm(halo_vals)] * n_col),
    )


def half_kernel(share, weight, bias, out, sem):
    half = weight.shape[0] // share
    start = lax.rem(lax.axis_index("dom"), share) * half
    src = weight.at[pl.ds(pl.multiple_of(start, half), half)]
    copy = pltpu.make_async_copy(src, out.at[pl.ds(0, half)], sem)
    copy.start()
    tail = (out.shape[0] - half, out.shape[1])
    out[pl.ds(half, tail[0]), :] = jnp.broadcast_to(bias[...], tail)
    copy.wait()


def weight_half(weight, bias, share):
    rows = weight.shape[0] // share + 16
    return pl.pallas_call(
        functools.partial(half_kernel, share),
        out_shape=jax.ShapeDtypeStruct((rows, weight.shape[1]), weight.dtype),
        in_specs=[RAW, VMEM],
        out_specs=VMEM,
        scratch_shapes=[pltpu.SemaphoreType.DMA],
        compiler_params=grant(4),
        cost_estimate=cost(1e8, 1 << 20),
        name="weight_half",
    )(in_hbm(weight), bias)


def join_kernel(n_col, share, *refs):
    own, own_bias = refs[:2]
    mine = refs[2 : n_col + 1]
    theirs = refs[n_col + 1 : -2] or mine
    joined, bias = refs[-2:]
    width = own.shape[1]
    half = own.shape[0] // share
    odd = lax.rem(lax.axis_index("dom"), share)
    for s in range(n_col):
        row = lax.rem(lax.axis_index("col") + n_col - s, n_col) * width
        at = pl.ds(s * width, width)
        joined[0, at, :] = own[pl.ds(pl.multiple_of(row, width), width), :]
        side = lax.div(row, half)
        row = pl.ds(pl.multiple_of(row - side * half, width), width)
        for k in range(1, n_col):

            @pl.when(side == odd)
            def _(k=k, at=at, row=row):
                joined[k, at, :] = mine[k - 1][row, :]

            @pl.when(side != odd)
            def _(k=k, at=at, row=row):
                joined[k, at, :] = theirs[k - 1][row, :]

    bias[pl.ds(0, 1), :] = own_bias[...].astype(jnp.float32)
    for k in range(1, n_col):
        got = mine[k - 1][pl.ds(half, 16), :].astype(jnp.float32)
        bias[pl.ds(k, 1), :] = got[:1]


def join_weights(weight, bias, mine, theirs, share):
    n_col = len(mine) + 1
    channels, width = weight.shape
    return pl.pallas_call(
        functools.partial(join_kernel, n_col, share),
        out_shape=[
            jax.ShapeDtypeStruct((n_col, channels, width), weight.dtype),
            jax.ShapeDtypeStruct((n_col, width), jnp.float32),
        ],
        in_specs=[VMEM] * (2 + len(mine) + len(theirs)),
        out_specs=[VMEM] * 2,
        compiler_params=grant(8),
        cost_estimate=cost(1e9, 4 << 20),
        name="join_weights",
    )(weight, bias, *mine, *theirs)


def mix_kernel(n_col, channels, first, *refs):
    pieces, held, bias = refs[:n_col], refs[n_col], refs[n_col + 1]
    outs, stats = refs[-n_col - 1 : -1], refs[-1]

    @pl.when(pl.program_id(0) == 0)
    def _():
        stats[...] = jnp.zeros_like(stats) if first else refs[n_col + 2][...]

    spread = jnp.concatenate([piece[...] for piece in pieces], axis=1)
    active, power = [], 0.0
    for k in range(n_col):
        mixed = jnp.dot(spread, held[k], preferred_element_type=jnp.float32)
        mixed = jnp.maximum(mixed + bias[pl.ds(k, 1), :], 0.0)
        power = power + jnp.sum(mixed * mixed, axis=1, keepdims=True)
        active.append(mixed)
    scale = lax.rsqrt(power * (1.0 / channels) + EPS)
    for k in range(n_col):
        scaled = active[k] * scale
        outs[k][...] = scaled.astype(outs[k].dtype)
        stats[pl.ds(2 * k, 1), :] += jnp.sum(scaled, axis=0, keepdims=True)
        stats[pl.ds(2 * k + 1, 1), :] += jnp.sum(scaled * scaled, axis=0, keepdims=True)


def mix_rows(pieces, weights, bias, before):
    n_col = len(pieces)
    rows, width = pieces[0].shape
    channels = n_col * width
    block = TILE
    piece = pl.BlockSpec((block, width), lambda i: (i, 0))
    first = before is None
    out = pl.pallas_call(
        functools.partial(mix_kernel, n_col, channels, first),
        out_shape=[jax.ShapeDtypeStruct((rows, width), jnp.bfloat16)] * n_col
        + [jax.ShapeDtypeStruct((2 * n_col, width), jnp.float32)],
        grid=(rows // block,),
        in_specs=[piece] * n_col + [VMEM] * (2 if first else 3),
        out_specs=[piece] * n_col + [VMEM],
        compiler_params=grant(10),
        cost_estimate=cost(2 * rows * channels * channels, 4 << 20),
        name="mix_rows",
    )(*pieces, weights, bias, *([] if first else [before]))
    return out[:n_col], out[n_col]


def place_kernel(n_col, per_dest, base, nodes, *refs):
    pieces = refs[:n_col]
    parts = refs[n_col : 2 * n_col] if nodes else ()
    out, put = refs[-2 - bool(nodes)], refs[-1]
    rows = pieces[0].shape[0]
    stores = []
    for k in range(n_col):
        dest = lax.rem(lax.axis_index("col") + k, n_col)
        at = pl.ds(pl.multiple_of((dest * per_dest + base) * TILE, TILE), rows)
        stores.append(pltpu.make_async_copy(pieces[k], out.at[at], put.at[k]))
    for store in stores:
        store.start()
    if nodes:
        total = parts[0][...]
        for part in parts[1:]:
            total = total + part[...]
        total = total / nodes
        mean = total[0:1]
        refs[-2][pl.ds(0, 1), :] = mean
        refs[-2][pl.ds(1, 1), :] = total[1:2] - mean * mean
    for store in stores:
        store.wait()


def place_rows(pieces, out, n_rows, base, parts=(), nodes=0):
    n_col = len(pieces)
    _, width = pieces[0].shape
    per_dest = n_rows // TILE // n_col
    extra = list(parts) + ([] if out is None else [out])
    out_shape = [jax.ShapeDtypeStruct((n_rows, width), jnp.bfloat16)]
    out_specs = [HBM]
    if nodes:
        out_shape.append(jax.ShapeDtypeStruct((2, width), jnp.float32))
        out_specs.append(VMEM)
    return pl.pallas_call(
        functools.partial(place_kernel, n_col, per_dest, base, nodes),
        out_shape=out_shape,
        in_specs=[VMEM] * (n_col + len(parts)) + ([] if out is None else [HBM]),
        out_specs=out_specs,
        scratch_shapes=[pltpu.SemaphoreType.DMA((n_col,))],
        input_output_aliases={} if out is None else {n_col + len(extra) - 1: 0},
        compiler_params=grant(8),
        cost_estimate=cost(1e8, 2 << 20),
        name="place_rows",
    )(*pieces, *extra)


def chunk_plan(per_dest):
    if per_dest % 8:
        return [(0, per_dest)]
    u = per_dest // 8
    cuts = [0, u, 2 * u, 4 * u, 6 * u, 8 * u]
    return [(a, b - a) for a, b in zip(cuts, cuts[1:])]


def on_device(
    features,
    weight,
    out_bias,
    local_index,
    local_count,
    local_vals,
    halo_index,
    halo_count,
    halo_vals,
    send_rows,
    send_count,
):
    n_rows, width = features.shape
    n_dom, n_col = lax.axis_size("dom"), lax.axis_size("col")

    if n_dom & (n_dom - 1) == 0:
        peer = lambda d, k: d ^ abs(k)
    else:
        peer = lambda d, k: (d + k + n_dom) % n_dom
    along_dom = lambda x, k: lax.ppermute(x, "dom", [(i, peer(i, k)) for i in range(n_dom)])
    along_col = lambda x, k: lax.ppermute(x, "col", [(i, (i + k) % n_col) for i in range(n_col)])

    far = list(reversed(range(1, n_dom)))
    halo = [None] * (n_dom - 1)
    rows, first_row, within = storage_order(send_rows[0])
    slots = send_rows.shape[2]
    tables, own_tiles = [], features
    cut = (n_dom - 1) // 2
    for peers in (far[:cut], far[cut:]):
        if not peers:
            continue
        outgoing, made = gather_rows(
            rows, first_row, within, send_count[0], features, tables, peers, peer, slots
        )
        if made:
            tables, own_tiles = made[:-1], made[-1]
        for k, piece in zip(peers, outgoing):
            halo[k - 1] = along_dom(piece, k)

    share = 2 if n_dom % 2 == 0 else 1
    order = sorted(range(1, n_col), key=lambda k: min(k, n_col - k), reverse=True)
    bias_row = out_bias.reshape(1, width)
    mine = weight_half(weight, bias_row, share)
    arrived = {k: along_col(mine, k) for k in order}
    mine = [arrived[k] for k in range(1, n_col)]
    theirs = []
    if share == 2:
        swap = [(i, i ^ 1) for i in range(n_dom)]
        theirs = [lax.ppermute(got, "dom", swap) for got in mine]
    weights, bias = join_weights(weight, bias_row, mine, theirs, share)

    plan = chunk_plan(n_rows // TILE // n_col)
    index_tables = (local_index[0].T, local_count[0], halo_index[0].T, halo_count[0])
    incoming = []
    for base, size in plan:
        sums = tile_sums(
            index_tables, halo, own_tiles, local_vals[0], halo_vals[0],
            n_dom, n_col, peer, base, size,
        )
        moved = {k: along_col(sums[k], k) for k in order}
        incoming.append([sums[0]] + [moved[k] for k in range(1, n_col)])

    stats = None
    returned = []
    for pieces in incoming:
        done, stats = mix_rows(pieces, weights, bias, stats)
        moved = {k: along_col(done[k], -k) for k in order}
        returned.append([done[0]] + [moved[k] for k in range(1, n_col)])

    over_dom = lax.all_gather(stats, "dom", axis=0)
    over_dom = over_dom.sum(axis=0)
    totals = [over_dom[:2]]
    for k in range(1, n_col):
        totals.append(along_col(over_dom[2 * k : 2 * k + 2], -k))

    out = None
    for g, ((base, _), pieces) in enumerate(zip(plan, returned)):
        if g < len(plan) - 1:
            (out,) = place_rows(pieces, out, n_rows, base)
        else:
            out, channel_stats = place_rows(
                pieces, out, n_rows, base, totals, n_rows * n_dom
            )
    return (out, channel_stats)


def solution(mesh):
    in_specs = (
        P("dom", "col"),
        P(None, "col"),
        P("col"),
        P("dom", None, None),
        P("dom", None),
        P("dom", None, None, None, None),
        P("dom", None, None),
        P("dom", None),
        P("dom", None, None, None, None),
        P("dom", None, None),
        P("dom", None),
    )
    out_specs = (P("dom", "col"), P(None, "col"))
    return jax.shard_map(
        on_device, mesh=mesh, in_specs=in_specs, out_specs=out_specs, check_vma=False
    )
```

```python
import functools

import jax
import jax.numpy as jnp
from jax import lax
from jax.experimental import pallas as pl
from jax.experimental.pallas import tpu as pltpu
from jax.sharding import PartitionSpec as P


TILE = 128
EPS = 1e-06

HBM = pl.BlockSpec(memory_space=pl.ANY)
VMEM = pl.BlockSpec(memory_space=pltpu.VMEM)
RAW = pl.BlockSpec(memory_space=pltpu.HBM)


def cost(flops, nbytes):
    return pl.CostEstimate(flops=int(flops), bytes_accessed=int(nbytes), transcendentals=0)


def in_hbm(x):
    return pltpu.with_memory_space_constraint(x, pltpu.HBM)


def grant(mib):
    return pltpu.CompilerParams(vmem_limit_bytes=int(mib) << 20)


LANES = 128
SUBLANES = 8
UNROLL = 16


def storage_order(send_rows):
    n, slots = send_rows.shape
    if n % SUBLANES or slots % LANES:
        return send_rows.reshape(-1), lambda q: q * slots, lambda b: b * UNROLL
    blocks = slots // LANES
    tiled = send_rows.reshape(n // SUBLANES, SUBLANES, blocks, LANES)
    tile = SUBLANES * LANES
    per = LANES // UNROLL

    def first(q):
        return (q >> 3) * (blocks * tile) + (q & (SUBLANES - 1)) * LANES

    def within(b):
        return lax.div(b, per) * tile + lax.rem(b, per) * UNROLL

    return tiled.transpose(0, 2, 1, 3).reshape(-1), first, within


def widen(feat, table, raw, sems):
    n_rows = raw.shape[0]
    parts = sems.shape[0]
    part = n_rows // parts
    step = 64
    copies = [
        pltpu.make_async_copy(
            feat.at[pl.ds(c * part, part)], raw.at[pl.ds(c * part, part)], sems.at[c]
        )
        for c in range(parts)
    ]
    for copy in copies:
        copy.start()
    for c in range(parts):
        copies[c].wait()

        def one(b, carry, c=c):
            row = pl.multiple_of(c * part + b * step, step)
            halves = raw.shape[1] // LANES
            for h in range(halves):
                wide = raw[pl.ds(row, step), pl.ds(h * LANES, LANES)].astype(jnp.float32)
                table[pl.ds(row * halves + h, step, stride=halves), :] = wide
            return carry

        lax.fori_loop(0, part // step, one, 0)


def gather_kernel(peers, peer, first_row, within, first, halves, rows_in, counts_in, *refs):
    n_out = len(peers)
    if first:
        feat, outs, (table, raw) = refs[0], refs[1 : n_out + 1], refs[n_out + 1 : n_out + 3]
        rows, counts, index_sems, stage, sems = refs[n_out + 3 :]
    else:
        table, outs = refs[0], refs[1 : n_out + 1]
        rows, counts, index_sems, stage = refs[n_out + 1 :]
    load_rows = pltpu.make_async_copy(rows_in, rows, index_sems.at[0])
    load_counts = pltpu.make_async_copy(counts_in, counts, index_sems.at[1])
    load_rows.start()
    load_counts.start()
    if first:
        widen(feat, table, raw, sems)
    load_rows.wait()
    load_counts.wait()
    me = lax.axis_index("dom")
    slots = outs[0].shape[0]
    for out, k in zip(outs, peers):
        q = peer(me, k)
        used = counts[q]
        begin = first_row(q)

        def pick(b, carry, begin=begin):
            base = begin + within(b)
            put = pl.multiple_of(b * (UNROLL * halves), UNROLL * halves)
            source = [rows[base + j] for j in range(UNROLL)]
            got = [table[pl.ds(r * halves, halves), :] for r in source]
            for j in range(UNROLL):
                stage[pl.ds(put + j * halves, halves), :] = got[j]
            return carry

        lax.fori_loop(0, (used + UNROLL - 1) // UNROLL, pick, 0)
        for b in range(slots // 64):
            slot = b * 64 + lax.broadcasted_iota(jnp.int32, (64, LANES), 0)
            for h in range(halves):
                wide = stage[pl.ds(b * 64 * halves + h, 64, stride=halves), :]
                kept = jnp.where(slot < used, wide, 0.0)
                out[pl.ds(b * 64, 64), pl.ds(h * LANES, LANES)] = kept.astype(out.dtype)


def gather_rows(rows, first_row, within, send_count, features, table, peers, peer, slots):
    n_rows, width = features.shape
    halves = width // LANES
    first = table is None
    piece = jax.ShapeDtypeStruct((slots, width), features.dtype)
    parts = 8 if n_rows % (8 * 64) == 0 else 1
    made = [
        jax.ShapeDtypeStruct((n_rows * halves, LANES), jnp.float32),
        jax.ShapeDtypeStruct(features.shape, features.dtype),
    ]
    out = pl.pallas_call(
        functools.partial(gather_kernel, peers, peer, first_row, within, first, halves),
        out_shape=[piece] * len(peers) + made * first,
        in_specs=[RAW, RAW, RAW if first else VMEM],
        out_specs=[VMEM] * (len(peers) + 2 * first),
        scratch_shapes=[
            pltpu.SMEM(rows.shape, jnp.int32),
            pltpu.SMEM(send_count.shape, jnp.int32),
            pltpu.SemaphoreType.DMA((2,)),
            pltpu.VMEM((slots * halves, LANES), jnp.float32),
        ]
        + [pltpu.SemaphoreType.DMA((parts,))] * first,
        compiler_params=grant(18 + len(peers) if first else 4),
        cost_estimate=cost(4e9, 6 << 20),
        name="gather_rows",
    )(in_hbm(rows), in_hbm(send_count), in_hbm(features) if first else table)
    return out[: len(peers)], out[len(peers) :]


def sum_kernel(
    n_dom, n_col, peer, slots, piece_rows, per_dest, base,
    own_index, own_counts, halo_index, halo_counts, *refs
):
    pieces = refs[: n_dom - 1]
    feat = refs[n_dom - 1]
    own_vals = refs[n_dom : n_dom + n_col]
    halo_vals = refs[n_dom + n_col : n_dom + 2 * n_col]
    outs = refs[n_dom + 2 * n_col : n_dom + 3 * n_col]
    (halo,) = refs[n_dom + 3 * n_col :]
    sub = pl.program_id(0)
    group = own_vals[0].shape[0]
    col = lax.axis_index("col")

    @pl.when(sub == 0)
    def _():
        me = lax.axis_index("dom")
        for k in range(1, n_dom):
            at = pl.ds(pl.multiple_of(peer(me, -k) * piece_rows, piece_rows), piece_rows)
            halo[at, :] = pieces[k - 1][...]
        own = pl.ds(pl.multiple_of(me * piece_rows, piece_rows), piece_rows)
        halo[own, :] = jnp.zeros((piece_rows, halo.shape[1]), halo.dtype)

    for k in range(n_col):
        dest = lax.rem(col + k, n_col)
        for t in range(group):
            row_tile = dest * per_dest + base + sub * group + t
            left, right = [], []
            for src, index, counts, vals in (
                (feat, own_index, own_counts, own_vals[k]),
                (halo, halo_index, halo_counts, halo_vals[k]),
            ):
                used = counts[row_tile]
                for s in range(slots):
                    left.append(jnp.where(s < used, vals[t, s], jnp.zeros_like(vals[t, s])))
                    at = pl.multiple_of(index[s, row_tile] * TILE, TILE)
                    right.append(src[pl.ds(at, TILE), :])
            total = jnp.dot(
                jnp.concatenate(left, axis=1),
                jnp.concatenate(right, axis=0),
                preferred_element_type=jnp.float32,
            )
            at = pl.ds(pl.multiple_of((sub * group + t) * TILE, TILE), TILE)
            outs[k][at, :] = total.astype(outs[k].dtype)


def tile_sums(tables, pieces, features, own_vals, halo_vals, n_dom, n_col, peer, base, size):
    tiles, slots = own_vals.shape[:2]
    width = features.shape[1]
    piece_rows = pieces[0].shape[0]
    per_dest = tiles // n_col
    group = min(size, 2)
    while base % group or size % group:
        group -= 1

    def vals_spec(k):
        def place(i, *_):
            dest = lax.rem(lax.axis_index("col") + k, n_col)
            return ((dest * per_dest + base) // group + i, 0, 0, 0)

        return pl.BlockSpec((group, slots, TILE, TILE), place)

    rows = size * TILE
    return pl.pallas_call(
        functools.partial(sum_kernel, n_dom, n_col, peer, slots, piece_rows, per_dest, base),
        out_shape=[jax.ShapeDtypeStruct((rows, width), jnp.bfloat16)] * n_col,
        grid_spec=pltpu.PrefetchScalarGridSpec(
            num_scalar_prefetch=4,
            grid=(size // group,),
            in_specs=[VMEM] * n_dom + [vals_spec(k) for k in range(n_col)] * 2,
            out_specs=[VMEM] * n_col,
            scratch_shapes=[pltpu.VMEM((n_dom * piece_rows, width), jnp.bfloat16)],
        ),
        compiler_params=grant(10 + n_dom),
        cost_estimate=cost(2e9, 6 << 20),
        name="tile_sums",
    )(
        *tables, *pieces, pltpu.with_memory_space_constraint(features, pltpu.VMEM),
        *([in_hbm(own_vals)] * n_col), *([in_hbm(halo_vals)] * n_col),
    )


PAD = 16


def part_kernel(share, weight, bias, out, sem):
    part = weight.shape[0] // share
    start = lax.rem(lax.axis_index("dom"), share) * part
    src = weight.at[pl.ds(pl.multiple_of(start, part), part)]
    copy = pltpu.make_async_copy(src, out.at[pl.ds(0, part)], sem)
    copy.start()
    out[pl.ds(part, PAD), :] = jnp.broadcast_to(bias[...], (PAD, out.shape[1]))
    copy.wait()


def weight_part(weight, bias, share):
    rows = weight.shape[0] // share + PAD
    return pl.pallas_call(
        functools.partial(part_kernel, share),
        out_shape=jax.ShapeDtypeStruct((rows, weight.shape[1]), weight.dtype),
        in_specs=[RAW, VMEM],
        out_specs=VMEM,
        scratch_shapes=[pltpu.SemaphoreType.DMA],
        compiler_params=grant(4),
        cost_estimate=cost(1e8, 1 << 20),
        name="weight_part",
    )(in_hbm(weight), bias)


def pack_kernel(*refs):
    rows = refs[0].shape[0]
    for k, ref in enumerate(refs[:-1]):
        refs[-1][pl.ds(k * rows, rows), :] = ref[...]


def pack_rows(arrays):
    rows, width = arrays[0].shape
    return pl.pallas_call(
        pack_kernel,
        out_shape=jax.ShapeDtypeStruct((rows * len(arrays), width), arrays[0].dtype),
        in_specs=[VMEM] * len(arrays),
        out_specs=VMEM,
        compiler_params=grant(4),
        cost_estimate=cost(1e8, 1 << 20),
        name="pack_rows",
    )(*arrays)


def join_kernel(n_col, share, own, own_bias, *refs):
    parts = refs[:share]
    joined, bias = refs[share:]
    width = own.shape[1]
    part = own.shape[0] // share
    me = lax.rem(lax.axis_index("dom"), share)
    block = min(width, part)
    for s in range(n_col):
        for b in range(width // block):
            row = lax.rem(lax.axis_index("col") + n_col - s, n_col) * width + b * block
            row = pl.multiple_of(row, block)
            at = pl.ds(s * width + b * block, block)
            joined[0, at, :] = own[pl.ds(row, block), :]
            side = lax.div(row, part)
            offset = row - side * part
            for flip in range(share):

                @pl.when(side == me ^ flip)
                def _(flip=flip, at=at, offset=offset):
                    for k in range(1, n_col):
                        start = pl.multiple_of((k - 1) * (part + PAD) + offset, PAD)
                        joined[k, at, :] = parts[flip][pl.ds(start, block), :]

    bias[pl.ds(0, 1), :] = own_bias[...].astype(jnp.float32)
    for k in range(1, n_col):
        got = parts[0][pl.ds(k * part + (k - 1) * PAD, PAD), :].astype(jnp.float32)
        bias[pl.ds(k, 1), :] = got[:1]


def join_weights(weight, bias, parts, n_col):
    channels, width = weight.shape
    share = len(parts)
    return pl.pallas_call(
        functools.partial(join_kernel, n_col, share),
        out_shape=[
            jax.ShapeDtypeStruct((n_col, channels, width), weight.dtype),
            jax.ShapeDtypeStruct((n_col, width), jnp.float32),
        ],
        in_specs=[VMEM] * (2 + share),
        out_specs=[VMEM] * 2,
        compiler_params=grant(8),
        cost_estimate=cost(1e9, 4 << 20),
        name="join_weights",
    )(weight, bias, *parts)


def mix_kernel(n_col, channels, first, *refs):
    pieces, held, bias = refs[:n_col], refs[n_col], refs[n_col + 1]
    outs, stats = refs[-n_col - 1 : -1], refs[-1]

    @pl.when(pl.program_id(0) == 0)
    def _():
        stats[...] = jnp.zeros_like(stats) if first else refs[n_col + 2][...]

    spread = jnp.concatenate([piece[...] for piece in pieces], axis=1)
    active, power = [], 0.0
    for k in range(n_col):
        mixed = jnp.dot(spread, held[k], preferred_element_type=jnp.float32)
        mixed = jnp.maximum(mixed + bias[pl.ds(k, 1), :], 0.0)
        power = power + jnp.sum(mixed * mixed, axis=1, keepdims=True)
        active.append(mixed)
    scale = lax.rsqrt(power * (1.0 / channels) + EPS)
    for k in range(n_col):
        scaled = active[k] * scale
        outs[k][...] = scaled.astype(outs[k].dtype)
        stats[pl.ds(2 * k, 1), :] += jnp.sum(scaled, axis=0, keepdims=True)
        stats[pl.ds(2 * k + 1, 1), :] += jnp.sum(scaled * scaled, axis=0, keepdims=True)


def mix_rows(pieces, weights, bias, before):
    n_col = len(pieces)
    rows, width = pieces[0].shape
    channels = n_col * width
    block = TILE
    piece = pl.BlockSpec((block, width), lambda i: (i, 0))
    first = before is None
    out = pl.pallas_call(
        functools.partial(mix_kernel, n_col, channels, first),
        out_shape=[jax.ShapeDtypeStruct((rows, width), jnp.bfloat16)] * n_col
        + [jax.ShapeDtypeStruct((2 * n_col, width), jnp.float32)],
        grid=(rows // block,),
        in_specs=[piece] * n_col + [VMEM] * (2 if first else 3),
        out_specs=[piece] * n_col + [VMEM],
        compiler_params=grant(10),
        cost_estimate=cost(2 * rows * channels * channels, 4 << 20),
        name="mix_rows",
    )(*pieces, weights, bias, *([] if first else [before]))
    return out[:n_col], out[n_col]


def place_kernel(n_col, per_dest, base, nodes, *refs):
    pieces = refs[:n_col]
    parts = refs[n_col : 2 * n_col] if nodes else ()
    out, put = refs[-2 - bool(nodes)], refs[-1]
    rows = pieces[0].shape[0]
    stores = []
    for k in range(n_col):
        dest = lax.rem(lax.axis_index("col") + k, n_col)
        at = pl.ds(pl.multiple_of((dest * per_dest + base) * TILE, TILE), rows)
        stores.append(pltpu.make_async_copy(pieces[k], out.at[at], put.at[k]))
    for store in stores:
        store.start()
    if nodes:
        total = parts[0][...]
        for part in parts[1:]:
            total = total + part[...]
        total = total / nodes
        mean = total[0:1]
        refs[-2][pl.ds(0, 1), :] = mean
        refs[-2][pl.ds(1, 1), :] = total[1:2] - mean * mean
    for store in stores:
        store.wait()


def place_rows(pieces, out, n_rows, base, parts=(), nodes=0):
    n_col = len(pieces)
    _, width = pieces[0].shape
    per_dest = n_rows // TILE // n_col
    extra = list(parts) + ([] if out is None else [out])
    out_shape = [jax.ShapeDtypeStruct((n_rows, width), jnp.bfloat16)]
    out_specs = [HBM]
    if nodes:
        out_shape.append(jax.ShapeDtypeStruct((2, width), jnp.float32))
        out_specs.append(VMEM)
    return pl.pallas_call(
        functools.partial(place_kernel, n_col, per_dest, base, nodes),
        out_shape=out_shape,
        in_specs=[VMEM] * (n_col + len(parts)) + ([] if out is None else [HBM]),
        out_specs=out_specs,
        scratch_shapes=[pltpu.SemaphoreType.DMA((n_col,))],
        input_output_aliases={} if out is None else {n_col + len(extra) - 1: 0},
        compiler_params=grant(8),
        cost_estimate=cost(1e8, 2 << 20),
        name="place_rows",
    )(*pieces, *extra)


def chunk_plan(per_dest):
    if per_dest % 8:
        return [(0, per_dest)]
    u = per_dest // 8
    cuts = [0, u, 2 * u, 4 * u, 6 * u, 8 * u]
    return [(a, b - a) for a, b in zip(cuts, cuts[1:])]


def on_device(
    features,
    weight,
    out_bias,
    local_index,
    local_count,
    local_vals,
    halo_index,
    halo_count,
    halo_vals,
    send_rows,
    send_count,
):
    n_rows, width = features.shape
    n_dom, n_col = lax.axis_size("dom"), lax.axis_size("col")

    if n_dom & (n_dom - 1) == 0:
        peer = lambda d, k: d ^ abs(k)
    else:
        peer = lambda d, k: (d + k + n_dom) % n_dom
    along_dom = lambda x, k: lax.ppermute(x, "dom", [(i, peer(i, k)) for i in range(n_dom)])
    along_col = lambda x, k: lax.ppermute(x, "col", [(i, (i + k) % n_col) for i in range(n_col)])

    far = list(reversed(range(1, n_dom)))
    halo = [None] * (n_dom - 1)
    rows, first_row, within = storage_order(send_rows[0])
    slots = send_rows.shape[2]
    table, own_tiles = None, features
    cut = (n_dom - 1) // 2
    for peers in (far[:cut], far[cut:]):
        if not peers:
            continue
        outgoing, made = gather_rows(
            rows, first_row, within, send_count[0], features, table, peers, peer, slots
        )
        if made:
            table, own_tiles = made
        for k, piece in zip(peers, outgoing):
            halo[k - 1] = along_dom(piece, k)

    share = 1
    while share < min(4, n_col) and n_dom % (2 * share) == 0:
        share *= 2
    order = sorted(range(1, n_col), key=lambda k: min(k, n_col - k), reverse=True)
    bias_row = out_bias.reshape(1, width)
    mine = weight_part(weight, bias_row, share)
    arrived = {k: along_col(mine, k) for k in order}
    parts = [pack_rows([arrived[k] for k in range(1, n_col)])]
    step = share // 2
    got = {0: parts[0]}
    while step:
        swap = [(i, i ^ step) for i in range(n_dom)]
        for flip in list(got):
            got[flip ^ step] = lax.ppermute(got[flip], "dom", swap)
        step //= 2
    weights, bias = join_weights(weight, bias_row, [got[f] for f in range(share)], n_col)

    plan = chunk_plan(n_rows // TILE // n_col)
    index_tables = (local_index[0].T, local_count[0], halo_index[0].T, halo_count[0])
    incoming = []
    for base, size in plan:
        sums = tile_sums(
            index_tables, halo, own_tiles, local_vals[0], halo_vals[0],
            n_dom, n_col, peer, base, size,
        )
        moved = {k: along_col(sums[k], k) for k in order}
        incoming.append([sums[0]] + [moved[k] for k in range(1, n_col)])

    stats = None
    returned = []
    for pieces in incoming:
        done, stats = mix_rows(pieces, weights, bias, stats)
        moved = {k: along_col(done[k], -k) for k in order}
        returned.append([done[0]] + [moved[k] for k in range(1, n_col)])

    over_dom = lax.all_gather(stats, "dom", axis=0)
    over_dom = over_dom.sum(axis=0)
    totals = [over_dom[:2]]
    for k in range(1, n_col):
        totals.append(along_col(over_dom[2 * k : 2 * k + 2], -k))

    out = None
    for g, ((base, _), pieces) in enumerate(zip(plan, returned)):
        if g < len(plan) - 1:
            (out,) = place_rows(pieces, out, n_rows, base)
        else:
            out, channel_stats = place_rows(
                pieces, out, n_rows, base, totals, n_rows * n_dom
            )
    return (out, channel_stats)


def solution(mesh):
    in_specs = (
        P("dom", "col"),
        P(None, "col"),
        P("col"),
        P("dom", None, None),
        P("dom", None),
        P("dom", None, None, None, None),
        P("dom", None, None),
        P("dom", None),
        P("dom", None, None, None, None),
        P("dom", None, None),
        P("dom", None),
    )
    out_specs = (P("dom", "col"), P(None, "col"))
    return jax.shard_map(
        on_device, mesh=mesh, in_specs=in_specs, out_specs=out_specs, check_vma=False
    )
```

```python
import functools

import jax
import jax.numpy as jnp
from jax import lax
from jax.experimental import pallas as pl
from jax.experimental.pallas import tpu as pltpu
from jax.sharding import PartitionSpec as P


TILE = 128
EPS = 1e-06

HBM = pl.BlockSpec(memory_space=pl.ANY)
VMEM = pl.BlockSpec(memory_space=pltpu.VMEM)
RAW = pl.BlockSpec(memory_space=pltpu.HBM)


def cost(flops, nbytes):
    return pl.CostEstimate(flops=int(flops), bytes_accessed=int(nbytes), transcendentals=0)


def in_hbm(x):
    return pltpu.with_memory_space_constraint(x, pltpu.HBM)


def in_vmem(x):
    return pltpu.with_memory_space_constraint(x, pltpu.VMEM)


def grant(mib):
    return pltpu.CompilerParams(vmem_limit_bytes=int(mib) << 20)


LANES = 128
SUBLANES = 8
UNROLL = 32


def storage_order(send_rows):
    n, slots = send_rows.shape
    if n % SUBLANES or slots % LANES:
        return send_rows.reshape(-1), lambda q: q * slots, lambda b: b * UNROLL
    blocks = slots // LANES
    tiled = send_rows.reshape(n // SUBLANES, SUBLANES, blocks, LANES)
    tile = SUBLANES * LANES
    per = LANES // UNROLL

    def first(q):
        return (q >> 3) * (blocks * tile) + (q & (SUBLANES - 1)) * LANES

    def within(b):
        return (b >> (per.bit_length() - 1)) * tile + (b & (per - 1)) * UNROLL

    return tiled.transpose(0, 2, 1, 3).reshape(-1), first, within


def widen(feat, table, raw, sems):
    n_rows = raw.shape[0]
    parts = sems.shape[0]
    part = n_rows // parts
    step = 64
    copies = [
        pltpu.make_async_copy(
            feat.at[pl.ds(c * part, part)], raw.at[pl.ds(c * part, part)], sems.at[c]
        )
        for c in range(parts)
    ]
    for copy in copies:
        copy.start()
    for c in range(parts):
        copies[c].wait()

        def one(b, carry, c=c):
            row = pl.multiple_of(c * part + b * step, step)
            halves = raw.shape[1] // LANES
            for h in range(halves):
                wide = raw[pl.ds(row, step), pl.ds(h * LANES, LANES)].astype(jnp.float32)
                table[pl.ds(row * halves + h, step, stride=halves), :] = wide
            return carry

        lax.fori_loop(0, part // step, one, 0)


def gather_kernel(peers, peer, first_row, within, first, halves, rows_in, counts_in, *refs):
    n_out = len(peers)
    if first:
        feat, outs, (table, raw) = refs[0], refs[1 : n_out + 1], refs[n_out + 1 : n_out + 3]
        rows, counts, index_sems, stage, sems = refs[n_out + 3 :]
    else:
        table, outs = refs[0], refs[1 : n_out + 1]
        rows, counts, index_sems, stage = refs[n_out + 1 :]
    load_rows = pltpu.make_async_copy(rows_in, rows, index_sems.at[0])
    load_counts = pltpu.make_async_copy(counts_in, counts, index_sems.at[1])
    load_rows.start()
    load_counts.start()
    if first:
        widen(feat, table, raw, sems)
    load_rows.wait()
    load_counts.wait()
    me = lax.axis_index("dom")
    slots = outs[0].shape[0]
    for out, k in zip(outs, peers):
        q = peer(me, k)
        used = counts[q]
        begin = first_row(q)

        def pick(b, carry, begin=begin):
            base = begin + within(b)
            put = pl.multiple_of(b * (UNROLL * halves), UNROLL * halves)
            source = [rows[base + j] for j in range(UNROLL)]
            got = [table[pl.ds(r * halves, halves), :] for r in source]
            for j in range(UNROLL):
                stage[pl.ds(put + j * halves, halves), :] = got[j]
            return carry

        lax.fori_loop(0, (used + UNROLL - 1) // UNROLL, pick, 0)
        for b in range(slots // 64):
            slot = b * 64 + lax.broadcasted_iota(jnp.int32, (64, LANES), 0)
            for h in range(halves):
                wide = stage[pl.ds(b * 64 * halves + h, 64, stride=halves), :]
                kept = jnp.where(slot < used, wide, 0.0)
                out[pl.ds(b * 64, 64), pl.ds(h * LANES, LANES)] = kept.astype(out.dtype)


def gather_rows(rows, first_row, within, send_count, features, table, peers, peer, slots):
    n_rows, width = features.shape
    halves = width // LANES
    first = table is None
    piece = jax.ShapeDtypeStruct((slots, width), features.dtype)
    parts = 8 if n_rows % (8 * 64) == 0 else 1
    made = [
        jax.ShapeDtypeStruct((n_rows * halves, LANES), jnp.float32),
        jax.ShapeDtypeStruct(features.shape, features.dtype),
    ]
    out = pl.pallas_call(
        functools.partial(gather_kernel, peers, peer, first_row, within, first, halves),
        out_shape=[piece] * len(peers) + made * first,
        in_specs=[RAW, RAW, RAW if first else VMEM],
        out_specs=[VMEM] * (len(peers) + 2 * first),
        scratch_shapes=[
            pltpu.SMEM(rows.shape, jnp.int32),
            pltpu.SMEM(send_count.shape, jnp.int32),
            pltpu.SemaphoreType.DMA((2,)),
            pltpu.VMEM((slots * halves, LANES), jnp.float32),
        ]
        + [pltpu.SemaphoreType.DMA((parts,))] * first,
        compiler_params=grant(18 + len(peers) if first else 4),
        cost_estimate=cost(4e9, 6 << 20),
        name="gather_rows",
    )(in_hbm(rows), in_hbm(send_count), in_hbm(features) if first else table)
    return out[: len(peers)], out[len(peers) :]


def masked(vals, used):
    return [
        jnp.where(s < used, vals[s], jnp.zeros_like(vals[s])) for s in range(vals.shape[0])
    ]


def tiles_of(src, index, row_tile, slots):
    starts = [pl.multiple_of(index[s, row_tile] * TILE, TILE) for s in range(slots)]
    return [src[pl.ds(at, TILE), :] for at in starts]


def product(left, right):
    return jnp.dot(
        jnp.concatenate(left, axis=1),
        jnp.concatenate(right, axis=0),
        preferred_element_type=jnp.float32,
    )


def vals_specs(n_col, per_dest, base, group, slots):
    def spec(k):
        def place(i, *_):
            dest = lax.rem(lax.axis_index("col") + k, n_col)
            return ((dest * per_dest + base) // group + i, 0, 0, 0)

        return pl.BlockSpec((group, slots, TILE, TILE), place)

    return [spec(k) for k in range(n_col)]


def row_tile_of(k, n_col, per_dest, tile):
    return lax.rem(lax.axis_index("col") + k, n_col) * per_dest + tile


def early_kernel(n_col, slots, per_dest, own_index, own_counts, halo_counts, feat, *refs):
    own_vals, halo_vals, (part, kept) = refs[:n_col], refs[n_col:-2], refs[-2:]
    i = pl.program_id(0)
    for k in range(n_col):
        row_tile = row_tile_of(k, n_col, per_dest, i)
        part[k, pl.ds(pl.multiple_of(i * TILE, TILE), TILE), :] = product(
            masked(own_vals[k][0], own_counts[row_tile]),
            tiles_of(feat, own_index, row_tile, slots),
        )
        for s, vals in enumerate(masked(halo_vals[k][0], halo_counts[row_tile])):
            kept[k, i, s] = vals


def early_sums(tables, features, own_vals, halo_vals, n_col, size):
    tiles, slots = own_vals.shape[:2]
    width = features.shape[1]
    per_dest = tiles // n_col
    own_index, own_counts, _, halo_counts = tables
    return pl.pallas_call(
        functools.partial(early_kernel, n_col, slots, per_dest),
        out_shape=[
            jax.ShapeDtypeStruct((n_col, size * TILE, width), jnp.float32),
            jax.ShapeDtypeStruct((n_col, size, slots, TILE, TILE), halo_vals.dtype),
        ],
        grid_spec=pltpu.PrefetchScalarGridSpec(
            num_scalar_prefetch=3,
            grid=(size,),
            in_specs=[VMEM] + vals_specs(n_col, per_dest, 0, 1, slots) * 2,
            out_specs=[VMEM] * 2,
        ),
        compiler_params=grant(16),
        cost_estimate=cost(2e9, 4 << 20),
        name="early_sums",
    )(
        own_index, own_counts, halo_counts, in_vmem(features),
        *([in_hbm(own_vals)] * n_col), *([in_hbm(halo_vals)] * n_col),
    )


def put_piece(halo, piece, q):
    rows = piece.shape[0]
    halo[pl.ds(pl.multiple_of(q * rows, rows), rows), :] = piece[...]


def assemble_kernel(ks, peer, *refs):
    pieces, halo = refs[:-1], refs[-1]
    me = lax.axis_index("dom")
    for k, piece in zip(ks, pieces):
        put_piece(halo, piece, peer(me, -k))
    rows = pieces[0].shape[0]
    own = pl.ds(pl.multiple_of(me * rows, rows), rows)
    halo[own, :] = jnp.zeros((rows, halo.shape[1]), halo.dtype)


def assemble(ks, pieces, n_dom, peer):
    rows, width = pieces[0].shape
    return pl.pallas_call(
        functools.partial(assemble_kernel, ks, peer),
        out_shape=jax.ShapeDtypeStruct((n_dom * rows, width), pieces[0].dtype),
        in_specs=[VMEM] * len(pieces),
        out_specs=VMEM,
        compiler_params=grant(4 + n_dom),
        cost_estimate=cost(2e9, 4 << 20),
        name="assemble",
    )(*pieces)


def first_kernel(n_col, slots, per_dest, ks, peer, index, *refs):
    pieces = refs[: len(ks)]
    part, kept = refs[len(ks) : len(ks) + 2]
    outs, halo = refs[-n_col - 1 : -1], refs[-1]
    me = lax.axis_index("dom")
    for k, piece in zip(ks, pieces):
        put_piece(halo, piece, peer(me, -k))
    for t in range(kept.shape[1]):
        at = pl.ds(t * TILE, TILE)
        for k in range(n_col):
            right = tiles_of(halo, index, row_tile_of(k, n_col, per_dest, t), slots)
            total = part[k, at, :] + product([kept[k, t, s] for s in range(slots)], right)
            outs[k][at, :] = total.astype(outs[k].dtype)


def first_sums(index, ks, pieces, part, kept, halo, per_dest, peer):
    n_col, size, slots = kept.shape[:3]
    width = halo.shape[1]
    out = pl.pallas_call(
        functools.partial(first_kernel, n_col, slots, per_dest, ks, peer),
        out_shape=[jax.ShapeDtypeStruct((size * TILE, width), halo.dtype)] * n_col
        + [jax.ShapeDtypeStruct(halo.shape, halo.dtype)],
        in_specs=[pl.BlockSpec(memory_space=pltpu.SMEM)] + [VMEM] * (len(ks) + 3),
        out_specs=[VMEM] * (n_col + 1),
        input_output_aliases={len(ks) + 3: n_col},
        compiler_params=grant(6 + halo.shape[0] // (1 << 12)),
        cost_estimate=cost(2e9, 4 << 20),
        name="first_sums",
    )(index, *pieces, part, kept, halo)
    return out[:n_col], out[n_col]


def sum_kernel(n_col, slots, per_dest, base, *refs):
    own_index, own_counts, halo_index, halo_counts, feat, halo = refs[:6]
    own_vals, halo_vals = refs[6 : 6 + n_col], refs[6 + n_col : 6 + 2 * n_col]
    outs = refs[6 + 2 * n_col :]
    sub = pl.program_id(0)
    group = own_vals[0].shape[0]
    for k in range(n_col):
        for t in range(group):
            row_tile = row_tile_of(k, n_col, per_dest, base + sub * group + t)
            left = masked(own_vals[k][t], own_counts[row_tile])
            left += masked(halo_vals[k][t], halo_counts[row_tile])
            right = tiles_of(feat, own_index, row_tile, slots)
            right += tiles_of(halo, halo_index, row_tile, slots)
            at = pl.ds(pl.multiple_of((sub * group + t) * TILE, TILE), TILE)
            outs[k][at, :] = product(left, right).astype(outs[k].dtype)


def tile_sums(tables, halo, features, own_vals, halo_vals, n_col, base, size):
    tiles, slots = own_vals.shape[:2]
    width = features.shape[1]
    per_dest = tiles // n_col
    group = min(size, 2)
    while base % group or size % group:
        group -= 1
    specs = vals_specs(n_col, per_dest, base, group, slots)
    return pl.pallas_call(
        functools.partial(sum_kernel, n_col, slots, per_dest, base),
        out_shape=[jax.ShapeDtypeStruct((size * TILE, width), jnp.bfloat16)] * n_col,
        grid_spec=pltpu.PrefetchScalarGridSpec(
            num_scalar_prefetch=4,
            grid=(size // group,),
            in_specs=[VMEM] * 2 + specs * 2,
            out_specs=[VMEM] * n_col,
        ),
        compiler_params=grant(18),
        cost_estimate=cost(2e9, 6 << 20),
        name="tile_sums",
    )(
        *tables, in_vmem(features), in_vmem(halo),
        *([in_hbm(own_vals)] * n_col), *([in_hbm(halo_vals)] * n_col),
    )


PAD = 16


def part_kernel(share, weight, bias, out, sem):
    part = weight.shape[0] // share
    start = lax.rem(lax.axis_index("dom"), share) * part
    src = weight.at[pl.ds(pl.multiple_of(start, part), part)]
    copy = pltpu.make_async_copy(src, out.at[pl.ds(0, part)], sem)
    copy.start()
    out[pl.ds(part, PAD), :] = jnp.broadcast_to(bias[...], (PAD, out.shape[1]))
    copy.wait()


def weight_part(weight, bias, share):
    rows = weight.shape[0] // share + PAD
    return pl.pallas_call(
        functools.partial(part_kernel, share),
        out_shape=jax.ShapeDtypeStruct((rows, weight.shape[1]), weight.dtype),
        in_specs=[RAW, VMEM],
        out_specs=VMEM,
        scratch_shapes=[pltpu.SemaphoreType.DMA],
        compiler_params=grant(4),
        cost_estimate=cost(1e8, 1 << 20),
        name="weight_part",
    )(in_hbm(weight), bias)


def pack_kernel(*refs):
    rows = refs[0].shape[0]
    for k, ref in enumerate(refs[:-1]):
        refs[-1][pl.ds(k * rows, rows), :] = ref[...]


def pack_rows(arrays):
    rows, width = arrays[0].shape
    return pl.pallas_call(
        pack_kernel,
        out_shape=jax.ShapeDtypeStruct((rows * len(arrays), width), arrays[0].dtype),
        in_specs=[VMEM] * len(arrays),
        out_specs=VMEM,
        compiler_params=grant(4),
        cost_estimate=cost(1e8, 1 << 20),
        name="pack_rows",
    )(*arrays)


def join_kernel(n_col, share, own, own_bias, *refs):
    parts = refs[:share]
    joined, bias = refs[share:]
    width = own.shape[1]
    part = own.shape[0] // share
    me = lax.rem(lax.axis_index("dom"), share)
    block = min(width, part)
    for s in range(n_col):
        for b in range(width // block):
            row = lax.rem(lax.axis_index("col") + n_col - s, n_col) * width + b * block
            row = pl.multiple_of(row, block)
            at = pl.ds(s * width + b * block, block)
            joined[0, at, :] = own[pl.ds(row, block), :]
            side = lax.div(row, part)
            offset = row - side * part
            for flip in range(share):

                @pl.when(side == me ^ flip)
                def _(flip=flip, at=at, offset=offset):
                    for k in range(1, n_col):
                        start = pl.multiple_of((k - 1) * (part + PAD) + offset, PAD)
                        joined[k, at, :] = parts[flip][pl.ds(start, block), :]

    bias[pl.ds(0, 1), :] = own_bias[...].astype(jnp.float32)
    for k in range(1, n_col):
        got = parts[0][pl.ds(k * part + (k - 1) * PAD, PAD), :].astype(jnp.float32)
        bias[pl.ds(k, 1), :] = got[:1]


def join_weights(weight, bias, parts, n_col):
    channels, width = weight.shape
    share = len(parts)
    return pl.pallas_call(
        functools.partial(join_kernel, n_col, share),
        out_shape=[
            jax.ShapeDtypeStruct((n_col, channels, width), weight.dtype),
            jax.ShapeDtypeStruct((n_col, width), jnp.float32),
        ],
        in_specs=[VMEM] * (2 + share),
        out_specs=[VMEM] * 2,
        compiler_params=grant(8),
        cost_estimate=cost(1e9, 4 << 20),
        name="join_weights",
    )(weight, bias, *parts)


def mix_kernel(n_col, channels, first, *refs):
    pieces, held, bias = refs[:n_col], refs[n_col], refs[n_col + 1]
    outs, stats = refs[-n_col - 1 : -1], refs[-1]

    @pl.when(pl.program_id(0) == 0)
    def _():
        stats[...] = jnp.zeros_like(stats) if first else refs[n_col + 2][...]

    spread = jnp.concatenate([piece[...] for piece in pieces], axis=1)
    active, power = [], 0.0
    for k in range(n_col):
        mixed = jnp.dot(spread, held[k], preferred_element_type=jnp.float32)
        mixed = jnp.maximum(mixed + bias[pl.ds(k, 1), :], 0.0)
        power = power + jnp.sum(mixed * mixed, axis=1, keepdims=True)
        active.append(mixed)
    scale = lax.rsqrt(power * (1.0 / channels) + EPS)
    for k in range(n_col):
        scaled = active[k] * scale
        outs[k][...] = scaled.astype(outs[k].dtype)
        stats[pl.ds(2 * k, 1), :] += jnp.sum(scaled, axis=0, keepdims=True)
        stats[pl.ds(2 * k + 1, 1), :] += jnp.sum(scaled * scaled, axis=0, keepdims=True)


def mix_rows(pieces, weights, bias, before):
    n_col = len(pieces)
    rows, width = pieces[0].shape
    channels = n_col * width
    block = TILE
    piece = pl.BlockSpec((block, width), lambda i: (i, 0))
    first = before is None
    out = pl.pallas_call(
        functools.partial(mix_kernel, n_col, channels, first),
        out_shape=[jax.ShapeDtypeStruct((rows, width), jnp.bfloat16)] * n_col
        + [jax.ShapeDtypeStruct((2 * n_col, width), jnp.float32)],
        grid=(rows // block,),
        in_specs=[piece] * n_col + [VMEM] * (2 if first else 3),
        out_specs=[piece] * n_col + [VMEM],
        compiler_params=grant(10),
        cost_estimate=cost(2 * rows * channels * channels, 4 << 20),
        name="mix_rows",
    )(*pieces, weights, bias, *([] if first else [before]))
    return out[:n_col], out[n_col]


def place_kernel(n_col, per_dest, base, nodes, *refs):
    pieces = refs[:n_col]
    parts = refs[n_col : 2 * n_col] if nodes else ()
    out, put = refs[-2 - bool(nodes)], refs[-1]
    rows = pieces[0].shape[0]
    stores = []
    for k in range(n_col):
        dest = lax.rem(lax.axis_index("col") + k, n_col)
        at = pl.ds(pl.multiple_of((dest * per_dest + base) * TILE, TILE), rows)
        stores.append(pltpu.make_async_copy(pieces[k], out.at[at], put.at[k]))
    for store in stores:
        store.start()
    if nodes:
        total = parts[0][...]
        for part in parts[1:]:
            total = total + part[...]
        total = total / nodes
        mean = total[0:1]
        refs[-2][pl.ds(0, 1), :] = mean
        refs[-2][pl.ds(1, 1), :] = total[1:2] - mean * mean
    for store in stores:
        store.wait()


def place_rows(pieces, out, n_rows, base, parts=(), nodes=0):
    n_col = len(pieces)
    _, width = pieces[0].shape
    per_dest = n_rows // TILE // n_col
    extra = list(parts) + ([] if out is None else [out])
    out_shape = [jax.ShapeDtypeStruct((n_rows, width), jnp.bfloat16)]
    out_specs = [HBM]
    if nodes:
        out_shape.append(jax.ShapeDtypeStruct((2, width), jnp.float32))
        out_specs.append(VMEM)
    return pl.pallas_call(
        functools.partial(place_kernel, n_col, per_dest, base, nodes),
        out_shape=out_shape,
        in_specs=[VMEM] * (n_col + len(parts)) + ([] if out is None else [HBM]),
        out_specs=out_specs,
        scratch_shapes=[pltpu.SemaphoreType.DMA((n_col,))],
        input_output_aliases={} if out is None else {n_col + len(extra) - 1: 0},
        compiler_params=grant(8),
        cost_estimate=cost(1e8, 2 << 20),
        name="place_rows",
    )(*pieces, *extra)


def chunk_plan(per_dest):
    if per_dest % 8:
        return [(0, per_dest)]
    u = per_dest // 8
    cuts = [0, u, 2 * u, 4 * u, 6 * u, 8 * u]
    return [(a, b - a) for a, b in zip(cuts, cuts[1:])]


def on_device(
    features,
    weight,
    out_bias,
    local_index,
    local_count,
    local_vals,
    halo_index,
    halo_count,
    halo_vals,
    send_rows,
    send_count,
):
    n_rows, width = features.shape
    n_dom, n_col = lax.axis_size("dom"), lax.axis_size("col")

    if n_dom & (n_dom - 1) == 0:
        peer = lambda d, k: d ^ abs(k)
    else:
        peer = lambda d, k: (d + k + n_dom) % n_dom
    along_dom = lambda x, k: lax.ppermute(x, "dom", [(i, peer(i, k)) for i in range(n_dom)])
    along_col = lambda x, k: lax.ppermute(x, "col", [(i, (i + k) % n_col) for i in range(n_col)])

    far = list(reversed(range(1, n_dom)))
    halo = [None] * (n_dom - 1)
    rows, first_row, within = storage_order(send_rows[0])
    slots = send_rows.shape[2]
    table, own_tiles = None, features
    lead = far[0:3:2]
    for part, peers in enumerate((lead, [k for k in far if k not in lead])):
        if not peers:
            continue
        outgoing, made = gather_rows(
            rows, first_row, within, send_count[0], features, table, peers, peer, slots
        )
        if made:
            table, own_tiles = made
        for k, piece in zip(peers, outgoing):
            halo[k - 1] = along_dom(piece, k)

    share = 1
    while share < min(4, n_col) and n_dom % (2 * share) == 0:
        share *= 2
    order = sorted(range(1, n_col), key=lambda k: min(k, n_col - k), reverse=True)
    bias_row = out_bias.reshape(1, width)
    mine = weight_part(weight, bias_row, share)
    arrived = {k: along_col(mine, k) for k in order}
    parts = [pack_rows([arrived[k] for k in range(1, n_col)])]
    step = share // 2
    got = {0: parts[0]}
    while step:
        swap = [(i, i ^ step) for i in range(n_dom)]
        for flip in list(got):
            got[flip ^ step] = lax.ppermute(got[flip], "dom", swap)
        step //= 2
    weights, bias = join_weights(weight, bias_row, [got[f] for f in range(share)], n_col)

    plan = chunk_plan(n_rows // TILE // n_col)
    index_tables = (local_index[0].T, local_count[0], halo_index[0].T, halo_count[0])
    part, kept = early_sums(index_tables, own_tiles, local_vals[0], halo_vals[0], n_col, plan[0][1])
    late = far[-2:-1] or far
    soon = [k for k in far if k not in late]
    received = assemble(soon, [halo[k - 1] for k in soon], n_dom, peer)
    incoming = []
    for g, (base, size) in enumerate(plan):
        if g == 0:
            sums, received = first_sums(
                index_tables[2], late, [halo[k - 1] for k in late], part, kept,
                received, n_rows // TILE // n_col, peer,
            )
        else:
            sums = tile_sums(
                index_tables, received, own_tiles, local_vals[0], halo_vals[0],
                n_col, base, size,
            )
        moved = {k: along_col(sums[k], k) for k in order}
        incoming.append([sums[0]] + [moved[k] for k in range(1, n_col)])

    stats = None
    returned = []
    for pieces in incoming:
        done, stats = mix_rows(pieces, weights, bias, stats)
        moved = {k: along_col(done[k], -k) for k in order}
        returned.append([done[0]] + [moved[k] for k in range(1, n_col)])

    over_dom = lax.all_gather(stats, "dom", axis=0)
    over_dom = over_dom.sum(axis=0)
    totals = [over_dom[:2]]
    for k in range(1, n_col):
        totals.append(along_col(over_dom[2 * k : 2 * k + 2], -k))

    out = None
    for g, ((base, _), pieces) in enumerate(zip(plan, returned)):
        if g < len(plan) - 1:
            (out,) = place_rows(pieces, out, n_rows, base)
        else:
            out, channel_stats = place_rows(
                pieces, out, n_rows, base, totals, n_rows * n_dom
            )
    return (out, channel_stats)


def solution(mesh):
    in_specs = (
        P("dom", "col"),
        P(None, "col"),
        P("col"),
        P("dom", None, None),
        P("dom", None),
        P("dom", None, None, None, None),
        P("dom", None, None),
        P("dom", None),
        P("dom", None, None, None, None),
        P("dom", None, None),
        P("dom", None),
    )
    out_specs = (P("dom", "col"), P(None, "col"))
    return jax.shard_map(
        on_device, mesh=mesh, in_specs=in_specs, out_specs=out_specs, check_vma=False
    )
```

```python
import functools

import jax
import jax.numpy as jnp
from jax import lax
from jax.experimental import pallas as pl
from jax.experimental.pallas import tpu as pltpu
from jax.sharding import PartitionSpec as P


TILE = 128
EPS = 1e-06

HBM = pl.BlockSpec(memory_space=pl.ANY)
VMEM = pl.BlockSpec(memory_space=pltpu.VMEM)
RAW = pl.BlockSpec(memory_space=pltpu.HBM)


def cost(flops, nbytes):
    return pl.CostEstimate(flops=int(flops), bytes_accessed=int(nbytes), transcendentals=0)


def in_hbm(x):
    return pltpu.with_memory_space_constraint(x, pltpu.HBM)


def in_vmem(x):
    return pltpu.with_memory_space_constraint(x, pltpu.VMEM)


def grant(mib):
    return pltpu.CompilerParams(vmem_limit_bytes=int(mib) << 20)


LANES = 128
SUBLANES = 8
UNROLL = 32


def storage_order(send_rows):
    n, slots = send_rows.shape
    if n % SUBLANES or slots % LANES:
        return send_rows.reshape(-1), lambda q: q * slots, lambda b: b * UNROLL
    blocks = slots // LANES
    tiled = send_rows.reshape(n // SUBLANES, SUBLANES, blocks, LANES)
    tile = SUBLANES * LANES
    per = LANES // UNROLL

    def first(q):
        return (q >> 3) * (blocks * tile) + (q & (SUBLANES - 1)) * LANES

    def within(b):
        return (b >> (per.bit_length() - 1)) * tile + (b & (per - 1)) * UNROLL

    return tiled.transpose(0, 2, 1, 3).reshape(-1), first, within


def widen(feat, half, table, raw, sems):
    n_rows = raw.shape[0]
    parts = sems.shape[0]
    part = n_rows // parts
    step = 128 if part % 128 == 0 else 16
    lanes = pl.ds(half * LANES, LANES)
    copies = [
        pltpu.make_async_copy(
            feat.at[pl.ds(c * part, part), lanes], raw.at[pl.ds(c * part, part)], sems.at[c]
        )
        for c in range(parts)
    ]
    for copy in copies:
        copy.start()
    for c in range(parts):
        copies[c].wait()

        def one(b, carry, c=c):
            at = pl.ds(pl.multiple_of(c * part + b * step, step), step)
            table[at, :] = raw[at, :].astype(jnp.float32)
            return carry

        lax.fori_loop(0, part // step, one, 0)


def gather_kernel(peers, peer, first_row, within, half, build, rows_in, counts_in, *refs):
    n_out = len(peers)
    outs = refs[1 : n_out + 1]
    if build:
        feat, (table, raw) = refs[0], refs[n_out + 1 : n_out + 3]
        rows, counts, index_sems, stage, sems = refs[n_out + 3 :]
    else:
        table = refs[0]
        rows, counts, index_sems, stage = refs[n_out + 1 :]
    load_rows = pltpu.make_async_copy(rows_in, rows, index_sems.at[0])
    load_counts = pltpu.make_async_copy(counts_in, counts, index_sems.at[1])
    load_rows.start()
    load_counts.start()
    if build:
        widen(feat, half, table, raw, sems)
    load_rows.wait()
    load_counts.wait()
    me = lax.axis_index("dom")
    slots = outs[0].shape[0]
    for out, k in zip(outs, peers):
        q = peer(me, k)
        used = counts[q]
        begin = first_row(q)

        def pick(b, carry, begin=begin):
            base = begin + within(b)
            put = pl.multiple_of(b * UNROLL, UNROLL)
            source = [rows[base + j] for j in range(UNROLL)]
            got = [table[pl.ds(r, 1), :] for r in source]
            for j in range(UNROLL):
                stage[pl.ds(put + j, 1), :] = got[j]
            return carry

        lax.fori_loop(0, (used + UNROLL - 1) // UNROLL, pick, 0)
        for b in range(slots // 64):
            at = pl.ds(b * 64, 64)
            slot = b * 64 + lax.broadcasted_iota(jnp.int32, (64, LANES), 0)
            out[at, :] = jnp.where(slot < used, stage[at, :], 0.0).astype(out.dtype)


def gather_rows(rows, first_row, within, send_count, features, half, table, peers, peer, slots):
    n_rows = features.shape[0]
    build = table is None
    piece = jax.ShapeDtypeStruct((slots, LANES), features.dtype)
    parts = 8 if n_rows % (8 * 16) == 0 else 1
    made = [
        jax.ShapeDtypeStruct((n_rows, LANES), jnp.float32),
        jax.ShapeDtypeStruct((n_rows, LANES), features.dtype),
    ]
    out = pl.pallas_call(
        functools.partial(gather_kernel, peers, peer, first_row, within, half, build),
        out_shape=[piece] * len(peers) + made * build,
        in_specs=[RAW, RAW, RAW if build else VMEM],
        out_specs=[VMEM] * (len(peers) + 2 * build),
        scratch_shapes=[
            pltpu.SMEM(rows.shape, jnp.int32),
            pltpu.SMEM(send_count.shape, jnp.int32),
            pltpu.SemaphoreType.DMA((2,)),
            pltpu.VMEM((slots, LANES), jnp.float32),
        ]
        + [pltpu.SemaphoreType.DMA((parts,))] * build,
        compiler_params=grant(10 + len(peers) if build else 4),
        cost_estimate=cost(4e9, 6 << 20),
        name="gather_rows",
    )(in_hbm(rows), in_hbm(send_count), in_hbm(features) if build else table)
    return out[: len(peers)], out[len(peers) :]


def masked(vals, used):
    return [
        jnp.where(s < used, vals[s], jnp.zeros_like(vals[s])) for s in range(vals.shape[0])
    ]


def tiles_of(src, index, row_tile, slots):
    starts = [pl.multiple_of(index[s, row_tile] * TILE, TILE) for s in range(slots)]
    return [src[pl.ds(at, TILE), :] for at in starts]


def product(left, right):
    return jnp.dot(
        jnp.concatenate(left, axis=1),
        jnp.concatenate(right, axis=0),
        preferred_element_type=jnp.float32,
    )


def vals_specs(n_col, per_dest, base, group, slots):
    def spec(k):
        def place(i, *_):
            dest = lax.rem(lax.axis_index("col") + k, n_col)
            return ((dest * per_dest + base) // group + i, 0, 0, 0)

        return pl.BlockSpec((group, slots, TILE, TILE), place)

    return [spec(k) for k in range(n_col)]


def row_tile_of(k, n_col, per_dest, tile):
    return lax.rem(lax.axis_index("col") + k, n_col) * per_dest + tile


def early_kernel(n_col, slots, per_dest, own_index, own_counts, halo_counts, feat, *refs):
    own_vals, halo_vals, (part, kept) = refs[:n_col], refs[n_col:-2], refs[-2:]
    i = pl.program_id(0)
    for k in range(n_col):
        row_tile = row_tile_of(k, n_col, per_dest, i)
        part[k, pl.ds(pl.multiple_of(i * TILE, TILE), TILE), :] = product(
            masked(own_vals[k][0], own_counts[row_tile]),
            tiles_of(feat, own_index, row_tile, slots),
        )
        for s, vals in enumerate(masked(halo_vals[k][0], halo_counts[row_tile])):
            kept[k, i, s] = vals


def early_sums(tables, features, own_vals, halo_vals, n_col, size):
    tiles, slots = own_vals.shape[:2]
    width = features.shape[1]
    per_dest = tiles // n_col
    own_index, own_counts, _, halo_counts = tables
    return pl.pallas_call(
        functools.partial(early_kernel, n_col, slots, per_dest),
        out_shape=[
            jax.ShapeDtypeStruct((n_col, size * TILE, width), jnp.float32),
            jax.ShapeDtypeStruct((n_col, size, slots, TILE, TILE), halo_vals.dtype),
        ],
        grid_spec=pltpu.PrefetchScalarGridSpec(
            num_scalar_prefetch=3,
            grid=(size,),
            in_specs=[VMEM] + vals_specs(n_col, per_dest, 0, 1, slots) * 2,
            out_specs=[VMEM] * 2,
        ),
        compiler_params=grant(16),
        cost_estimate=cost(2e9, 4 << 20),
        name="early_sums",
    )(
        own_index, own_counts, halo_counts, in_vmem(features),
        *([in_hbm(own_vals)] * n_col), *([in_hbm(halo_vals)] * n_col),
    )


def put_piece(halo, piece, q):
    rows = piece.shape[0]
    halo[pl.ds(pl.multiple_of(q * rows, rows), rows), :] = piece[...]


def assemble_kernel(ks, peer, *refs):
    pieces, halo = refs[:-1], refs[-1]
    me = lax.axis_index("dom")
    for k, piece in zip(ks, pieces):
        put_piece(halo, piece, peer(me, -k))
    rows = pieces[0].shape[0]
    own = pl.ds(pl.multiple_of(me * rows, rows), rows)
    halo[own, :] = jnp.zeros((rows, halo.shape[1]), halo.dtype)


def assemble(ks, pieces, n_dom, peer):
    rows, width = pieces[0].shape
    return pl.pallas_call(
        functools.partial(assemble_kernel, ks, peer),
        out_shape=jax.ShapeDtypeStruct((n_dom * rows, width), pieces[0].dtype),
        in_specs=[VMEM] * len(pieces),
        out_specs=VMEM,
        compiler_params=grant(4 + n_dom),
        cost_estimate=cost(2e9, 4 << 20),
        name="assemble",
    )(*pieces)


def first_kernel(n_col, slots, per_dest, ks, peer, index, *refs):
    pieces = refs[: len(ks)]
    part, kept = refs[len(ks) : len(ks) + 2]
    outs, halo = refs[-n_col - 1 : -1], refs[-1]
    me = lax.axis_index("dom")
    for k, piece in zip(ks, pieces):
        put_piece(halo, piece, peer(me, -k))
    for t in range(kept.shape[1]):
        at = pl.ds(t * TILE, TILE)
        for k in range(n_col):
            right = tiles_of(halo, index, row_tile_of(k, n_col, per_dest, t), slots)
            total = part[k, at, :] + product([kept[k, t, s] for s in range(slots)], right)
            outs[k][at, :] = total.astype(outs[k].dtype)


def first_sums(index, ks, pieces, part, kept, halo, per_dest, peer):
    n_col, size, slots = kept.shape[:3]
    width = halo.shape[1]
    out = pl.pallas_call(
        functools.partial(first_kernel, n_col, slots, per_dest, ks, peer),
        out_shape=[jax.ShapeDtypeStruct((size * TILE, width), halo.dtype)] * n_col
        + [jax.ShapeDtypeStruct(halo.shape, halo.dtype)],
        in_specs=[pl.BlockSpec(memory_space=pltpu.SMEM)] + [VMEM] * (len(ks) + 3),
        out_specs=[VMEM] * (n_col + 1),
        input_output_aliases={len(ks) + 3: n_col},
        compiler_params=grant(6 + halo.shape[0] // (1 << 12)),
        cost_estimate=cost(2e9, 4 << 20),
        name="first_sums",
    )(index, *pieces, part, kept, halo)
    return out[:n_col], out[n_col]


def sum_kernel(n_col, slots, per_dest, base, *refs):
    own_index, own_counts, halo_index, halo_counts, feat, halo = refs[:6]
    own_vals, halo_vals = refs[6 : 6 + n_col], refs[6 + n_col : 6 + 2 * n_col]
    outs = refs[6 + 2 * n_col :]
    sub = pl.program_id(0)
    group = own_vals[0].shape[0]
    for k in range(n_col):
        for t in range(group):
            row_tile = row_tile_of(k, n_col, per_dest, base + sub * group + t)
            left = masked(own_vals[k][t], own_counts[row_tile])
            left += masked(halo_vals[k][t], halo_counts[row_tile])
            right = tiles_of(feat, own_index, row_tile, slots)
            right += tiles_of(halo, halo_index, row_tile, slots)
            at = pl.ds(pl.multiple_of((sub * group + t) * TILE, TILE), TILE)
            outs[k][at, :] = product(left, right).astype(outs[k].dtype)


def tile_sums(tables, halo, features, own_vals, halo_vals, n_col, base, size):
    tiles, slots = own_vals.shape[:2]
    width = features.shape[1]
    per_dest = tiles // n_col
    group = min(size, 2)
    while base % group or size % group:
        group -= 1
    specs = vals_specs(n_col, per_dest, base, group, slots)
    return pl.pallas_call(
        functools.partial(sum_kernel, n_col, slots, per_dest, base),
        out_shape=[jax.ShapeDtypeStruct((size * TILE, width), jnp.bfloat16)] * n_col,
        grid_spec=pltpu.PrefetchScalarGridSpec(
            num_scalar_prefetch=4,
            grid=(size // group,),
            in_specs=[VMEM] * 2 + specs * 2,
            out_specs=[VMEM] * n_col,
        ),
        compiler_params=grant(18),
        cost_estimate=cost(2e9, 6 << 20),
        name="tile_sums",
    )(
        *tables, in_vmem(features), in_vmem(halo),
        *([in_hbm(own_vals)] * n_col), *([in_hbm(halo_vals)] * n_col),
    )


PAD = 16


def part_kernel(share, weight, bias, out, sem):
    part = weight.shape[0] // share
    start = lax.rem(lax.axis_index("dom"), share) * part
    src = weight.at[pl.ds(pl.multiple_of(start, part), part)]
    copy = pltpu.make_async_copy(src, out.at[pl.ds(0, part)], sem)
    copy.start()
    out[pl.ds(part, PAD), :] = jnp.broadcast_to(bias[...], (PAD, out.shape[1]))
    copy.wait()


def weight_part(weight, bias, share):
    rows = weight.shape[0] // share + PAD
    return pl.pallas_call(
        functools.partial(part_kernel, share),
        out_shape=jax.ShapeDtypeStruct((rows, weight.shape[1]), weight.dtype),
        in_specs=[RAW, VMEM],
        out_specs=VMEM,
        scratch_shapes=[pltpu.SemaphoreType.DMA],
        compiler_params=grant(4),
        cost_estimate=cost(1e8, 1 << 20),
        name="weight_part",
    )(in_hbm(weight), bias)


def pack_kernel(*refs):
    rows = refs[0].shape[0]
    for k, ref in enumerate(refs[:-1]):
        refs[-1][pl.ds(k * rows, rows), :] = ref[...]


def pack_rows(arrays):
    rows, width = arrays[0].shape
    return pl.pallas_call(
        pack_kernel,
        out_shape=jax.ShapeDtypeStruct((rows * len(arrays), width), arrays[0].dtype),
        in_specs=[VMEM] * len(arrays),
        out_specs=VMEM,
        compiler_params=grant(4),
        cost_estimate=cost(1e8, 1 << 20),
        name="pack_rows",
    )(*arrays)


def join_kernel(n_col, share, own, own_bias, *refs):
    parts = refs[:share]
    joined, bias = refs[share:]
    width = own.shape[1]
    part = own.shape[0] // share
    me = lax.rem(lax.axis_index("dom"), share)
    block = min(width, part)
    for s in range(n_col):
        for b in range(width // block):
            row = lax.rem(lax.axis_index("col") + n_col - s, n_col) * width + b * block
            row = pl.multiple_of(row, block)
            at = pl.ds(s * width + b * block, block)
            joined[0, at, :] = own[pl.ds(row, block), :]
            side = lax.div(row, part)
            offset = row - side * part
            for flip in range(share):

                @pl.when(side == me ^ flip)
                def _(flip=flip, at=at, offset=offset):
                    for k in range(1, n_col):
                        start = pl.multiple_of((k - 1) * (part + PAD) + offset, PAD)
                        joined[k, at, :] = parts[flip][pl.ds(start, block), :]

    bias[pl.ds(0, 1), :] = own_bias[...].astype(jnp.float32)
    for k in range(1, n_col):
        got = parts[0][pl.ds(k * part + (k - 1) * PAD, PAD), :].astype(jnp.float32)
        bias[pl.ds(k, 1), :] = got[:1]


def join_weights(weight, bias, parts, n_col):
    channels, width = weight.shape
    share = len(parts)
    return pl.pallas_call(
        functools.partial(join_kernel, n_col, share),
        out_shape=[
            jax.ShapeDtypeStruct((n_col, channels, width), weight.dtype),
            jax.ShapeDtypeStruct((n_col, width), jnp.float32),
        ],
        in_specs=[VMEM] * (2 + share),
        out_specs=[VMEM] * 2,
        compiler_params=grant(8),
        cost_estimate=cost(1e9, 4 << 20),
        name="join_weights",
    )(weight, bias, *parts)


def mix_kernel(n_col, n_in, channels, first, *refs):
    pieces, held, bias = refs[:n_in], refs[n_in], refs[n_in + 1]
    outs, stats = refs[-n_col - 1 : -1], refs[-1]

    @pl.when(pl.program_id(0) == 0)
    def _():
        stats[...] = jnp.zeros_like(stats) if first else refs[n_in + 2][...]

    spread = jnp.concatenate([piece[...] for piece in pieces], axis=1)
    active, power = [], 0.0
    for k in range(n_col):
        mixed = jnp.dot(spread, held[k], preferred_element_type=jnp.float32)
        mixed = jnp.maximum(mixed + bias[pl.ds(k, 1), :], 0.0)
        power = power + jnp.sum(mixed * mixed, axis=1, keepdims=True)
        active.append(mixed)
    scale = lax.rsqrt(power * (1.0 / channels) + EPS)
    for k in range(n_col):
        scaled = active[k] * scale
        outs[k][...] = scaled.astype(outs[k].dtype)
        stats[pl.ds(2 * k, 1), :] += jnp.sum(scaled, axis=0, keepdims=True)
        stats[pl.ds(2 * k + 1, 1), :] += jnp.sum(scaled * scaled, axis=0, keepdims=True)


def mix_rows(pieces, weights, bias, before):
    n_col, channels, width = weights.shape
    rows = pieces[0].shape[0]
    block = TILE
    spec = lambda w: pl.BlockSpec((block, w), lambda i: (i, 0))
    first = before is None
    out = pl.pallas_call(
        functools.partial(mix_kernel, n_col, len(pieces), channels, first),
        out_shape=[jax.ShapeDtypeStruct((rows, width), jnp.bfloat16)] * n_col
        + [jax.ShapeDtypeStruct((2 * n_col, width), jnp.float32)],
        grid=(rows // block,),
        in_specs=[spec(piece.shape[1]) for piece in pieces] + [VMEM] * (2 if first else 3),
        out_specs=[spec(width)] * n_col + [VMEM],
        compiler_params=grant(10),
        cost_estimate=cost(2 * rows * channels * channels, 4 << 20),
        name="mix_rows",
    )(*pieces, weights, bias, *([] if first else [before]))
    return out[:n_col], out[n_col]


def place_kernel(n_col, per_dest, base, nodes, *refs):
    pieces = refs[:n_col]
    parts = refs[n_col : 2 * n_col] if nodes else ()
    out, put = refs[-2 - bool(nodes)], refs[-1]
    rows = pieces[0].shape[0]
    stores = []
    for k in range(n_col):
        dest = lax.rem(lax.axis_index("col") + k, n_col)
        at = pl.ds(pl.multiple_of((dest * per_dest + base) * TILE, TILE), rows)
        stores.append(pltpu.make_async_copy(pieces[k], out.at[at], put.at[k]))
    for store in stores:
        store.start()
    if nodes:
        total = parts[0][...]
        for part in parts[1:]:
            total = total + part[...]
        total = total / nodes
        mean = total[0:1]
        refs[-2][pl.ds(0, 1), :] = mean
        refs[-2][pl.ds(1, 1), :] = total[1:2] - mean * mean
    for store in stores:
        store.wait()


def place_rows(pieces, out, n_rows, base, parts=(), nodes=0):
    n_col = len(pieces)
    _, width = pieces[0].shape
    per_dest = n_rows // TILE // n_col
    extra = list(parts) + ([] if out is None else [out])
    out_shape = [jax.ShapeDtypeStruct((n_rows, width), jnp.bfloat16)]
    out_specs = [HBM]
    if nodes:
        out_shape.append(jax.ShapeDtypeStruct((2, width), jnp.float32))
        out_specs.append(VMEM)
    return pl.pallas_call(
        functools.partial(place_kernel, n_col, per_dest, base, nodes),
        out_shape=out_shape,
        in_specs=[VMEM] * (n_col + len(parts)) + ([] if out is None else [HBM]),
        out_specs=out_specs,
        scratch_shapes=[pltpu.SemaphoreType.DMA((n_col,))],
        input_output_aliases={} if out is None else {n_col + len(extra) - 1: 0},
        compiler_params=grant(8),
        cost_estimate=cost(1e8, 2 << 20),
        name="place_rows",
    )(*pieces, *extra)


def chunk_plan(per_dest):
    if per_dest % 4:
        return [(0, per_dest)]
    u = per_dest // 4
    return [(0, u), (u, u), (2 * u, u), (3 * u, u)]


def on_device(
    features,
    weight,
    out_bias,
    local_index,
    local_count,
    local_vals,
    halo_index,
    halo_count,
    halo_vals,
    send_rows,
    send_count,
):
    n_rows, width = features.shape
    n_dom, n_col = lax.axis_size("dom"), lax.axis_size("col")

    if n_dom & (n_dom - 1) == 0:
        peer = lambda d, k: d ^ abs(k)
    else:
        peer = lambda d, k: (d + k + n_dom) % n_dom
    along_dom = lambda x, k: lax.ppermute(x, "dom", [(i, peer(i, k)) for i in range(n_dom)])
    along_col = lambda x, k: lax.ppermute(x, "col", [(i, (i + k) % n_col) for i in range(n_col)])

    far = list(reversed(range(1, n_dom)))
    lead = far[0:3:2]
    rest = [k for k in far if k not in lead]
    rows, first_row, within = storage_order(send_rows[0])
    slots = send_rows.shape[2]
    halves = width // LANES
    halo, own_tiles = [], []
    for h in range(halves):
        pieces, table = {}, None
        for peers in [lead, rest] if h == 0 else [lead + rest]:
            if not peers:
                continue
            outgoing, made = gather_rows(
                rows, first_row, within, send_count[0], features, h, table, peers, peer, slots
            )
            if made:
                table, tiles = made
            for k, piece in zip(peers, outgoing):
                pieces[k] = along_dom(piece, k)
        halo.append(pieces)
        own_tiles.append(tiles)

    share = 1
    channels = n_col * width
    while share < 8 and n_dom % (2 * share) == 0 and channels % (2 * share * PAD) == 0:
        share *= 2
    order = sorted(range(1, n_col), key=lambda k: min(k, n_col - k), reverse=True)
    bias_row = out_bias.reshape(1, width)
    mine = weight_part(weight, bias_row, share)
    arrived = {k: along_col(mine, k) for k in order}
    parts = [pack_rows([arrived[k] for k in range(1, n_col)])]
    step = share // 2
    got = {0: parts[0]}
    while step:
        swap = [(i, i ^ step) for i in range(n_dom)]
        for flip in list(got):
            got[flip ^ step] = lax.ppermute(got[flip], "dom", swap)
        step //= 2
    weights, bias = join_weights(weight, bias_row, [got[f] for f in range(share)], n_col)

    per_dest = n_rows // TILE // n_col
    plan = chunk_plan(per_dest)
    index_tables = (local_index[0].T, local_count[0], halo_index[0].T, halo_count[0])
    part, kept = early_sums(
        index_tables, own_tiles[0], local_vals[0], halo_vals[0], n_col, plan[0][1]
    )
    late = far[-2:-1] or far
    incoming = [[[] for _ in range(n_col)] for _ in plan]
    for h in range(halves):
        soon = [k for k in far if h or k not in late]
        received = assemble(soon, [halo[h][k] for k in soon], n_dom, peer)
        for g, (base, size) in enumerate(plan):
            if g == h == 0:
                sums, received = first_sums(
                    index_tables[2], late, [halo[h][k] for k in late], part, kept,
                    received, per_dest, peer,
                )
            else:
                sums = tile_sums(
                    index_tables, received, own_tiles[h], local_vals[0], halo_vals[0],
                    n_col, base, size,
                )
            moved = {k: along_col(sums[k], k) for k in order}
            for k in range(n_col):
                incoming[g][k].append(moved[k] if k else sums[0])

    stats = None
    returned = []
    for pieces in incoming:
        done, stats = mix_rows(sum(pieces, []), weights, bias, stats)
        moved = {k: along_col(done[k], -k) for k in order}
        returned.append([done[0]] + [moved[k] for k in range(1, n_col)])

    over_dom = lax.all_gather(stats, "dom", axis=0)
    over_dom = over_dom.sum(axis=0)
    totals = [over_dom[:2]]
    for k in range(1, n_col):
        totals.append(along_col(over_dom[2 * k : 2 * k + 2], -k))

    out = None
    for g, ((base, _), pieces) in enumerate(zip(plan, returned)):
        if g < len(plan) - 1:
            (out,) = place_rows(pieces, out, n_rows, base)
        else:
            out, channel_stats = place_rows(
                pieces, out, n_rows, base, totals, n_rows * n_dom
            )
    return (out, channel_stats)


def solution(mesh):
    in_specs = (
        P("dom", "col"),
        P(None, "col"),
        P("col"),
        P("dom", None, None),
        P("dom", None),
        P("dom", None, None, None, None),
        P("dom", None, None),
        P("dom", None),
        P("dom", None, None, None, None),
        P("dom", None, None),
        P("dom", None),
    )
    out_specs = (P("dom", "col"), P(None, "col"))
    return jax.shard_map(
        on_device, mesh=mesh, in_specs=in_specs, out_specs=out_specs, check_vma=False
    )
```

```python
import functools

import jax
import jax.numpy as jnp
from jax import lax
from jax.experimental import pallas as pl
from jax.experimental.pallas import tpu as pltpu
from jax.sharding import PartitionSpec as P


TILE = 128
EPS = 1e-06

HBM = pl.BlockSpec(memory_space=pl.ANY)
VMEM = pl.BlockSpec(memory_space=pltpu.VMEM)
RAW = pl.BlockSpec(memory_space=pltpu.HBM)


def cost(flops, nbytes):
    return pl.CostEstimate(flops=int(flops), bytes_accessed=int(nbytes), transcendentals=0)


def in_hbm(x):
    return pltpu.with_memory_space_constraint(x, pltpu.HBM)


def in_vmem(x):
    return pltpu.with_memory_space_constraint(x, pltpu.VMEM)


def grant(mib):
    return pltpu.CompilerParams(vmem_limit_bytes=int(mib) << 20)


LANES = 128
SUBLANES = 8
UNROLL = 32


def storage_order(send_rows):
    n, slots = send_rows.shape
    if n % SUBLANES or slots % LANES:
        return send_rows.reshape(-1), lambda q: q * slots, lambda b: b * UNROLL
    blocks = slots // LANES
    tiled = send_rows.reshape(n // SUBLANES, SUBLANES, blocks, LANES)
    tile = SUBLANES * LANES
    per = LANES // UNROLL

    def first(q):
        return (q >> 3) * (blocks * tile) + (q & (SUBLANES - 1)) * LANES

    def within(b):
        return (b >> (per.bit_length() - 1)) * tile + (b & (per - 1)) * UNROLL

    return tiled.transpose(0, 2, 1, 3).reshape(-1), first, within


def widen(feat, half, table, raw, sems):
    n_rows = raw.shape[0]
    parts = sems.shape[0]
    part = n_rows // parts
    step = 128 if part % 128 == 0 else 16
    lanes = pl.ds(half * LANES, LANES)
    copies = [
        pltpu.make_async_copy(
            feat.at[pl.ds(c * part, part), lanes], raw.at[pl.ds(c * part, part)], sems.at[c]
        )
        for c in range(parts)
    ]
    for copy in copies:
        copy.start()
    for c in range(parts):
        copies[c].wait()

        def one(b, carry, c=c):
            at = pl.ds(pl.multiple_of(c * part + b * step, step), step)
            table[at, :] = raw[at, :].astype(jnp.float32)
            return carry

        lax.fori_loop(0, part // step, one, 0)


def gather_kernel(peers, peer, first_row, within, half, build, ahead, rows_in, counts_in, *refs):
    n_out = len(peers)
    refs = list(refs)
    source = refs.pop(0)
    vals = [refs.pop(0) for _ in range(2 * bool(ahead))]
    outs, refs = refs[:n_out], refs[n_out:]
    if build:
        feat, table, raw = source, refs.pop(0), refs.pop(0)
    else:
        table = source
    block = refs.pop(0) if ahead else None
    rows, counts, index_sems, stage = refs[:4]
    loads = block_copies(vals, block, refs[-1], *ahead) if ahead else []
    for load in loads:
        load.start()
    load_rows = pltpu.make_async_copy(rows_in, rows, index_sems.at[0])
    load_counts = pltpu.make_async_copy(counts_in, counts, index_sems.at[1])
    load_rows.start()
    load_counts.start()
    if build:
        widen(feat, half, table, raw, refs[4])
    load_rows.wait()
    load_counts.wait()
    me = lax.axis_index("dom")
    slots = outs[0].shape[0]
    for out, k in zip(outs, peers):
        q = peer(me, k)
        used = counts[q]
        begin = first_row(q)

        def pick(b, carry, begin=begin):
            base = begin + within(b)
            put = pl.multiple_of(b * UNROLL, UNROLL)
            source = [rows[base + j] for j in range(UNROLL)]
            got = [table[pl.ds(r, 1), :] for r in source]
            for j in range(UNROLL):
                stage[pl.ds(put + j, 1), :] = got[j]
            return carry

        lax.fori_loop(0, (used + UNROLL - 1) // UNROLL, pick, 0)
        for b in range(slots // 64):
            at = pl.ds(b * 64, 64)
            slot = b * 64 + lax.broadcasted_iota(jnp.int32, (64, LANES), 0)
            out[at, :] = jnp.where(slot < used, stage[at, :], 0.0).astype(out.dtype)
    for load in loads:
        load.wait()


def gather_rows(
    rows, first_row, within, send_count, features, half, table, peers, peer, slots, vals, ahead
):
    n_rows = features.shape[0]
    build = table is None
    piece = jax.ShapeDtypeStruct((slots, LANES), features.dtype)
    parts = 8 if n_rows % (8 * 16) == 0 else 1
    made = [
        jax.ShapeDtypeStruct((n_rows, LANES), jnp.float32),
        jax.ShapeDtypeStruct((n_rows, LANES), features.dtype),
    ]
    block = [block_shape(vals[0], *ahead)] if ahead else []
    out = pl.pallas_call(
        functools.partial(gather_kernel, peers, peer, first_row, within, half, build, ahead),
        out_shape=[piece] * len(peers) + made * build + block,
        in_specs=[RAW, RAW, RAW if build else VMEM] + [RAW] * (2 * len(block)),
        out_specs=[VMEM] * (len(peers) + 2 * build + len(block)),
        scratch_shapes=[
            pltpu.SMEM(rows.shape, jnp.int32),
            pltpu.SMEM(send_count.shape, jnp.int32),
            pltpu.SemaphoreType.DMA((2,)),
            pltpu.VMEM((slots, LANES), jnp.float32),
        ]
        + [pltpu.SemaphoreType.DMA((parts,))] * build
        + [pltpu.SemaphoreType.DMA((2 * cols[0],)) for cols in [ahead] if ahead],
        compiler_params=grant(10 + len(peers) if build else 8),
        cost_estimate=cost(4e9, 6 << 20),
        name="gather_rows",
    )(
        in_hbm(rows), in_hbm(send_count), in_hbm(features) if build else table,
        *([in_hbm(v) for v in vals] * len(block)),
    )
    n_out = len(peers)
    return out[:n_out], out[n_out : n_out + 2 * build], out[n_out + 2 * build :]


def masked(vals, used):
    return [
        jnp.where(s < used, vals[s], jnp.zeros_like(vals[s])) for s in range(vals.shape[0])
    ]


def tiles_of(src, index, row_tile, slots):
    starts = [pl.multiple_of(index[s, row_tile] * TILE, TILE) for s in range(slots)]
    return [src[pl.ds(at, TILE), :] for at in starts]


def product(left, right):
    return jnp.dot(
        jnp.concatenate(left, axis=1),
        jnp.concatenate(right, axis=0),
        preferred_element_type=jnp.float32,
    )


def row_tile_of(k, n_col, per_dest, tile):
    return lax.rem(lax.axis_index("col") + k, n_col) * per_dest + tile


def block_shape(vals, n_col, per_dest, base, size):
    return jax.ShapeDtypeStruct((n_col, 2, size) + vals.shape[1:], vals.dtype)


def block_copies(vals, block, sems, n_col, per_dest, base, size):
    copies = []
    for k in range(n_col):
        at = pl.ds(row_tile_of(k, n_col, per_dest, base), size)
        for v in range(2):
            copies.append(
                pltpu.make_async_copy(vals[v].at[at], block.at[k, v], sems.at[2 * k + v])
            )
    return copies


def put_piece(halo, piece, q):
    rows = piece.shape[0]
    halo[pl.ds(pl.multiple_of(q * rows, rows), rows), :] = piece[...]


def assemble_kernel(ks, peer, *refs):
    pieces, halo = refs[:-1], refs[-1]
    me = lax.axis_index("dom")
    for k, piece in zip(ks, pieces):
        put_piece(halo, piece, peer(me, -k))
    rows = pieces[0].shape[0]
    own = pl.ds(pl.multiple_of(me * rows, rows), rows)
    halo[own, :] = jnp.zeros((rows, halo.shape[1]), halo.dtype)


def assemble(ks, pieces, n_dom, peer):
    rows, width = pieces[0].shape
    return pl.pallas_call(
        functools.partial(assemble_kernel, ks, peer),
        out_shape=jax.ShapeDtypeStruct((n_dom * rows, width), pieces[0].dtype),
        in_specs=[VMEM] * len(pieces),
        out_specs=VMEM,
        compiler_params=grant(4 + n_dom),
        cost_estimate=cost(2e9, 4 << 20),
        name="assemble",
    )(*pieces)


def sum_kernel(n_col, slots, per_dest, base, ahead, *refs):
    own_index, own_counts, halo_index, halo_counts, feat, halo, block = refs[:7]
    refs = refs[7:]
    loads = []
    if ahead:
        loads = block_copies(refs[:2], refs[2 + n_col], refs[-1], *ahead)
        refs = refs[2:]
    outs = refs[:n_col]
    for load in loads:
        load.start()

    def one(t, carry):
        for k in range(n_col):
            row_tile = row_tile_of(k, n_col, per_dest, base + t)
            left = masked(block.at[k, 0, t], own_counts[row_tile])
            left += masked(block.at[k, 1, t], halo_counts[row_tile])
            right = tiles_of(feat, own_index, row_tile, slots)
            right += tiles_of(halo, halo_index, row_tile, slots)
            at = pl.ds(pl.multiple_of(t * TILE, TILE), TILE)
            outs[k][at, :] = product(left, right).astype(outs[k].dtype)
        return carry

    lax.fori_loop(0, block.shape[2], one, 0)
    for load in loads:
        load.wait()


def tile_sums(tables, halo, features, block, vals, per_dest, base, ahead):
    n_col, _, size, slots = block.shape[:4]
    width = features.shape[1]
    made = [block_shape(vals[0], *ahead)] if ahead else []
    smem = pl.BlockSpec(memory_space=pltpu.SMEM)
    out = pl.pallas_call(
        functools.partial(sum_kernel, n_col, slots, per_dest, base, ahead),
        out_shape=[jax.ShapeDtypeStruct((size * TILE, width), jnp.bfloat16)] * n_col + made,
        grid_spec=pltpu.PrefetchScalarGridSpec(
            num_scalar_prefetch=4,
            grid=(1,),
            in_specs=[VMEM] * 3 + [RAW] * (2 * len(made)),
            out_specs=[VMEM] * (n_col + len(made)),
            scratch_shapes=[pltpu.SemaphoreType.DMA((2 * n_col,))] * len(made),
        ),
        compiler_params=grant(8),
        cost_estimate=cost(2e9, 6 << 20),
        name="tile_sums",
    )(
        *tables, in_vmem(features), in_vmem(halo), in_vmem(block),
        *([in_hbm(v) for v in vals] * len(made)),
    )
    return out[:n_col], out[n_col:]


PAD = 16


def part_kernel(share, weight, bias, out, sem):
    part = weight.shape[0] // share
    start = lax.rem(lax.axis_index("dom"), share) * part
    src = weight.at[pl.ds(pl.multiple_of(start, part), part)]
    copy = pltpu.make_async_copy(src, out.at[pl.ds(0, part)], sem)
    copy.start()
    out[pl.ds(part, PAD), :] = jnp.broadcast_to(bias[...], (PAD, out.shape[1]))
    copy.wait()


def weight_part(weight, bias, share):
    rows = weight.shape[0] // share + PAD
    return pl.pallas_call(
        functools.partial(part_kernel, share),
        out_shape=jax.ShapeDtypeStruct((rows, weight.shape[1]), weight.dtype),
        in_specs=[RAW, VMEM],
        out_specs=VMEM,
        scratch_shapes=[pltpu.SemaphoreType.DMA],
        compiler_params=grant(4),
        cost_estimate=cost(1e8, 1 << 20),
        name="weight_part",
    )(in_hbm(weight), bias)


def pack_kernel(*refs):
    rows = refs[0].shape[0]
    for k, ref in enumerate(refs[:-1]):
        refs[-1][pl.ds(k * rows, rows), :] = ref[...]


def pack_rows(arrays):
    rows, width = arrays[0].shape
    return pl.pallas_call(
        pack_kernel,
        out_shape=jax.ShapeDtypeStruct((rows * len(arrays), width), arrays[0].dtype),
        in_specs=[VMEM] * len(arrays),
        out_specs=VMEM,
        compiler_params=grant(4),
        cost_estimate=cost(1e8, 1 << 20),
        name="pack_rows",
    )(*arrays)


def join_kernel(n_col, share, own, own_bias, *refs):
    parts = refs[:share]
    joined, bias = refs[share:]
    width = own.shape[1]
    part = own.shape[0] // share
    me = lax.rem(lax.axis_index("dom"), share)
    block = min(width, part)
    for s in range(n_col):
        for b in range(width // block):
            row = lax.rem(lax.axis_index("col") + n_col - s, n_col) * width + b * block
            row = pl.multiple_of(row, block)
            at = pl.ds(s * width + b * block, block)
            joined[0, at, :] = own[pl.ds(row, block), :]
            side = lax.div(row, part)
            offset = row - side * part
            for flip in range(share):

                @pl.when(side == me ^ flip)
                def _(flip=flip, at=at, offset=offset):
                    for k in range(1, n_col):
                        start = pl.multiple_of((k - 1) * (part + PAD) + offset, PAD)
                        joined[k, at, :] = parts[flip][pl.ds(start, block), :]

    bias[pl.ds(0, 1), :] = own_bias[...].astype(jnp.float32)
    for k in range(1, n_col):
        got = parts[0][pl.ds(k * part + (k - 1) * PAD, PAD), :].astype(jnp.float32)
        bias[pl.ds(k, 1), :] = got[:1]


def join_weights(weight, bias, parts, n_col):
    channels, width = weight.shape
    share = len(parts)
    return pl.pallas_call(
        functools.partial(join_kernel, n_col, share),
        out_shape=[
            jax.ShapeDtypeStruct((n_col, channels, width), weight.dtype),
            jax.ShapeDtypeStruct((n_col, width), jnp.float32),
        ],
        in_specs=[VMEM] * (2 + share),
        out_specs=[VMEM] * 2,
        compiler_params=grant(8),
        cost_estimate=cost(1e9, 4 << 20),
        name="join_weights",
    )(weight, bias, *parts)


def mix_kernel(n_col, n_in, channels, first, *refs):
    pieces, held, bias = refs[:n_in], refs[n_in], refs[n_in + 1]
    outs, stats = refs[-n_col - 1 : -1], refs[-1]

    @pl.when(pl.program_id(0) == 0)
    def _():
        stats[...] = jnp.zeros_like(stats) if first else refs[n_in + 2][...]

    spread = jnp.concatenate([piece[...] for piece in pieces], axis=1)
    active, power = [], 0.0
    for k in range(n_col):
        mixed = jnp.dot(spread, held[k], preferred_element_type=jnp.float32)
        mixed = jnp.maximum(mixed + bias[pl.ds(k, 1), :], 0.0)
        power = power + jnp.sum(mixed * mixed, axis=1, keepdims=True)
        active.append(mixed)
    scale = lax.rsqrt(power * (1.0 / channels) + EPS)
    for k in range(n_col):
        scaled = active[k] * scale
        outs[k][...] = scaled.astype(outs[k].dtype)
        stats[pl.ds(2 * k, 1), :] += jnp.sum(scaled, axis=0, keepdims=True)
        stats[pl.ds(2 * k + 1, 1), :] += jnp.sum(scaled * scaled, axis=0, keepdims=True)


def mix_rows(pieces, weights, bias, before):
    n_col, channels, width = weights.shape
    rows = pieces[0].shape[0]
    block = TILE
    spec = lambda w: pl.BlockSpec((block, w), lambda i: (i, 0))
    first = before is None
    out = pl.pallas_call(
        functools.partial(mix_kernel, n_col, len(pieces), channels, first),
        out_shape=[jax.ShapeDtypeStruct((rows, width), jnp.bfloat16)] * n_col
        + [jax.ShapeDtypeStruct((2 * n_col, width), jnp.float32)],
        grid=(rows // block,),
        in_specs=[spec(piece.shape[1]) for piece in pieces] + [VMEM] * (2 if first else 3),
        out_specs=[spec(width)] * n_col + [VMEM],
        compiler_params=grant(10),
        cost_estimate=cost(2 * rows * channels * channels, 4 << 20),
        name="mix_rows",
    )(*pieces, weights, bias, *([] if first else [before]))
    return out[:n_col], out[n_col]


def place_kernel(n_col, per_dest, base, nodes, *refs):
    pieces = refs[:n_col]
    parts = refs[n_col : 2 * n_col] if nodes else ()
    out, put = refs[-2 - bool(nodes)], refs[-1]
    rows = pieces[0].shape[0]
    stores = []
    for k in range(n_col):
        dest = lax.rem(lax.axis_index("col") + k, n_col)
        at = pl.ds(pl.multiple_of((dest * per_dest + base) * TILE, TILE), rows)
        stores.append(pltpu.make_async_copy(pieces[k], out.at[at], put.at[k]))
    for store in stores:
        store.start()
    if nodes:
        total = parts[0][...]
        for part in parts[1:]:
            total = total + part[...]
        total = total / nodes
        mean = total[0:1]
        refs[-2][pl.ds(0, 1), :] = mean
        refs[-2][pl.ds(1, 1), :] = total[1:2] - mean * mean
    for store in stores:
        store.wait()


def place_rows(pieces, out, n_rows, base, parts=(), nodes=0):
    n_col = len(pieces)
    _, width = pieces[0].shape
    per_dest = n_rows // TILE // n_col
    extra = list(parts) + ([] if out is None else [out])
    out_shape = [jax.ShapeDtypeStruct((n_rows, width), jnp.bfloat16)]
    out_specs = [HBM]
    if nodes:
        out_shape.append(jax.ShapeDtypeStruct((2, width), jnp.float32))
        out_specs.append(VMEM)
    return pl.pallas_call(
        functools.partial(place_kernel, n_col, per_dest, base, nodes),
        out_shape=out_shape,
        in_specs=[VMEM] * (n_col + len(parts)) + ([] if out is None else [HBM]),
        out_specs=out_specs,
        scratch_shapes=[pltpu.SemaphoreType.DMA((n_col,))],
        input_output_aliases={} if out is None else {n_col + len(extra) - 1: 0},
        compiler_params=grant(8),
        cost_estimate=cost(1e8, 2 << 20),
        name="place_rows",
    )(*pieces, *extra)


def chunk_plan(per_dest):
    if per_dest % 4:
        return [(0, per_dest)]
    u = per_dest // 4
    return [(0, u), (u, u), (2 * u, u), (3 * u, u)]


def on_device(
    features,
    weight,
    out_bias,
    local_index,
    local_count,
    local_vals,
    halo_index,
    halo_count,
    halo_vals,
    send_rows,
    send_count,
):
    n_rows, width = features.shape
    n_dom, n_col = lax.axis_size("dom"), lax.axis_size("col")

    if n_dom & (n_dom - 1) == 0:
        peer = lambda d, k: d ^ abs(k)
    else:
        peer = lambda d, k: (d + k + n_dom) % n_dom
    along_dom = lambda x, k: lax.ppermute(x, "dom", [(i, peer(i, k)) for i in range(n_dom)])
    along_col = lambda x, k: lax.ppermute(x, "col", [(i, (i + k) % n_col) for i in range(n_col)])

    far = list(reversed(range(1, n_dom)))
    lead = far[0:3:2]
    rest = [k for k in far if k not in lead]
    rows, first_row, within = storage_order(send_rows[0])
    slots = send_rows.shape[2]
    halves = width // LANES
    vals = (local_vals[0], halo_vals[0])
    per_dest = n_rows // TILE // n_col
    plan = chunk_plan(per_dest)
    ahead = [(n_col, per_dest, base, size) for base, size in plan]
    halo, own_tiles = [], []
    for h in range(halves):
        pieces, table = {}, None
        groups = [g for g in (lead, rest) if g] if h == 0 else [lead + rest]
        for peers in groups:
            load = ahead[0] if h == 0 and peers is groups[-1] else ()
            outgoing, made, block = gather_rows(
                rows, first_row, within, send_count[0], features, h, table, peers, peer,
                slots, vals, load,
            )
            if load:
                blocks = [block[0]]
            if made:
                table, tiles = made
            for k, piece in zip(peers, outgoing):
                pieces[k] = along_dom(piece, k)
        halo.append(pieces)
        own_tiles.append(tiles)

    share = 1
    channels = n_col * width
    while share < 8 and n_dom % (2 * share) == 0 and channels % (2 * share * PAD) == 0:
        share *= 2
    order = sorted(range(1, n_col), key=lambda k: min(k, n_col - k), reverse=True)
    bias_row = out_bias.reshape(1, width)
    mine = weight_part(weight, bias_row, share)
    arrived = {k: along_col(mine, k) for k in order}
    parts = [pack_rows([arrived[k] for k in range(1, n_col)])]
    step = share // 2
    got = {0: parts[0]}
    while step:
        swap = [(i, i ^ step) for i in range(n_dom)]
        for flip in list(got):
            got[flip ^ step] = lax.ppermute(got[flip], "dom", swap)
        step //= 2
    weights, bias = join_weights(weight, bias_row, [got[f] for f in range(share)], n_col)

    index_tables = (local_index[0].T, local_count[0], halo_index[0].T, halo_count[0])
    incoming = [[[] for _ in range(n_col)] for _ in plan]
    for h in range(halves):
        received = assemble(far, [halo[h][k] for k in far], n_dom, peer)
        for g, (base, size) in enumerate(plan):
            load = ahead[g + 1] if h == 0 and g + 1 < len(plan) else ()
            sums, block = tile_sums(
                index_tables, received, own_tiles[h], blocks[g], vals, per_dest, base, load
            )
            blocks += block
            moved = {k: along_col(sums[k], k) for k in order}
            for k in range(n_col):
                incoming[g][k].append(moved[k] if k else sums[0])

    stats = None
    returned = []
    for pieces in incoming:
        done, stats = mix_rows(sum(pieces, []), weights, bias, stats)
        moved = {k: along_col(done[k], -k) for k in order}
        returned.append([done[0]] + [moved[k] for k in range(1, n_col)])

    over_dom = lax.all_gather(stats, "dom", axis=0)
    over_dom = over_dom.sum(axis=0)
    totals = [over_dom[:2]]
    for k in range(1, n_col):
        totals.append(along_col(over_dom[2 * k : 2 * k + 2], -k))

    out = None
    for g, ((base, _), pieces) in enumerate(zip(plan, returned)):
        if g < len(plan) - 1:
            (out,) = place_rows(pieces, out, n_rows, base)
        else:
            out, channel_stats = place_rows(
                pieces, out, n_rows, base, totals, n_rows * n_dom
            )
    return (out, channel_stats)


def solution(mesh):
    in_specs = (
        P("dom", "col"),
        P(None, "col"),
        P("col"),
        P("dom", None, None),
        P("dom", None),
        P("dom", None, None, None, None),
        P("dom", None, None),
        P("dom", None),
        P("dom", None, None, None, None),
        P("dom", None, None),
        P("dom", None),
    )
    out_specs = (P("dom", "col"), P(None, "col"))
    return jax.shard_map(
        on_device, mesh=mesh, in_specs=in_specs, out_specs=out_specs, check_vma=False
    )
```

```python
import functools

import jax
import jax.numpy as jnp
from jax import lax
from jax.experimental import pallas as pl
from jax.experimental.pallas import tpu as pltpu
from jax.sharding import PartitionSpec as P


TILE = 128
EPS = 1e-06

HBM = pl.BlockSpec(memory_space=pl.ANY)
VMEM = pl.BlockSpec(memory_space=pltpu.VMEM)
RAW = pl.BlockSpec(memory_space=pltpu.HBM)


def cost(flops, nbytes):
    return pl.CostEstimate(flops=int(flops), bytes_accessed=int(nbytes), transcendentals=0)


def partner(c, k, n):
    return c ^ abs(k) if n & (n - 1) == 0 else (c + k + n) % n


def in_hbm(x):
    return pltpu.with_memory_space_constraint(x, pltpu.HBM)


def in_vmem(x):
    return pltpu.with_memory_space_constraint(x, pltpu.VMEM)


def grant(mib):
    return pltpu.CompilerParams(vmem_limit_bytes=int(mib) << 20)


LANES = 128
SUBLANES = 8
UNROLL = 32


def storage_order(send_rows):
    n, slots = send_rows.shape
    if n % SUBLANES or slots % LANES:
        return send_rows.reshape(-1), lambda q: q * slots, lambda b: b * UNROLL
    blocks = slots // LANES
    tiled = send_rows.reshape(n // SUBLANES, SUBLANES, blocks, LANES)
    tile = SUBLANES * LANES
    per = LANES // UNROLL

    def first(q):
        return (q >> 3) * (blocks * tile) + (q & (SUBLANES - 1)) * LANES

    def within(b):
        return (b >> (per.bit_length() - 1)) * tile + (b & (per - 1)) * UNROLL

    return tiled.transpose(0, 2, 1, 3).reshape(-1), first, within


def widen(feat, half, table, raw, sems):
    n_rows = raw.shape[0]
    parts = sems.shape[0]
    part = n_rows // parts
    step = 128 if part % 128 == 0 else 16
    lanes = pl.ds(half * LANES, LANES)
    copies = [
        pltpu.make_async_copy(
            feat.at[pl.ds(c * part, part), lanes], raw.at[pl.ds(c * part, part)], sems.at[c]
        )
        for c in range(parts)
    ]
    for copy in copies:
        copy.start()
    for c in range(parts):
        copies[c].wait()

        def one(b, carry, c=c):
            at = pl.ds(pl.multiple_of(c * part + b * step, step), step)
            table[at, :] = raw[at, :].astype(jnp.float32)
            return carry

        lax.fori_loop(0, part // step, one, 0)


def gather_kernel(peers, peer, first_row, within, half, build, ahead, rows_in, counts_in, *refs):
    n_out = len(peers)
    refs = list(refs)
    source = refs.pop(0)
    vals = [refs.pop(0) for _ in range(2 * bool(ahead))]
    outs, refs = refs[:n_out], refs[n_out:]
    if build:
        feat, table, raw = source, refs.pop(0), refs.pop(0)
    else:
        table = source
    block = refs.pop(0) if ahead else None
    rows, counts, index_sems, stage = refs[:4]
    loads = block_copies(vals, block, refs[-1], *ahead) if ahead else []
    for load in loads:
        load.start()
    load_rows = pltpu.make_async_copy(rows_in, rows, index_sems.at[0])
    load_counts = pltpu.make_async_copy(counts_in, counts, index_sems.at[1])
    load_rows.start()
    load_counts.start()
    if build:
        widen(feat, half, table, raw, refs[4])
    load_rows.wait()
    load_counts.wait()
    me = lax.axis_index("dom")
    slots = outs[0].shape[0]
    for out, k in zip(outs, peers):
        q = peer(me, k)
        used = counts[q]
        begin = first_row(q)

        def pick(b, carry, begin=begin):
            base = begin + within(b)
            put = pl.multiple_of(b * UNROLL, UNROLL)
            source = [rows[base + j] for j in range(UNROLL)]
            got = [table[pl.ds(r, 1), :] for r in source]
            for j in range(UNROLL):
                stage[pl.ds(put + j, 1), :] = got[j]
            return carry

        lax.fori_loop(0, (used + UNROLL - 1) // UNROLL, pick, 0)
        for b in range(slots // 64):
            at = pl.ds(b * 64, 64)
            slot = b * 64 + lax.broadcasted_iota(jnp.int32, (64, LANES), 0)
            out[at, :] = jnp.where(slot < used, stage[at, :], 0.0).astype(out.dtype)
    for load in loads:
        load.wait()


def gather_rows(
    rows, first_row, within, send_count, features, half, table, peers, peer, slots, vals, ahead
):
    n_rows = features.shape[0]
    build = table is None
    piece = jax.ShapeDtypeStruct((slots, LANES), features.dtype)
    parts = 8 if n_rows % (8 * 16) == 0 else 1
    made = [
        jax.ShapeDtypeStruct((n_rows, LANES), jnp.float32),
        jax.ShapeDtypeStruct((n_rows, LANES), features.dtype),
    ]
    block = [block_shape(vals[0], *ahead)] if ahead else []
    out = pl.pallas_call(
        functools.partial(gather_kernel, peers, peer, first_row, within, half, build, ahead),
        out_shape=[piece] * len(peers) + made * build + block,
        in_specs=[RAW, RAW, RAW if build else VMEM] + [RAW] * (2 * len(block)),
        out_specs=[VMEM] * (len(peers) + 2 * build + len(block)),
        scratch_shapes=[
            pltpu.SMEM(rows.shape, jnp.int32),
            pltpu.SMEM(send_count.shape, jnp.int32),
            pltpu.SemaphoreType.DMA((2,)),
            pltpu.VMEM((slots, LANES), jnp.float32),
        ]
        + [pltpu.SemaphoreType.DMA((parts,))] * build
        + [pltpu.SemaphoreType.DMA((2 * cols[0],)) for cols in [ahead] if ahead],
        compiler_params=grant(10 + len(peers) if build else 8),
        cost_estimate=cost(4e9, 6 << 20),
        name="gather_rows",
    )(
        in_hbm(rows), in_hbm(send_count), in_hbm(features) if build else table,
        *([in_hbm(v) for v in vals] * len(block)),
    )
    n_out = len(peers)
    return out[:n_out], out[n_out : n_out + 2 * build], out[n_out + 2 * build :]


def masked(vals, used):
    return [
        jnp.where(s < used, vals[s], jnp.zeros_like(vals[s])) for s in range(vals.shape[0])
    ]


def tiles_of(src, index, row_tile, slots):
    starts = [pl.multiple_of(index[s, row_tile] * TILE, TILE) for s in range(slots)]
    return [src[pl.ds(at, TILE), :] for at in starts]


def product(left, right):
    return jnp.dot(
        jnp.concatenate(left, axis=1),
        jnp.concatenate(right, axis=0),
        preferred_element_type=jnp.float32,
    )


def row_tile_of(k, n_col, per_dest, tile):
    return partner(lax.axis_index("col"), k, n_col) * per_dest + tile


def block_shape(vals, n_col, per_dest, base, size):
    return jax.ShapeDtypeStruct((n_col, 2, size) + vals.shape[1:], vals.dtype)


def block_copies(vals, block, sems, n_col, per_dest, base, size):
    copies = []
    for k in range(n_col):
        at = pl.ds(row_tile_of(k, n_col, per_dest, base), size)
        for v in range(2):
            copies.append(
                pltpu.make_async_copy(vals[v].at[at], block.at[k, v], sems.at[2 * k + v])
            )
    return copies


def put_piece(halo, piece, q):
    rows = piece.shape[0]
    halo[pl.ds(pl.multiple_of(q * rows, rows), rows), :] = piece[...]


def assemble_kernel(ks, peer, *refs):
    pieces, halo = refs[:-1], refs[-1]
    me = lax.axis_index("dom")
    for k, piece in zip(ks, pieces):
        put_piece(halo, piece, peer(me, -k))
    rows = pieces[0].shape[0]
    own = pl.ds(pl.multiple_of(me * rows, rows), rows)
    halo[own, :] = jnp.zeros((rows, halo.shape[1]), halo.dtype)


def assemble(ks, pieces, n_dom, peer):
    rows, width = pieces[0].shape
    return pl.pallas_call(
        functools.partial(assemble_kernel, ks, peer),
        out_shape=jax.ShapeDtypeStruct((n_dom * rows, width), pieces[0].dtype),
        in_specs=[VMEM] * len(pieces),
        out_specs=VMEM,
        compiler_params=grant(4 + n_dom),
        cost_estimate=cost(2e9, 4 << 20),
        name="assemble",
    )(*pieces)


def sum_kernel(n_col, slots, per_dest, base, ahead, *refs):
    own_index, own_counts, halo_index, halo_counts, feat, halo, block = refs[:7]
    refs = refs[7:]
    loads = []
    if ahead:
        loads = block_copies(refs[:2], refs[2 + n_col], refs[-1], *ahead)
        refs = refs[2:]
    outs = refs[:n_col]
    for load in loads:
        load.start()

    def one(t, carry):
        for k in range(n_col):
            row_tile = row_tile_of(k, n_col, per_dest, base + t)
            left = masked(block.at[k, 0, t], own_counts[row_tile])
            left += masked(block.at[k, 1, t], halo_counts[row_tile])
            right = tiles_of(feat, own_index, row_tile, slots)
            right += tiles_of(halo, halo_index, row_tile, slots)
            at = pl.ds(pl.multiple_of(t * TILE, TILE), TILE)
            outs[k][at, :] = product(left, right).astype(outs[k].dtype)
        return carry

    lax.fori_loop(0, block.shape[2], one, 0)
    for load in loads:
        load.wait()


def tile_sums(tables, halo, features, block, vals, per_dest, base, ahead):
    n_col, _, size, slots = block.shape[:4]
    width = features.shape[1]
    made = [block_shape(vals[0], *ahead)] if ahead else []
    smem = pl.BlockSpec(memory_space=pltpu.SMEM)
    out = pl.pallas_call(
        functools.partial(sum_kernel, n_col, slots, per_dest, base, ahead),
        out_shape=[jax.ShapeDtypeStruct((size * TILE, width), jnp.bfloat16)] * n_col + made,
        grid_spec=pltpu.PrefetchScalarGridSpec(
            num_scalar_prefetch=4,
            grid=(1,),
            in_specs=[VMEM] * 3 + [RAW] * (2 * len(made)),
            out_specs=[VMEM] * (n_col + len(made)),
            scratch_shapes=[pltpu.SemaphoreType.DMA((2 * n_col,))] * len(made),
        ),
        compiler_params=grant(8),
        cost_estimate=cost(2e9, 6 << 20),
        name="tile_sums",
    )(
        *tables, in_vmem(features), in_vmem(halo), in_vmem(block),
        *([in_hbm(v) for v in vals] * len(made)),
    )
    return out[:n_col], out[n_col:]


PAD = 16


def part_kernel(share, weight, bias, out, sem):
    part = weight.shape[0] // share
    start = lax.rem(lax.axis_index("dom"), share) * part
    src = weight.at[pl.ds(pl.multiple_of(start, part), part)]
    copy = pltpu.make_async_copy(src, out.at[pl.ds(0, part)], sem)
    copy.start()
    out[pl.ds(part, PAD), :] = jnp.broadcast_to(bias[...], (PAD, out.shape[1]))
    copy.wait()


def weight_part(weight, bias, share):
    rows = weight.shape[0] // share + PAD
    return pl.pallas_call(
        functools.partial(part_kernel, share),
        out_shape=jax.ShapeDtypeStruct((rows, weight.shape[1]), weight.dtype),
        in_specs=[RAW, VMEM],
        out_specs=VMEM,
        scratch_shapes=[pltpu.SemaphoreType.DMA],
        compiler_params=grant(4),
        cost_estimate=cost(1e8, 1 << 20),
        name="weight_part",
    )(in_hbm(weight), bias)


def pack_kernel(*refs):
    rows = refs[0].shape[0]
    for k, ref in enumerate(refs[:-1]):
        refs[-1][pl.ds(k * rows, rows), :] = ref[...]


def pack_rows(arrays):
    rows, width = arrays[0].shape
    return pl.pallas_call(
        pack_kernel,
        out_shape=jax.ShapeDtypeStruct((rows * len(arrays), width), arrays[0].dtype),
        in_specs=[VMEM] * len(arrays),
        out_specs=VMEM,
        compiler_params=grant(4),
        cost_estimate=cost(1e8, 1 << 20),
        name="pack_rows",
    )(*arrays)


def join_kernel(n_col, share, own, own_bias, *refs):
    parts = refs[:share]
    joined, bias = refs[share:]
    width = own.shape[1]
    part = own.shape[0] // share
    me = lax.rem(lax.axis_index("dom"), share)
    block = min(width, part)
    for s in range(n_col):
        for b in range(width // block):
            row = partner(lax.axis_index("col"), -s, n_col) * width + b * block
            row = pl.multiple_of(row, block)
            at = pl.ds(s * width + b * block, block)
            joined[0, at, :] = own[pl.ds(row, block), :]
            side = lax.div(row, part)
            offset = row - side * part
            for flip in range(share):

                @pl.when(side == me ^ flip)
                def _(flip=flip, at=at, offset=offset):
                    for k in range(1, n_col):
                        start = pl.multiple_of((k - 1) * (part + PAD) + offset, PAD)
                        joined[k, at, :] = parts[flip][pl.ds(start, block), :]

    bias[pl.ds(0, 1), :] = own_bias[...].astype(jnp.float32)
    for k in range(1, n_col):
        got = parts[0][pl.ds(k * part + (k - 1) * PAD, PAD), :].astype(jnp.float32)
        bias[pl.ds(k, 1), :] = got[:1]


def join_weights(weight, bias, parts, n_col):
    channels, width = weight.shape
    share = len(parts)
    return pl.pallas_call(
        functools.partial(join_kernel, n_col, share),
        out_shape=[
            jax.ShapeDtypeStruct((n_col, channels, width), weight.dtype),
            jax.ShapeDtypeStruct((n_col, width), jnp.float32),
        ],
        in_specs=[VMEM] * (2 + share),
        out_specs=[VMEM] * 2,
        compiler_params=grant(8),
        cost_estimate=cost(1e9, 4 << 20),
        name="join_weights",
    )(weight, bias, *parts)


def mix_kernel(n_col, n_in, channels, first, *refs):
    pieces, held, bias = refs[:n_in], refs[n_in], refs[n_in + 1]
    outs, stats = refs[-n_col - 1 : -1], refs[-1]

    @pl.when(pl.program_id(0) == 0)
    def _():
        stats[...] = jnp.zeros_like(stats) if first else refs[n_in + 2][...]

    spread = jnp.concatenate([piece[...] for piece in pieces], axis=1)
    active, power = [], 0.0
    for k in range(n_col):
        mixed = jnp.dot(spread, held[k], preferred_element_type=jnp.float32)
        mixed = jnp.maximum(mixed + bias[pl.ds(k, 1), :], 0.0)
        power = power + jnp.sum(mixed * mixed, axis=1, keepdims=True)
        active.append(mixed)
    scale = lax.rsqrt(power * (1.0 / channels) + EPS)
    for k in range(n_col):
        scaled = active[k] * scale
        outs[k][...] = scaled.astype(outs[k].dtype)
        stats[pl.ds(2 * k, 1), :] += jnp.sum(scaled, axis=0, keepdims=True)
        stats[pl.ds(2 * k + 1, 1), :] += jnp.sum(scaled * scaled, axis=0, keepdims=True)


def mix_rows(pieces, weights, bias, before):
    n_col, channels, width = weights.shape
    rows = pieces[0].shape[0]
    block = TILE
    spec = lambda w: pl.BlockSpec((block, w), lambda i: (i, 0))
    first = before is None
    out = pl.pallas_call(
        functools.partial(mix_kernel, n_col, len(pieces), channels, first),
        out_shape=[jax.ShapeDtypeStruct((rows, width), jnp.bfloat16)] * n_col
        + [jax.ShapeDtypeStruct((2 * n_col, width), jnp.float32)],
        grid=(rows // block,),
        in_specs=[spec(piece.shape[1]) for piece in pieces] + [VMEM] * (2 if first else 3),
        out_specs=[spec(width)] * n_col + [VMEM],
        compiler_params=grant(10),
        cost_estimate=cost(2 * rows * channels * channels, 4 << 20),
        name="mix_rows",
    )(*pieces, weights, bias, *([] if first else [before]))
    return out[:n_col], out[n_col]


def place_kernel(n_col, per_dest, base, nodes, *refs):
    pieces = refs[:n_col]
    parts = refs[n_col : 2 * n_col] if nodes else ()
    out, put = refs[-2 - bool(nodes)], refs[-1]
    rows = pieces[0].shape[0]
    stores = []
    for k in range(n_col):
        dest = partner(lax.axis_index("col"), k, n_col)
        at = pl.ds(pl.multiple_of((dest * per_dest + base) * TILE, TILE), rows)
        stores.append(pltpu.make_async_copy(pieces[k], out.at[at], put.at[k]))
    for store in stores:
        store.start()
    if nodes:
        total = parts[0][...]
        for part in parts[1:]:
            total = total + part[...]
        total = total / nodes
        mean = total[0:1]
        refs[-2][pl.ds(0, 1), :] = mean
        refs[-2][pl.ds(1, 1), :] = total[1:2] - mean * mean
    for store in stores:
        store.wait()


def place_rows(pieces, out, n_rows, base, parts=(), nodes=0):
    n_col = len(pieces)
    _, width = pieces[0].shape
    per_dest = n_rows // TILE // n_col
    extra = list(parts) + ([] if out is None else [out])
    out_shape = [jax.ShapeDtypeStruct((n_rows, width), jnp.bfloat16)]
    out_specs = [HBM]
    if nodes:
        out_shape.append(jax.ShapeDtypeStruct((2, width), jnp.float32))
        out_specs.append(VMEM)
    return pl.pallas_call(
        functools.partial(place_kernel, n_col, per_dest, base, nodes),
        out_shape=out_shape,
        in_specs=[VMEM] * (n_col + len(parts)) + ([] if out is None else [HBM]),
        out_specs=out_specs,
        scratch_shapes=[pltpu.SemaphoreType.DMA((n_col,))],
        input_output_aliases={} if out is None else {n_col + len(extra) - 1: 0},
        compiler_params=grant(8),
        cost_estimate=cost(1e8, 2 << 20),
        name="place_rows",
    )(*pieces, *extra)


def chunk_plan(per_dest):
    if per_dest < 16:
        return [(0, per_dest)]
    cuts = [per_dest * c // 16 for c in (0, 3, 7, 13, 16)]
    return [(a, b - a) for a, b in zip(cuts, cuts[1:])]


def sharers(n_dom, channels):
    share = 1
    while share < 8 and n_dom % (2 * share) == 0 and channels % (2 * share * PAD) == 0:
        share *= 2
    return share


def swap_stages(share):
    return [1 << b for b in reversed(range(share.bit_length() - 1))]


def on_device(
    features,
    weight,
    out_bias,
    local_index,
    local_count,
    local_vals,
    halo_index,
    halo_count,
    halo_vals,
    send_rows,
    send_count,
):
    n_rows, width = features.shape
    n_dom, n_col = lax.axis_size("dom"), lax.axis_size("col")

    peer = lambda d, k: partner(d, k, n_dom)
    along_dom = lambda x, k: lax.ppermute(x, "dom", [(i, peer(i, k)) for i in range(n_dom)])
    along_col = lambda x, k: lax.ppermute(
        x, "col", [(i, partner(i, k, n_col)) for i in range(n_col)]
    )
    order = list(reversed(range(1, n_col)))

    far = list(reversed(range(1, n_dom)))
    lead = far[:3]
    rest = [k for k in far if k not in lead]
    rows, first_row, within = storage_order(send_rows[0])
    slots = send_rows.shape[2]
    halves = width // LANES
    vals = (local_vals[0], halo_vals[0])
    per_dest = n_rows // TILE // n_col
    plan = chunk_plan(per_dest)
    ahead = [(n_col, per_dest, base, size) for base, size in plan]
    halo, own_tiles = [], []
    for h in range(halves):
        pieces, table = {}, None
        groups = [g for g in (lead, rest) if g] if h == 0 else [lead + rest]
        for peers in groups:
            load = ahead[0] if h == 0 and peers is groups[-1] else ()
            outgoing, made, block = gather_rows(
                rows, first_row, within, send_count[0], features, h, table, peers, peer,
                slots, vals, load,
            )
            if load:
                blocks = [block[0]]
            if made:
                table, tiles = made
            for k, piece in zip(peers, outgoing):
                pieces[k] = along_dom(piece, k)
        halo.append(pieces)
        own_tiles.append(tiles)

    share = sharers(n_dom, n_col * width)
    bias_row = out_bias.reshape(1, width)
    mine = weight_part(weight, bias_row, share)
    arrived = {k: along_col(mine, k) for k in order}
    parts = [pack_rows([arrived[k] for k in range(1, n_col)])]
    got = {0: parts[0]}
    for step in swap_stages(share):
        swap = [(i, i ^ step) for i in range(n_dom)]
        for flip in list(got):
            got[flip ^ step] = lax.ppermute(got[flip], "dom", swap)
    weights, bias = join_weights(weight, bias_row, [got[f] for f in range(share)], n_col)

    index_tables = (local_index[0].T, local_count[0], halo_index[0].T, halo_count[0])
    incoming = [[[] for _ in range(n_col)] for _ in plan]
    for h in range(halves):
        received = assemble(far, [halo[h][k] for k in far], n_dom, peer)
        for g, (base, size) in enumerate(plan):
            load = ahead[g + 1] if h == 0 and g + 1 < len(plan) else ()
            sums, block = tile_sums(
                index_tables, received, own_tiles[h], blocks[g], vals, per_dest, base, load
            )
            blocks += block
            moved = {k: along_col(sums[k], k) for k in order}
            for k in range(n_col):
                incoming[g][k].append(moved[k] if k else sums[0])

    stats = None
    returned = []
    for pieces in incoming:
        done, stats = mix_rows(sum(pieces, []), weights, bias, stats)
        moved = {k: along_col(done[k], -k) for k in order}
        returned.append([done[0]] + [moved[k] for k in range(1, n_col)])

    over_dom = lax.all_gather(stats, "dom", axis=0)
    over_dom = over_dom.sum(axis=0)
    totals = [over_dom[:2]]
    for k in range(1, n_col):
        totals.append(along_col(over_dom[2 * k : 2 * k + 2], -k))

    out = None
    for g, ((base, _), pieces) in enumerate(zip(plan, returned)):
        if g < len(plan) - 1:
            (out,) = place_rows(pieces, out, n_rows, base)
        else:
            out, channel_stats = place_rows(
                pieces, out, n_rows, base, totals, n_rows * n_dom
            )
    return (out, channel_stats)


def solution(mesh):
    in_specs = (
        P("dom", "col"),
        P(None, "col"),
        P("col"),
        P("dom", None, None),
        P("dom", None),
        P("dom", None, None, None, None),
        P("dom", None, None),
        P("dom", None),
        P("dom", None, None, None, None),
        P("dom", None, None),
        P("dom", None),
    )
    out_specs = (P("dom", "col"), P(None, "col"))
    return jax.shard_map(
        on_device, mesh=mesh, in_specs=in_specs, out_specs=out_specs, check_vma=False
    )
```

```python
import functools

import jax
import jax.numpy as jnp
from jax import lax
from jax.experimental import pallas as pl
from jax.experimental.pallas import tpu as pltpu
from jax.sharding import PartitionSpec as P


TILE = 128
EPS = 1e-06

HBM = pl.BlockSpec(memory_space=pl.ANY)
VMEM = pl.BlockSpec(memory_space=pltpu.VMEM)
RAW = pl.BlockSpec(memory_space=pltpu.HBM)


def cost(flops, nbytes):
    return pl.CostEstimate(flops=int(flops), bytes_accessed=int(nbytes), transcendentals=0)


def partner(c, k, n):
    return c ^ abs(k) if n & (n - 1) == 0 else (c + k + n) % n


def in_hbm(x):
    return pltpu.with_memory_space_constraint(x, pltpu.HBM)


def in_vmem(x):
    return pltpu.with_memory_space_constraint(x, pltpu.VMEM)


def grant(mib):
    return pltpu.CompilerParams(vmem_limit_bytes=int(mib) << 20)


LANES = 128
SUBLANES = 8
UNROLL = 32


def storage_order(send_rows):
    n, slots = send_rows.shape
    if n % SUBLANES or slots % LANES:
        return send_rows.reshape(-1), lambda q: q * slots, lambda b: b * UNROLL
    blocks = slots // LANES
    tiled = send_rows.reshape(n // SUBLANES, SUBLANES, blocks, LANES)
    tile = SUBLANES * LANES
    per = LANES // UNROLL

    def first(q):
        return (q >> 3) * (blocks * tile) + (q & (SUBLANES - 1)) * LANES

    def within(b):
        return (b >> (per.bit_length() - 1)) * tile + (b & (per - 1)) * UNROLL

    return tiled.transpose(0, 2, 1, 3).reshape(-1), first, within


def widen(feat, half, table, raw, sems):
    n_rows = raw.shape[0]
    parts = sems.shape[0]
    part = n_rows // parts
    step = 128 if part % 128 == 0 else 16
    lanes = pl.ds(half * LANES, LANES)
    copies = [
        pltpu.make_async_copy(
            feat.at[pl.ds(c * part, part), lanes], raw.at[pl.ds(c * part, part)], sems.at[c]
        )
        for c in range(parts)
    ]
    for copy in copies:
        copy.start()
    for c in range(parts):
        copies[c].wait()

        def one(b, carry, c=c):
            at = pl.ds(pl.multiple_of(c * part + b * step, step), step)
            table[at, :] = raw[at, :].astype(jnp.float32)
            return carry

        lax.fori_loop(0, part // step, one, 0)


def gather_kernel(peers, peer, first_row, within, half, build, ahead, rows_in, counts_in, *refs):
    n_out = len(peers)
    refs = list(refs)
    source = refs.pop(0)
    vals = [refs.pop(0) for _ in range(2 * bool(ahead))]
    outs, refs = refs[:n_out], refs[n_out:]
    if build:
        feat, table, raw = source, refs.pop(0), refs.pop(0)
    else:
        table = source
    block = refs.pop(0) if ahead else None
    rows, counts, index_sems, stage = refs[:4]
    loads = block_copies(vals, block, refs[-1], *ahead) if ahead else []
    for load in loads:
        load.start()
    load_rows = pltpu.make_async_copy(rows_in, rows, index_sems.at[0])
    load_counts = pltpu.make_async_copy(counts_in, counts, index_sems.at[1])
    load_rows.start()
    load_counts.start()
    if build:
        widen(feat, half, table, raw, refs[4])
    load_rows.wait()
    load_counts.wait()
    me = lax.axis_index("dom")
    slots = outs[0].shape[0]
    for out, k in zip(outs, peers):
        q = peer(me, k)
        used = counts[q]
        begin = first_row(q)

        def pick(b, carry, begin=begin):
            base = begin + within(b)
            put = pl.multiple_of(b * UNROLL, UNROLL)
            source = [rows[base + j] for j in range(UNROLL)]
            got = [table[pl.ds(r, 1), :] for r in source]
            for j in range(UNROLL):
                stage[pl.ds(put + j, 1), :] = got[j]
            return carry

        lax.fori_loop(0, (used + UNROLL - 1) // UNROLL, pick, 0)
        for b in range(slots // 64):
            at = pl.ds(b * 64, 64)
            slot = b * 64 + lax.broadcasted_iota(jnp.int32, (64, LANES), 0)
            out[at, :] = jnp.where(slot < used, stage[at, :], 0.0).astype(out.dtype)
    for load in loads:
        load.wait()


def gather_rows(
    rows, first_row, within, send_count, features, half, table, peers, peer, slots, vals, ahead
):
    n_rows = features.shape[0]
    build = table is None
    piece = jax.ShapeDtypeStruct((slots, LANES), features.dtype)
    parts = 8 if n_rows % (8 * 16) == 0 else 1
    made = [
        jax.ShapeDtypeStruct((n_rows, LANES), jnp.float32),
        jax.ShapeDtypeStruct((n_rows, LANES), features.dtype),
    ]
    block = [block_shape(vals[0], *ahead)] if ahead else []
    out = pl.pallas_call(
        functools.partial(gather_kernel, peers, peer, first_row, within, half, build, ahead),
        out_shape=[piece] * len(peers) + made * build + block,
        in_specs=[RAW, RAW, RAW if build else VMEM] + [RAW] * (2 * len(block)),
        out_specs=[VMEM] * (len(peers) + 2 * build + len(block)),
        scratch_shapes=[
            pltpu.SMEM(rows.shape, jnp.int32),
            pltpu.SMEM(send_count.shape, jnp.int32),
            pltpu.SemaphoreType.DMA((2,)),
            pltpu.VMEM((slots, LANES), jnp.float32),
        ]
        + [pltpu.SemaphoreType.DMA((parts,))] * build
        + [pltpu.SemaphoreType.DMA((2 * cols[0],)) for cols in [ahead] if ahead],
        compiler_params=grant(10 + len(peers) if build else 8),
        cost_estimate=cost(4e9, 6 << 20),
        name="gather_rows",
    )(
        in_hbm(rows), in_hbm(send_count), in_hbm(features) if build else table,
        *([in_hbm(v) for v in vals] * len(block)),
    )
    n_out = len(peers)
    return out[:n_out], out[n_out : n_out + 2 * build], out[n_out + 2 * build :]


def masked(vals, used):
    return [
        jnp.where(s < used, vals[s], jnp.zeros_like(vals[s])) for s in range(vals.shape[0])
    ]


def tiles_of(src, index, row_tile, slots):
    starts = [pl.multiple_of(index[s, row_tile] * TILE, TILE) for s in range(slots)]
    return [src[pl.ds(at, TILE), :] for at in starts]


def product(left, right):
    return jnp.dot(
        jnp.concatenate(left, axis=1),
        jnp.concatenate(right, axis=0),
        preferred_element_type=jnp.float32,
    )


def row_tile_of(k, n_col, per_dest, tile):
    return partner(lax.axis_index("col"), k, n_col) * per_dest + tile


def block_shape(vals, n_col, per_dest, base, size):
    return jax.ShapeDtypeStruct((n_col, 2, size) + vals.shape[1:], vals.dtype)


def block_copies(vals, block, sems, n_col, per_dest, base, size):
    copies = []
    for k in range(n_col):
        at = pl.ds(row_tile_of(k, n_col, per_dest, base), size)
        for v in range(2):
            copies.append(
                pltpu.make_async_copy(vals[v].at[at], block.at[k, v], sems.at[2 * k + v])
            )
    return copies


def put_piece(halo, piece, q):
    rows = piece.shape[0]
    halo[pl.ds(pl.multiple_of(q * rows, rows), rows), :] = piece[...]


def assemble_kernel(ks, peer, *refs):
    pieces, halo = refs[:-1], refs[-1]
    me = lax.axis_index("dom")
    for k, piece in zip(ks, pieces):
        put_piece(halo, piece, peer(me, -k))
    rows = pieces[0].shape[0]
    own = pl.ds(pl.multiple_of(me * rows, rows), rows)
    halo[own, :] = jnp.zeros((rows, halo.shape[1]), halo.dtype)


def assemble(ks, pieces, n_dom, peer):
    rows, width = pieces[0].shape
    return pl.pallas_call(
        functools.partial(assemble_kernel, ks, peer),
        out_shape=jax.ShapeDtypeStruct((n_dom * rows, width), pieces[0].dtype),
        in_specs=[VMEM] * len(pieces),
        out_specs=VMEM,
        compiler_params=grant(4 + n_dom),
        cost_estimate=cost(2e9, 4 << 20),
        name="assemble",
    )(*pieces)


def sum_kernel(n_col, slots, per_dest, base, ahead, *refs):
    own_index, own_counts, halo_index, halo_counts, feat, halo, block = refs[:7]
    refs = refs[7:]
    loads = []
    if ahead:
        loads = block_copies(refs[:2], refs[2 + n_col], refs[-1], *ahead)
        refs = refs[2:]
    outs = refs[:n_col]
    for load in loads:
        load.start()

    def one(t, carry):
        for k in range(n_col):
            row_tile = row_tile_of(k, n_col, per_dest, base + t)
            left = masked(block.at[k, 0, t], own_counts[row_tile])
            left += masked(block.at[k, 1, t], halo_counts[row_tile])
            right = tiles_of(feat, own_index, row_tile, slots)
            right += tiles_of(halo, halo_index, row_tile, slots)
            at = pl.ds(pl.multiple_of(t * TILE, TILE), TILE)
            outs[k][at, :] = product(left, right).astype(outs[k].dtype)
        return carry

    lax.fori_loop(0, block.shape[2], one, 0)
    for load in loads:
        load.wait()


def tile_sums(tables, halo, features, block, vals, per_dest, base, ahead):
    n_col, _, size, slots = block.shape[:4]
    width = features.shape[1]
    made = [block_shape(vals[0], *ahead)] if ahead else []
    smem = pl.BlockSpec(memory_space=pltpu.SMEM)
    out = pl.pallas_call(
        functools.partial(sum_kernel, n_col, slots, per_dest, base, ahead),
        out_shape=[jax.ShapeDtypeStruct((size * TILE, width), jnp.bfloat16)] * n_col + made,
        grid_spec=pltpu.PrefetchScalarGridSpec(
            num_scalar_prefetch=4,
            grid=(1,),
            in_specs=[VMEM] * 3 + [RAW] * (2 * len(made)),
            out_specs=[VMEM] * (n_col + len(made)),
            scratch_shapes=[pltpu.SemaphoreType.DMA((2 * n_col,))] * len(made),
        ),
        compiler_params=grant(8),
        cost_estimate=cost(2e9, 6 << 20),
        name="tile_sums",
    )(
        *tables, in_vmem(features), in_vmem(halo), in_vmem(block),
        *([in_hbm(v) for v in vals] * len(made)),
    )
    return out[:n_col], out[n_col:]


PAD = 16


def part_kernel(share, ahead, weight, bias, *refs):
    if ahead:
        out, block, sem, sems = refs[2:]
        loads = block_copies(refs[:2], block, sems, *ahead)
    else:
        (out, sem), loads = refs, []
    part = weight.shape[0] // share
    start = lax.rem(lax.axis_index("dom"), share) * part
    src = weight.at[pl.ds(pl.multiple_of(start, part), part)]
    copy = pltpu.make_async_copy(src, out.at[pl.ds(0, part)], sem)
    copy.start()
    for load in loads:
        load.start()
    out[pl.ds(part, PAD), :] = jnp.broadcast_to(bias[...], (PAD, out.shape[1]))
    copy.wait()
    for load in loads:
        load.wait()


def weight_part(weight, bias, share, vals, ahead):
    rows = weight.shape[0] // share + PAD
    made = [block_shape(vals[0], *ahead)] if ahead else []
    return pl.pallas_call(
        functools.partial(part_kernel, share, ahead),
        out_shape=[jax.ShapeDtypeStruct((rows, weight.shape[1]), weight.dtype)] + made,
        in_specs=[RAW, VMEM] + [RAW] * (2 * len(made)),
        out_specs=[VMEM] * (1 + len(made)),
        scratch_shapes=[pltpu.SemaphoreType.DMA]
        + [pltpu.SemaphoreType.DMA((2 * cols[0],)) for cols in [ahead] if ahead],
        compiler_params=grant(8),
        cost_estimate=cost(1e8, 1 << 20),
        name="weight_part",
    )(in_hbm(weight), bias, *([in_hbm(v) for v in vals] * len(made)))


def pack_kernel(*refs):
    rows = refs[0].shape[0]
    for k, ref in enumerate(refs[:-1]):
        refs[-1][pl.ds(k * rows, rows), :] = ref[...]


def pack_rows(arrays):
    rows, width = arrays[0].shape
    return pl.pallas_call(
        pack_kernel,
        out_shape=jax.ShapeDtypeStruct((rows * len(arrays), width), arrays[0].dtype),
        in_specs=[VMEM] * len(arrays),
        out_specs=VMEM,
        compiler_params=grant(4),
        cost_estimate=cost(1e8, 1 << 20),
        name="pack_rows",
    )(*arrays)


def join_kernel(n_col, share, own, own_bias, *refs):
    parts = refs[:share]
    joined, bias = refs[share:]
    width = own.shape[1]
    part = own.shape[0] // share
    me = lax.rem(lax.axis_index("dom"), share)
    block = min(width, part)
    for s in range(n_col):
        for b in range(width // block):
            row = partner(lax.axis_index("col"), -s, n_col) * width + b * block
            row = pl.multiple_of(row, block)
            at = pl.ds(s * width + b * block, block)
            joined[0, at, :] = own[pl.ds(row, block), :]
            side = lax.div(row, part)
            offset = row - side * part
            for flip in range(share):

                @pl.when(side == me ^ flip)
                def _(flip=flip, at=at, offset=offset):
                    for k in range(1, n_col):
                        start = pl.multiple_of((k - 1) * (part + PAD) + offset, PAD)
                        joined[k, at, :] = parts[flip][pl.ds(start, block), :]

    bias[pl.ds(0, 1), :] = own_bias[...].astype(jnp.float32)
    for k in range(1, n_col):
        got = parts[0][pl.ds(k * part + (k - 1) * PAD, PAD), :].astype(jnp.float32)
        bias[pl.ds(k, 1), :] = got[:1]


def join_weights(weight, bias, parts, n_col):
    channels, width = weight.shape
    share = len(parts)
    return pl.pallas_call(
        functools.partial(join_kernel, n_col, share),
        out_shape=[
            jax.ShapeDtypeStruct((n_col, channels, width), weight.dtype),
            jax.ShapeDtypeStruct((n_col, width), jnp.float32),
        ],
        in_specs=[VMEM] * (2 + share),
        out_specs=[VMEM] * 2,
        compiler_params=grant(8),
        cost_estimate=cost(1e9, 4 << 20),
        name="join_weights",
    )(weight, bias, *parts)


def mix_kernel(n_col, n_in, channels, first, *refs):
    pieces, held, bias = refs[:n_in], refs[n_in], refs[n_in + 1]
    outs, stats = refs[-n_col - 1 : -1], refs[-1]

    @pl.when(pl.program_id(0) == 0)
    def _():
        stats[...] = jnp.zeros_like(stats) if first else refs[n_in + 2][...]

    spread = jnp.concatenate([piece[...] for piece in pieces], axis=1)
    active, power = [], 0.0
    for k in range(n_col):
        mixed = jnp.dot(spread, held[k], preferred_element_type=jnp.float32)
        mixed = jnp.maximum(mixed + bias[pl.ds(k, 1), :], 0.0)
        power = power + jnp.sum(mixed * mixed, axis=1, keepdims=True)
        active.append(mixed)
    scale = lax.rsqrt(power * (1.0 / channels) + EPS)
    for k in range(n_col):
        scaled = active[k] * scale
        outs[k][...] = scaled.astype(outs[k].dtype)
        stats[pl.ds(2 * k, 1), :] += jnp.sum(scaled, axis=0, keepdims=True)
        stats[pl.ds(2 * k + 1, 1), :] += jnp.sum(scaled * scaled, axis=0, keepdims=True)


def mix_rows(pieces, weights, bias, before):
    n_col, channels, width = weights.shape
    rows = pieces[0].shape[0]
    block = TILE
    spec = lambda w: pl.BlockSpec((block, w), lambda i: (i, 0))
    first = before is None
    out = pl.pallas_call(
        functools.partial(mix_kernel, n_col, len(pieces), channels, first),
        out_shape=[jax.ShapeDtypeStruct((rows, width), jnp.bfloat16)] * n_col
        + [jax.ShapeDtypeStruct((2 * n_col, width), jnp.float32)],
        grid=(rows // block,),
        in_specs=[spec(piece.shape[1]) for piece in pieces] + [VMEM] * (2 if first else 3),
        out_specs=[spec(width)] * n_col + [VMEM],
        compiler_params=grant(10),
        cost_estimate=cost(2 * rows * channels * channels, 4 << 20),
        name="mix_rows",
    )(*pieces, weights, bias, *([] if first else [before]))
    return out[:n_col], out[n_col]


def place_kernel(n_col, per_dest, base, nodes, *refs):
    pieces = refs[:n_col]
    parts = refs[n_col : 2 * n_col] if nodes else ()
    out, put = refs[-2 - bool(nodes)], refs[-1]
    rows = pieces[0].shape[0]
    stores = []
    for k in range(n_col):
        dest = partner(lax.axis_index("col"), k, n_col)
        at = pl.ds(pl.multiple_of((dest * per_dest + base) * TILE, TILE), rows)
        stores.append(pltpu.make_async_copy(pieces[k], out.at[at], put.at[k]))
    for store in stores:
        store.start()
    if nodes:
        total = parts[0][...]
        for part in parts[1:]:
            total = total + part[...]
        total = total / nodes
        mean = total[0:1]
        refs[-2][pl.ds(0, 1), :] = mean
        refs[-2][pl.ds(1, 1), :] = total[1:2] - mean * mean
    for store in stores:
        store.wait()


def place_rows(pieces, out, n_rows, base, parts=(), nodes=0):
    n_col = len(pieces)
    _, width = pieces[0].shape
    per_dest = n_rows // TILE // n_col
    extra = list(parts) + ([] if out is None else [out])
    out_shape = [jax.ShapeDtypeStruct((n_rows, width), jnp.bfloat16)]
    out_specs = [HBM]
    if nodes:
        out_shape.append(jax.ShapeDtypeStruct((2, width), jnp.float32))
        out_specs.append(VMEM)
    return pl.pallas_call(
        functools.partial(place_kernel, n_col, per_dest, base, nodes),
        out_shape=out_shape,
        in_specs=[VMEM] * (n_col + len(parts)) + ([] if out is None else [HBM]),
        out_specs=out_specs,
        scratch_shapes=[pltpu.SemaphoreType.DMA((n_col,))],
        input_output_aliases={} if out is None else {n_col + len(extra) - 1: 0},
        compiler_params=grant(8),
        cost_estimate=cost(1e8, 2 << 20),
        name="place_rows",
    )(*pieces, *extra)


def chunk_plan(per_dest):
    if per_dest < 16:
        return [(0, per_dest)]
    cuts = [per_dest * c // 16 for c in (0, 3, 7, 13, 16)]
    return [(a, b - a) for a, b in zip(cuts, cuts[1:])]


def sharers(n_dom, channels):
    share = 1
    while share < 8 and n_dom % (2 * share) == 0 and channels % (2 * share * PAD) == 0:
        share *= 2
    return share


def swap_stages(share):
    return [1 << b for b in reversed(range(share.bit_length() - 1))]


def on_device(
    features,
    weight,
    out_bias,
    local_index,
    local_count,
    local_vals,
    halo_index,
    halo_count,
    halo_vals,
    send_rows,
    send_count,
):
    n_rows, width = features.shape
    n_dom, n_col = lax.axis_size("dom"), lax.axis_size("col")

    peer = lambda d, k: partner(d, k, n_dom)
    along_dom = lambda x, k: lax.ppermute(x, "dom", [(i, peer(i, k)) for i in range(n_dom)])
    along_col = lambda x, k: lax.ppermute(
        x, "col", [(i, partner(i, k, n_col)) for i in range(n_col)]
    )
    order = list(reversed(range(1, n_col)))

    far = list(reversed(range(1, n_dom)))
    lead = far[:3]
    rest = [k for k in far if k not in lead]
    rows, first_row, within = storage_order(send_rows[0])
    slots = send_rows.shape[2]
    halves = width // LANES
    vals = (local_vals[0], halo_vals[0])
    per_dest = n_rows // TILE // n_col
    plan = chunk_plan(per_dest)
    ahead = [(n_col, per_dest, base, size) for base, size in plan]
    halo, own_tiles = [], []
    for h in range(halves):
        pieces, table = {}, None
        groups = [g for g in (lead, rest) if g] if h == 0 else [lead + rest]
        for peers in groups:
            load = ahead[0] if h == 0 and peers is groups[-1] else ()
            outgoing, made, block = gather_rows(
                rows, first_row, within, send_count[0], features, h, table, peers, peer,
                slots, vals, load,
            )
            if load:
                blocks = [block[0]]
            if made:
                table, tiles = made
            for k, piece in zip(peers, outgoing):
                pieces[k] = along_dom(piece, k)
        halo.append(pieces)
        own_tiles.append(tiles)

    share = sharers(n_dom, n_col * width)
    bias_row = out_bias.reshape(1, width)
    mine, *block = weight_part(
        weight, bias_row, share, vals, ahead[1] if len(plan) > 1 else ()
    )
    blocks += block
    arrived = {k: along_col(mine, k) for k in order}
    parts = [pack_rows([arrived[k] for k in range(1, n_col)])]
    got = {0: parts[0]}
    for step in swap_stages(share):
        swap = [(i, i ^ step) for i in range(n_dom)]
        for flip in list(got):
            got[flip ^ step] = lax.ppermute(got[flip], "dom", swap)
    weights, bias = join_weights(weight, bias_row, [got[f] for f in range(share)], n_col)

    index_tables = (local_index[0].T, local_count[0], halo_index[0].T, halo_count[0])
    incoming = [[[] for _ in range(n_col)] for _ in plan]
    for h in range(halves):
        received = assemble(far, [halo[h][k] for k in far], n_dom, peer)
        for g, (base, size) in enumerate(plan):
            load = ahead[g + 1] if h == 0 < g < len(plan) - 1 else ()
            sums, block = tile_sums(
                index_tables, received, own_tiles[h], blocks[g], vals, per_dest, base, load
            )
            blocks += block
            moved = {k: along_col(sums[k], k) for k in order}
            for k in range(n_col):
                incoming[g][k].append(moved[k] if k else sums[0])

    stats = None
    returned = []
    for pieces in incoming:
        done, stats = mix_rows(sum(pieces, []), weights, bias, stats)
        moved = {k: along_col(done[k], -k) for k in order}
        returned.append([done[0]] + [moved[k] for k in range(1, n_col)])

    over_dom = lax.all_gather(stats, "dom", axis=0)
    over_dom = over_dom.sum(axis=0)
    totals = [over_dom[:2]]
    for k in range(1, n_col):
        totals.append(along_col(over_dom[2 * k : 2 * k + 2], -k))

    out = None
    for g, ((base, _), pieces) in enumerate(zip(plan, returned)):
        if g < len(plan) - 1:
            (out,) = place_rows(pieces, out, n_rows, base)
        else:
            out, channel_stats = place_rows(
                pieces, out, n_rows, base, totals, n_rows * n_dom
            )
    return (out, channel_stats)


def solution(mesh):
    in_specs = (
        P("dom", "col"),
        P(None, "col"),
        P("col"),
        P("dom", None, None),
        P("dom", None),
        P("dom", None, None, None, None),
        P("dom", None, None),
        P("dom", None),
        P("dom", None, None, None, None),
        P("dom", None, None),
        P("dom", None),
    )
    out_specs = (P("dom", "col"), P(None, "col"))
    return jax.shard_map(
        on_device, mesh=mesh, in_specs=in_specs, out_specs=out_specs, check_vma=False
    )
```

```python
import functools

import jax
import jax.numpy as jnp
from jax import lax
from jax.experimental import pallas as pl
from jax.experimental.pallas import tpu as pltpu
from jax.sharding import PartitionSpec as P


TILE = 128
EPS = 1e-06

HBM = pl.BlockSpec(memory_space=pl.ANY)
VMEM = pl.BlockSpec(memory_space=pltpu.VMEM)
RAW = pl.BlockSpec(memory_space=pltpu.HBM)


def cost(flops, nbytes):
    return pl.CostEstimate(flops=int(flops), bytes_accessed=int(nbytes), transcendentals=0)


def partner(c, k, n):
    return c ^ abs(k) if n & (n - 1) == 0 else (c + k + n) % n


def in_hbm(x):
    return pltpu.with_memory_space_constraint(x, pltpu.HBM)


def in_vmem(x):
    return pltpu.with_memory_space_constraint(x, pltpu.VMEM)


def grant(mib):
    return pltpu.CompilerParams(vmem_limit_bytes=int(mib) << 20)


LANES = 128
SUBLANES = 8
UNROLL = 32


def storage_order(send_rows):
    n, slots = send_rows.shape
    if n % SUBLANES or slots % LANES:
        return send_rows.reshape(-1), lambda q: q * slots, lambda b: b * UNROLL
    blocks = slots // LANES
    tiled = send_rows.reshape(n // SUBLANES, SUBLANES, blocks, LANES)
    tile = SUBLANES * LANES
    per = LANES // UNROLL

    def first(q):
        return (q >> 3) * (blocks * tile) + (q & (SUBLANES - 1)) * LANES

    def within(b):
        return (b >> (per.bit_length() - 1)) * tile + (b & (per - 1)) * UNROLL

    return tiled.transpose(0, 2, 1, 3).reshape(-1), first, within


def widen(feat, half, table, raw, sems):
    n_rows = raw.shape[0]
    parts = sems.shape[0]
    part = n_rows // parts
    step = 128 if part % 128 == 0 else 16
    lanes = pl.ds(half * LANES, LANES)
    copies = [
        pltpu.make_async_copy(
            feat.at[pl.ds(c * part, part), lanes], raw.at[pl.ds(c * part, part)], sems.at[c]
        )
        for c in range(parts)
    ]
    for copy in copies:
        copy.start()
    for c in range(parts):
        copies[c].wait()

        def one(b, carry, c=c):
            at = pl.ds(pl.multiple_of(c * part + b * step, step), step)
            table[at, :] = raw[at, :].astype(jnp.float32)
            return carry

        lax.fori_loop(0, part // step, one, 0)


def gather_kernel(peers, peer, first_row, within, half, build, ahead, rows_in, counts_in, *refs):
    n_out = len(peers)
    refs = list(refs)
    source = refs.pop(0)
    vals = [refs.pop(0) for _ in range(2 * bool(ahead))]
    outs, refs = refs[:n_out], refs[n_out:]
    if build:
        feat, table, raw = source, refs.pop(0), refs.pop(0)
    else:
        table = source
    blocks = [refs.pop(0) for _ in ahead]
    rows, counts, index_sems, stage = refs[:4]
    loads = []
    for spec, block, sem in zip(ahead, blocks, refs[len(refs) - len(ahead) :]):
        loads += block_copies(vals, block, sem, *spec)
    for load in loads:
        load.start()
    load_rows = pltpu.make_async_copy(rows_in, rows, index_sems.at[0])
    load_counts = pltpu.make_async_copy(counts_in, counts, index_sems.at[1])
    load_rows.start()
    load_counts.start()
    if build:
        widen(feat, half, table, raw, refs[4])
    load_rows.wait()
    load_counts.wait()
    me = lax.axis_index("dom")
    slots = outs[0].shape[0]
    for out, k in zip(outs, peers):
        q = peer(me, k)
        used = counts[q]
        begin = first_row(q)

        def pick(b, carry, begin=begin):
            base = begin + within(b)
            put = pl.multiple_of(b * UNROLL, UNROLL)
            source = [rows[base + j] for j in range(UNROLL)]
            got = [table[pl.ds(r, 1), :] for r in source]
            for j in range(UNROLL):
                stage[pl.ds(put + j, 1), :] = got[j]
            return carry

        lax.fori_loop(0, (used + UNROLL - 1) // UNROLL, pick, 0)
        for b in range(slots // 64):
            at = pl.ds(b * 64, 64)
            slot = b * 64 + lax.broadcasted_iota(jnp.int32, (64, LANES), 0)
            out[at, :] = jnp.where(slot < used, stage[at, :], 0.0).astype(out.dtype)
    for load in loads:
        load.wait()


def gather_rows(
    rows, first_row, within, send_count, features, half, table, peers, peer, slots, vals, ahead
):
    n_rows = features.shape[0]
    build = table is None
    piece = jax.ShapeDtypeStruct((slots, LANES), features.dtype)
    parts = 8 if n_rows % (8 * 16) == 0 else 1
    made = [
        jax.ShapeDtypeStruct((n_rows, LANES), jnp.float32),
        jax.ShapeDtypeStruct((n_rows, LANES), features.dtype),
    ]
    block = [block_shape(vals[0], *spec) for spec in ahead]
    out = pl.pallas_call(
        functools.partial(gather_kernel, peers, peer, first_row, within, half, build, ahead),
        out_shape=[piece] * len(peers) + made * build + block,
        in_specs=[RAW, RAW, RAW if build else VMEM] + [RAW] * (2 * bool(ahead)),
        out_specs=[VMEM] * (len(peers) + 2 * build + len(block)),
        scratch_shapes=[
            pltpu.SMEM(rows.shape, jnp.int32),
            pltpu.SMEM(send_count.shape, jnp.int32),
            pltpu.SemaphoreType.DMA((2,)),
            pltpu.VMEM((slots, LANES), jnp.float32),
        ]
        + [pltpu.SemaphoreType.DMA((parts,))] * build
        + [pltpu.SemaphoreType.DMA((2 * spec[0],)) for spec in ahead],
        compiler_params=grant(10 + len(peers) if build else 8),
        cost_estimate=cost(4e9, 6 << 20),
        name="gather_rows",
    )(
        in_hbm(rows), in_hbm(send_count), in_hbm(features) if build else table,
        *([in_hbm(v) for v in vals] * bool(ahead)),
    )
    n_out = len(peers)
    return out[:n_out], out[n_out : n_out + 2 * build], out[n_out + 2 * build :]


def masked(vals, used):
    return [
        jnp.where(s < used, vals[s], jnp.zeros_like(vals[s])) for s in range(vals.shape[0])
    ]


def tiles_of(src, index, row_tile, slots):
    starts = [pl.multiple_of(index[s, row_tile] * TILE, TILE) for s in range(slots)]
    return [src[pl.ds(at, TILE), :] for at in starts]


def product(left, right):
    return jnp.dot(
        jnp.concatenate(left, axis=1),
        jnp.concatenate(right, axis=0),
        preferred_element_type=jnp.float32,
    )


def row_tile_of(k, n_col, per_dest, tile):
    return partner(lax.axis_index("col"), k, n_col) * per_dest + tile


def block_shape(vals, n_col, per_dest, base, size):
    return jax.ShapeDtypeStruct((n_col, 2, size) + vals.shape[1:], vals.dtype)


def block_copies(vals, block, sems, n_col, per_dest, base, size):
    copies = []
    for k in range(n_col):
        at = pl.ds(row_tile_of(k, n_col, per_dest, base), size)
        for v in range(2):
            copies.append(
                pltpu.make_async_copy(vals[v].at[at], block.at[k, v], sems.at[2 * k + v])
            )
    return copies


def put_piece(halo, piece, q):
    rows = piece.shape[0]
    halo[pl.ds(pl.multiple_of(q * rows, rows), rows), :] = piece[...]


def assemble_kernel(ks, peer, *refs):
    pieces, halo = refs[:-1], refs[-1]
    me = lax.axis_index("dom")
    for k, piece in zip(ks, pieces):
        put_piece(halo, piece, peer(me, -k))
    rows = pieces[0].shape[0]
    own = pl.ds(pl.multiple_of(me * rows, rows), rows)
    halo[own, :] = jnp.zeros((rows, halo.shape[1]), halo.dtype)


def assemble(ks, pieces, n_dom, peer):
    rows, width = pieces[0].shape
    return pl.pallas_call(
        functools.partial(assemble_kernel, ks, peer),
        out_shape=jax.ShapeDtypeStruct((n_dom * rows, width), pieces[0].dtype),
        in_specs=[VMEM] * len(pieces),
        out_specs=VMEM,
        compiler_params=grant(4 + n_dom),
        cost_estimate=cost(2e9, 4 << 20),
        name="assemble",
    )(*pieces)


def sum_kernel(n_col, slots, per_dest, base, ahead, *refs):
    own_index, own_counts, halo_index, halo_counts, feat, halo, block = refs[:7]
    refs = refs[7:]
    loads = []
    if ahead:
        loads = block_copies(refs[:2], refs[2 + n_col], refs[-1], *ahead)
        refs = refs[2:]
    outs = refs[:n_col]
    for load in loads:
        load.start()

    def one(t, carry):
        for k in range(n_col):
            row_tile = row_tile_of(k, n_col, per_dest, base + t)
            left = masked(block.at[k, 0, t], own_counts[row_tile])
            left += masked(block.at[k, 1, t], halo_counts[row_tile])
            right = tiles_of(feat, own_index, row_tile, slots)
            right += tiles_of(halo, halo_index, row_tile, slots)
            at = pl.ds(pl.multiple_of(t * TILE, TILE), TILE)
            outs[k][at, :] = product(left, right).astype(outs[k].dtype)
        return carry

    lax.fori_loop(0, block.shape[2], one, 0)
    for load in loads:
        load.wait()


def tile_sums(tables, halo, features, block, vals, per_dest, base, ahead):
    n_col, _, size, slots = block.shape[:4]
    width = features.shape[1]
    made = [block_shape(vals[0], *ahead)] if ahead else []
    smem = pl.BlockSpec(memory_space=pltpu.SMEM)
    out = pl.pallas_call(
        functools.partial(sum_kernel, n_col, slots, per_dest, base, ahead),
        out_shape=[jax.ShapeDtypeStruct((size * TILE, width), jnp.bfloat16)] * n_col + made,
        grid_spec=pltpu.PrefetchScalarGridSpec(
            num_scalar_prefetch=4,
            grid=(1,),
            in_specs=[VMEM] * 3 + [RAW] * (2 * len(made)),
            out_specs=[VMEM] * (n_col + len(made)),
            scratch_shapes=[pltpu.SemaphoreType.DMA((2 * n_col,))] * len(made),
        ),
        compiler_params=grant(8),
        cost_estimate=cost(2e9, 6 << 20),
        name="tile_sums",
    )(
        *tables, in_vmem(features), in_vmem(halo), in_vmem(block),
        *([in_hbm(v) for v in vals] * len(made)),
    )
    return out[:n_col], out[n_col:]


PAD = 16


def part_kernel(share, weight, bias, out, sem):
    part = weight.shape[0] // share
    start = lax.rem(lax.axis_index("dom"), share) * part
    src = weight.at[pl.ds(pl.multiple_of(start, part), part)]
    copy = pltpu.make_async_copy(src, out.at[pl.ds(0, part)], sem)
    copy.start()
    out[pl.ds(part, PAD), :] = jnp.broadcast_to(bias[...], (PAD, out.shape[1]))
    copy.wait()


def weight_part(weight, bias, share):
    rows = weight.shape[0] // share + PAD
    return pl.pallas_call(
        functools.partial(part_kernel, share),
        out_shape=jax.ShapeDtypeStruct((rows, weight.shape[1]), weight.dtype),
        in_specs=[RAW, VMEM],
        out_specs=VMEM,
        scratch_shapes=[pltpu.SemaphoreType.DMA],
        compiler_params=grant(4),
        cost_estimate=cost(1e8, 1 << 20),
        name="weight_part",
    )(in_hbm(weight), bias)


def pack_kernel(*refs):
    rows = refs[0].shape[0]
    for k, ref in enumerate(refs[:-1]):
        refs[-1][pl.ds(k * rows, rows), :] = ref[...]


def pack_rows(arrays):
    rows, width = arrays[0].shape
    return pl.pallas_call(
        pack_kernel,
        out_shape=jax.ShapeDtypeStruct((rows * len(arrays), width), arrays[0].dtype),
        in_specs=[VMEM] * len(arrays),
        out_specs=VMEM,
        compiler_params=grant(4),
        cost_estimate=cost(1e8, 1 << 20),
        name="pack_rows",
    )(*arrays)


def join_kernel(n_col, share, own, own_bias, *refs):
    parts = refs[:share]
    joined, bias = refs[share:]
    width = own.shape[1]
    part = own.shape[0] // share
    me = lax.rem(lax.axis_index("dom"), share)
    block = min(width, part)
    for s in range(n_col):
        for b in range(width // block):
            row = partner(lax.axis_index("col"), -s, n_col) * width + b * block
            row = pl.multiple_of(row, block)
            at = pl.ds(s * width + b * block, block)
            joined[0, at, :] = own[pl.ds(row, block), :]
            side = lax.div(row, part)
            offset = row - side * part
            for flip in range(share):

                @pl.when(side == me ^ flip)
                def _(flip=flip, at=at, offset=offset):
                    for k in range(1, n_col):
                        start = pl.multiple_of((k - 1) * (part + PAD) + offset, PAD)
                        joined[k, at, :] = parts[flip][pl.ds(start, block), :]

    bias[pl.ds(0, 1), :] = own_bias[...].astype(jnp.float32)
    for k in range(1, n_col):
        got = parts[0][pl.ds(k * part + (k - 1) * PAD, PAD), :].astype(jnp.float32)
        bias[pl.ds(k, 1), :] = got[:1]


def join_weights(weight, bias, parts, n_col):
    channels, width = weight.shape
    share = len(parts)
    return pl.pallas_call(
        functools.partial(join_kernel, n_col, share),
        out_shape=[
            jax.ShapeDtypeStruct((n_col, channels, width), weight.dtype),
            jax.ShapeDtypeStruct((n_col, width), jnp.float32),
        ],
        in_specs=[VMEM] * (2 + share),
        out_specs=[VMEM] * 2,
        compiler_params=grant(8),
        cost_estimate=cost(1e9, 4 << 20),
        name="join_weights",
    )(weight, bias, *parts)


def mix_kernel(n_col, n_in, channels, first, *refs):
    pieces, held, bias = refs[:n_in], refs[n_in], refs[n_in + 1]
    outs, stats = refs[-n_col - 1 : -1], refs[-1]

    @pl.when(pl.program_id(0) == 0)
    def _():
        stats[...] = jnp.zeros_like(stats) if first else refs[n_in + 2][...]

    spread = jnp.concatenate([piece[...] for piece in pieces], axis=1)
    active, power = [], 0.0
    for k in range(n_col):
        mixed = jnp.dot(spread, held[k], preferred_element_type=jnp.float32)
        mixed = jnp.maximum(mixed + bias[pl.ds(k, 1), :], 0.0)
        power = power + jnp.sum(mixed * mixed, axis=1, keepdims=True)
        active.append(mixed)
    scale = lax.rsqrt(power * (1.0 / channels) + EPS)
    for k in range(n_col):
        scaled = active[k] * scale
        outs[k][...] = scaled.astype(outs[k].dtype)
        stats[pl.ds(2 * k, 1), :] += jnp.sum(scaled, axis=0, keepdims=True)
        stats[pl.ds(2 * k + 1, 1), :] += jnp.sum(scaled * scaled, axis=0, keepdims=True)


def mix_rows(pieces, weights, bias, before):
    n_col, channels, width = weights.shape
    rows = pieces[0].shape[0]
    block = TILE
    spec = lambda w: pl.BlockSpec((block, w), lambda i: (i, 0))
    first = before is None
    out = pl.pallas_call(
        functools.partial(mix_kernel, n_col, len(pieces), channels, first),
        out_shape=[jax.ShapeDtypeStruct((rows, width), jnp.bfloat16)] * n_col
        + [jax.ShapeDtypeStruct((2 * n_col, width), jnp.float32)],
        grid=(rows // block,),
        in_specs=[spec(piece.shape[1]) for piece in pieces] + [VMEM] * (2 if first else 3),
        out_specs=[spec(width)] * n_col + [VMEM],
        compiler_params=grant(10),
        cost_estimate=cost(2 * rows * channels * channels, 4 << 20),
        name="mix_rows",
    )(*pieces, weights, bias, *([] if first else [before]))
    return out[:n_col], out[n_col]


def place_kernel(n_col, per_dest, base, nodes, *refs):
    pieces = refs[:n_col]
    parts = refs[n_col : 2 * n_col] if nodes else ()
    out, put = refs[-2 - bool(nodes)], refs[-1]
    rows = pieces[0].shape[0]
    stores = []
    for k in range(n_col):
        dest = partner(lax.axis_index("col"), k, n_col)
        at = pl.ds(pl.multiple_of((dest * per_dest + base) * TILE, TILE), rows)
        stores.append(pltpu.make_async_copy(pieces[k], out.at[at], put.at[k]))
    for store in stores:
        store.start()
    if nodes:
        total = parts[0][...]
        for part in parts[1:]:
            total = total + part[...]
        total = total / nodes
        mean = total[0:1]
        refs[-2][pl.ds(0, 1), :] = mean
        refs[-2][pl.ds(1, 1), :] = total[1:2] - mean * mean
    for store in stores:
        store.wait()


def place_rows(pieces, out, n_rows, base, parts=(), nodes=0):
    n_col = len(pieces)
    _, width = pieces[0].shape
    per_dest = n_rows // TILE // n_col
    extra = list(parts) + ([] if out is None else [out])
    out_shape = [jax.ShapeDtypeStruct((n_rows, width), jnp.bfloat16)]
    out_specs = [HBM]
    if nodes:
        out_shape.append(jax.ShapeDtypeStruct((2, width), jnp.float32))
        out_specs.append(VMEM)
    return pl.pallas_call(
        functools.partial(place_kernel, n_col, per_dest, base, nodes),
        out_shape=out_shape,
        in_specs=[VMEM] * (n_col + len(parts)) + ([] if out is None else [HBM]),
        out_specs=out_specs,
        scratch_shapes=[pltpu.SemaphoreType.DMA((n_col,))],
        input_output_aliases={} if out is None else {n_col + len(extra) - 1: 0},
        compiler_params=grant(8),
        cost_estimate=cost(1e8, 2 << 20),
        name="place_rows",
    )(*pieces, *extra)


def chunk_plan(per_dest):
    if per_dest < 16:
        return [(0, per_dest)]
    cuts = [per_dest * c // 16 for c in (0, 3, 7, 13, 16)]
    return [(a, b - a) for a, b in zip(cuts, cuts[1:])]


def sharers(n_dom, channels):
    share = 1
    while share < 8 and n_dom % (2 * share) == 0 and channels % (2 * share * PAD) == 0:
        share *= 2
    return share


def swap_stages(share):
    return [1 << b for b in reversed(range(share.bit_length() - 1))]


def on_device(
    features,
    weight,
    out_bias,
    local_index,
    local_count,
    local_vals,
    halo_index,
    halo_count,
    halo_vals,
    send_rows,
    send_count,
):
    n_rows, width = features.shape
    n_dom, n_col = lax.axis_size("dom"), lax.axis_size("col")

    peer = lambda d, k: partner(d, k, n_dom)
    along_dom = lambda x, k: lax.ppermute(x, "dom", [(i, peer(i, k)) for i in range(n_dom)])
    along_col = lambda x, k: lax.ppermute(
        x, "col", [(i, partner(i, k, n_col)) for i in range(n_col)]
    )
    order = list(reversed(range(1, n_col)))

    far = list(reversed(range(1, n_dom)))
    lead, rest = far[:2], far[2:]
    rest = rest[0::2] + rest[1::2]
    rows, first_row, within = storage_order(send_rows[0])
    slots = send_rows.shape[2]
    halves = width // LANES
    vals = (local_vals[0], halo_vals[0])
    per_dest = n_rows // TILE // n_col
    plan = chunk_plan(per_dest)
    ahead = [(n_col, per_dest, base, size) for base, size in plan]
    halo, own_tiles = [], []
    for h in range(halves):
        pieces, table = {}, None
        groups = [g for g in (lead, rest) if g] if h == 0 else [lead + rest]
        for peers in groups:
            load = ahead[:2] if h == 0 and peers is groups[-1] else []
            outgoing, made, block = gather_rows(
                rows, first_row, within, send_count[0], features, h, table, peers, peer,
                slots, vals, load,
            )
            if load:
                blocks = list(block)
            if made:
                table, tiles = made
            for k, piece in zip(peers, outgoing):
                pieces[k] = along_dom(piece, k)
        halo.append(pieces)
        own_tiles.append(tiles)

    share = sharers(n_dom, n_col * width)
    bias_row = out_bias.reshape(1, width)
    mine = weight_part(weight, bias_row, share)
    arrived = {k: along_col(mine, k) for k in order}
    parts = [pack_rows([arrived[k] for k in range(1, n_col)])]
    got = {0: parts[0]}
    for step in swap_stages(share):
        swap = [(i, i ^ step) for i in range(n_dom)]
        for flip in list(got):
            got[flip ^ step] = lax.ppermute(got[flip], "dom", swap)
    weights, bias = join_weights(weight, bias_row, [got[f] for f in range(share)], n_col)

    index_tables = (local_index[0].T, local_count[0], halo_index[0].T, halo_count[0])
    incoming = [[[] for _ in range(n_col)] for _ in plan]
    for h in range(halves):
        received = assemble(far, [halo[h][k] for k in far], n_dom, peer)
        for g, (base, size) in enumerate(plan):
            load = ahead[g + 1] if h == 0 < g < len(plan) - 1 else ()
            sums, block = tile_sums(
                index_tables, received, own_tiles[h], blocks[g], vals, per_dest, base, load
            )
            blocks += block
            moved = {k: along_col(sums[k], k) for k in order}
            for k in range(n_col):
                incoming[g][k].append(moved[k] if k else sums[0])

    stats = None
    returned = []
    for pieces in incoming:
        done, stats = mix_rows(sum(pieces, []), weights, bias, stats)
        moved = {k: along_col(done[k], -k) for k in order}
        returned.append([done[0]] + [moved[k] for k in range(1, n_col)])

    over_dom = lax.all_gather(stats, "dom", axis=0)
    over_dom = over_dom.sum(axis=0)
    totals = [over_dom[:2]]
    for k in range(1, n_col):
        totals.append(along_col(over_dom[2 * k : 2 * k + 2], -k))

    out = None
    for g, ((base, _), pieces) in enumerate(zip(plan, returned)):
        if g < len(plan) - 1:
            (out,) = place_rows(pieces, out, n_rows, base)
        else:
            out, channel_stats = place_rows(
                pieces, out, n_rows, base, totals, n_rows * n_dom
            )
    return (out, channel_stats)


def solution(mesh):
    in_specs = (
        P("dom", "col"),
        P(None, "col"),
        P("col"),
        P("dom", None, None),
        P("dom", None),
        P("dom", None, None, None, None),
        P("dom", None, None),
        P("dom", None),
        P("dom", None, None, None, None),
        P("dom", None, None),
        P("dom", None),
    )
    out_specs = (P("dom", "col"), P(None, "col"))
    return jax.shard_map(
        on_device, mesh=mesh, in_specs=in_specs, out_specs=out_specs, check_vma=False
    )
```

```python
import functools

import jax
import jax.numpy as jnp
from jax import lax
from jax.experimental import pallas as pl
from jax.experimental.pallas import tpu as pltpu
from jax.sharding import PartitionSpec as P


TILE = 128
EPS = 1e-06

HBM = pl.BlockSpec(memory_space=pl.ANY)
VMEM = pl.BlockSpec(memory_space=pltpu.VMEM)
RAW = pl.BlockSpec(memory_space=pltpu.HBM)


def cost(flops, nbytes):
    return pl.CostEstimate(flops=int(flops), bytes_accessed=int(nbytes), transcendentals=0)


def partner(c, k, n):
    return c ^ abs(k) if n & (n - 1) == 0 else (c + k + n) % n


def in_hbm(x):
    return pltpu.with_memory_space_constraint(x, pltpu.HBM)


def in_vmem(x):
    return pltpu.with_memory_space_constraint(x, pltpu.VMEM)


def grant(mib):
    return pltpu.CompilerParams(vmem_limit_bytes=int(mib) << 20)


LANES = 128
SUBLANES = 8
UNROLL = 32


def storage_order(send_rows):
    n, slots = send_rows.shape
    if n % SUBLANES or slots % LANES:
        return send_rows.reshape(-1), lambda q: q * slots, lambda b: b * UNROLL
    blocks = slots // LANES
    tiled = send_rows.reshape(n // SUBLANES, SUBLANES, blocks, LANES)
    tile = SUBLANES * LANES
    per = LANES // UNROLL

    def first(q):
        return (q >> 3) * (blocks * tile) + (q & (SUBLANES - 1)) * LANES

    def within(b):
        return (b >> (per.bit_length() - 1)) * tile + (b & (per - 1)) * UNROLL

    return tiled.transpose(0, 2, 1, 3).reshape(-1), first, within


def widen(feat, half, table, raw, sems):
    n_rows = raw.shape[0]
    parts = sems.shape[0]
    part = n_rows // parts
    step = 128 if part % 128 == 0 else 16
    lanes = pl.ds(half * LANES, LANES)
    copies = [
        pltpu.make_async_copy(
            feat.at[pl.ds(c * part, part), lanes], raw.at[pl.ds(c * part, part)], sems.at[c]
        )
        for c in range(parts)
    ]
    for copy in copies:
        copy.start()
    for c in range(parts):
        copies[c].wait()

        def one(b, carry, c=c):
            at = pl.ds(pl.multiple_of(c * part + b * step, step), step)
            table[at, :] = raw[at, :].astype(jnp.float32)
            return carry

        lax.fori_loop(0, part // step, one, 0)


def gather_kernel(peers, peer, first_row, within, half, build, ahead, rows_in, counts_in, *refs):
    n_out = len(peers)
    refs = list(refs)
    source = refs.pop(0)
    vals = [refs.pop(0) for _ in range(2 * bool(ahead))]
    outs, refs = refs[:n_out], refs[n_out:]
    if build:
        feat, table, raw = source, refs.pop(0), refs.pop(0)
    else:
        table = source
    blocks = [refs.pop(0) for _ in ahead]
    rows, counts, index_sems, stage = refs[:4]
    loads = []
    for spec, block, sem in zip(ahead, blocks, refs[len(refs) - len(ahead) :]):
        loads += block_copies(vals, block, sem, *spec)
    for load in loads:
        load.start()
    load_rows = pltpu.make_async_copy(rows_in, rows, index_sems.at[0])
    load_counts = pltpu.make_async_copy(counts_in, counts, index_sems.at[1])
    load_rows.start()
    load_counts.start()
    if build:
        widen(feat, half, table, raw, refs[4])
    load_rows.wait()
    load_counts.wait()
    me = lax.axis_index("dom")
    slots = outs[0].shape[0]
    for out, k in zip(outs, peers):
        q = peer(me, k)
        used = counts[q]
        begin = first_row(q)

        def pick(b, carry, begin=begin):
            base = begin + within(b)
            put = pl.multiple_of(b * UNROLL, UNROLL)
            source = [rows[base + j] for j in range(UNROLL)]
            got = [table[pl.ds(r, 1), :] for r in source]
            for j in range(UNROLL):
                stage[pl.ds(put + j, 1), :] = got[j]
            return carry

        lax.fori_loop(0, (used + UNROLL - 1) // UNROLL, pick, 0)
        for b in range(slots // 64):
            at = pl.ds(b * 64, 64)
            slot = b * 64 + lax.broadcasted_iota(jnp.int32, (64, LANES), 0)
            out[at, :] = jnp.where(slot < used, stage[at, :], 0.0).astype(out.dtype)
    for load in loads:
        load.wait()


def gather_rows(
    rows, first_row, within, send_count, features, half, table, peers, peer, slots, vals, ahead
):
    n_rows = features.shape[0]
    build = table is None
    piece = jax.ShapeDtypeStruct((slots, LANES), features.dtype)
    parts = 8 if n_rows % (8 * 16) == 0 else 1
    made = [
        jax.ShapeDtypeStruct((n_rows, LANES), jnp.float32),
        jax.ShapeDtypeStruct((n_rows, LANES), features.dtype),
    ]
    block = [block_shape(vals[0], *spec) for spec in ahead]
    out = pl.pallas_call(
        functools.partial(gather_kernel, peers, peer, first_row, within, half, build, ahead),
        out_shape=[piece] * len(peers) + made * build + block,
        in_specs=[RAW, RAW, RAW if build else VMEM] + [RAW] * (2 * bool(ahead)),
        out_specs=[VMEM] * (len(peers) + 2 * build + len(block)),
        scratch_shapes=[
            pltpu.SMEM(rows.shape, jnp.int32),
            pltpu.SMEM(send_count.shape, jnp.int32),
            pltpu.SemaphoreType.DMA((2,)),
            pltpu.VMEM((slots, LANES), jnp.float32),
        ]
        + [pltpu.SemaphoreType.DMA((parts,))] * build
        + [pltpu.SemaphoreType.DMA((2 * spec[0],)) for spec in ahead],
        compiler_params=grant(10 + len(peers) if build else 8),
        cost_estimate=cost(4e9, 6 << 20),
        name="gather_rows",
    )(
        in_hbm(rows), in_hbm(send_count), in_hbm(features) if build else table,
        *([in_hbm(v) for v in vals] * bool(ahead)),
    )
    n_out = len(peers)
    return out[:n_out], out[n_out : n_out + 2 * build], out[n_out + 2 * build :]


def masked(vals, used):
    return [
        jnp.where(s < used, vals[s], jnp.zeros_like(vals[s])) for s in range(vals.shape[0])
    ]


def tiles_of(src, index, row_tile, slots):
    starts = [pl.multiple_of(index[s, row_tile] * TILE, TILE) for s in range(slots)]
    return [src[pl.ds(at, TILE), :] for at in starts]


def product(left, right):
    return jnp.dot(
        jnp.concatenate(left, axis=1),
        jnp.concatenate(right, axis=0),
        preferred_element_type=jnp.float32,
    )


def row_tile_of(k, n_col, per_dest, tile):
    return partner(lax.axis_index("col"), k, n_col) * per_dest + tile


def block_shape(vals, n_col, per_dest, base, size):
    return jax.ShapeDtypeStruct((n_col, 2, size) + vals.shape[1:], vals.dtype)


def block_copies(vals, block, sems, n_col, per_dest, base, size):
    copies = []
    for k in range(n_col):
        at = pl.ds(row_tile_of(k, n_col, per_dest, base), size)
        for v in range(2):
            copies.append(
                pltpu.make_async_copy(vals[v].at[at], block.at[k, v], sems.at[2 * k + v])
            )
    return copies


def put_piece(halo, piece, q):
    rows = piece.shape[0]
    halo[pl.ds(pl.multiple_of(q * rows, rows), rows), :] = piece[...]


def assemble_kernel(ks, peer, *refs):
    pieces, halo = refs[:-1], refs[-1]
    me = lax.axis_index("dom")
    for k, piece in zip(ks, pieces):
        put_piece(halo, piece, peer(me, -k))
    rows = pieces[0].shape[0]
    own = pl.ds(pl.multiple_of(me * rows, rows), rows)
    halo[own, :] = jnp.zeros((rows, halo.shape[1]), halo.dtype)


def assemble(ks, pieces, n_dom, peer):
    rows, width = pieces[0].shape
    return pl.pallas_call(
        functools.partial(assemble_kernel, ks, peer),
        out_shape=jax.ShapeDtypeStruct((n_dom * rows, width), pieces[0].dtype),
        in_specs=[VMEM] * len(pieces),
        out_specs=VMEM,
        compiler_params=grant(4 + n_dom),
        cost_estimate=cost(2e9, 4 << 20),
        name="assemble",
    )(*pieces)


def sum_kernel(ks, n_col, slots, per_dest, base, ahead, *refs):
    own_index, own_counts, halo_index, halo_counts, feat, halo, block = refs[:7]
    refs = refs[7:]
    loads = []
    if ahead:
        loads = block_copies(refs[:2], refs[2 + len(ks)], refs[-1], *ahead)
        refs = refs[2:]
    outs = refs[: len(ks)]
    for load in loads:
        load.start()

    def one(t, carry):
        for out, k in zip(outs, ks):
            row_tile = row_tile_of(k, n_col, per_dest, base + t)
            left = masked(block.at[k, 0, t], own_counts[row_tile])
            left += masked(block.at[k, 1, t], halo_counts[row_tile])
            right = tiles_of(feat, own_index, row_tile, slots)
            right += tiles_of(halo, halo_index, row_tile, slots)
            at = pl.ds(pl.multiple_of(t * TILE, TILE), TILE)
            out[at, :] = product(left, right).astype(out.dtype)
        return carry

    lax.fori_loop(0, block.shape[2], one, 0)
    for load in loads:
        load.wait()


def tile_sums(tables, halo, features, block, vals, per_dest, base, ahead, ks):
    n_col, _, size, slots = block.shape[:4]
    width = features.shape[1]
    made = [block_shape(vals[0], *ahead)] if ahead else []
    smem = pl.BlockSpec(memory_space=pltpu.SMEM)
    out = pl.pallas_call(
        functools.partial(sum_kernel, ks, n_col, slots, per_dest, base, ahead),
        out_shape=[jax.ShapeDtypeStruct((size * TILE, width), jnp.bfloat16)] * len(ks) + made,
        grid_spec=pltpu.PrefetchScalarGridSpec(
            num_scalar_prefetch=4,
            grid=(1,),
            in_specs=[VMEM] * 3 + [RAW] * (2 * len(made)),
            out_specs=[VMEM] * (len(ks) + len(made)),
            scratch_shapes=[pltpu.SemaphoreType.DMA((2 * n_col,))] * len(made),
        ),
        compiler_params=grant(8),
        cost_estimate=cost(2e9, 6 << 20),
        name="tile_sums",
    )(
        *tables, in_vmem(features), in_vmem(halo), in_vmem(block),
        *([in_hbm(v) for v in vals] * len(made)),
    )
    return dict(zip(ks, out)), out[len(ks) :]


PAD = 16


def part_kernel(share, weight, bias, out, sem):
    part = weight.shape[0] // share
    start = lax.rem(lax.axis_index("dom"), share) * part
    src = weight.at[pl.ds(pl.multiple_of(start, part), part)]
    copy = pltpu.make_async_copy(src, out.at[pl.ds(0, part)], sem)
    copy.start()
    out[pl.ds(part, PAD), :] = jnp.broadcast_to(bias[...], (PAD, out.shape[1]))
    copy.wait()


def weight_part(weight, bias, share):
    rows = weight.shape[0] // share + PAD
    return pl.pallas_call(
        functools.partial(part_kernel, share),
        out_shape=jax.ShapeDtypeStruct((rows, weight.shape[1]), weight.dtype),
        in_specs=[RAW, VMEM],
        out_specs=VMEM,
        scratch_shapes=[pltpu.SemaphoreType.DMA],
        compiler_params=grant(4),
        cost_estimate=cost(1e8, 1 << 20),
        name="weight_part",
    )(in_hbm(weight), bias)


def pack_kernel(*refs):
    rows = refs[0].shape[0]
    for k, ref in enumerate(refs[:-1]):
        refs[-1][pl.ds(k * rows, rows), :] = ref[...]


def pack_rows(arrays):
    rows, width = arrays[0].shape
    return pl.pallas_call(
        pack_kernel,
        out_shape=jax.ShapeDtypeStruct((rows * len(arrays), width), arrays[0].dtype),
        in_specs=[VMEM] * len(arrays),
        out_specs=VMEM,
        compiler_params=grant(4),
        cost_estimate=cost(1e8, 1 << 20),
        name="pack_rows",
    )(*arrays)


def join_kernel(n_col, share, own, own_bias, *refs):
    parts = refs[:share]
    joined, bias = refs[share:]
    width = own.shape[1]
    part = own.shape[0] // share
    me = lax.rem(lax.axis_index("dom"), share)
    block = min(width, part)
    for s in range(n_col):
        for b in range(width // block):
            row = partner(lax.axis_index("col"), -s, n_col) * width + b * block
            row = pl.multiple_of(row, block)
            at = pl.ds(s * width + b * block, block)
            joined[0, at, :] = own[pl.ds(row, block), :]
            side = lax.div(row, part)
            offset = row - side * part
            for flip in range(share):

                @pl.when(side == me ^ flip)
                def _(flip=flip, at=at, offset=offset):
                    for k in range(1, n_col):
                        start = pl.multiple_of((k - 1) * (part + PAD) + offset, PAD)
                        joined[k, at, :] = parts[flip][pl.ds(start, block), :]

    bias[pl.ds(0, 1), :] = own_bias[...].astype(jnp.float32)
    for k in range(1, n_col):
        got = parts[0][pl.ds(k * part + (k - 1) * PAD, PAD), :].astype(jnp.float32)
        bias[pl.ds(k, 1), :] = got[:1]


def join_weights(weight, bias, parts, n_col):
    channels, width = weight.shape
    share = len(parts)
    return pl.pallas_call(
        functools.partial(join_kernel, n_col, share),
        out_shape=[
            jax.ShapeDtypeStruct((n_col, channels, width), weight.dtype),
            jax.ShapeDtypeStruct((n_col, width), jnp.float32),
        ],
        in_specs=[VMEM] * (2 + share),
        out_specs=[VMEM] * 2,
        compiler_params=grant(8),
        cost_estimate=cost(1e9, 4 << 20),
        name="join_weights",
    )(weight, bias, *parts)


def mix_kernel(n_col, n_in, channels, first, *refs):
    pieces, held, bias = refs[:n_in], refs[n_in], refs[n_in + 1]
    outs, stats = refs[-n_col - 1 : -1], refs[-1]

    @pl.when(pl.program_id(0) == 0)
    def _():
        stats[...] = jnp.zeros_like(stats) if first else refs[n_in + 2][...]

    spread = jnp.concatenate([piece[...] for piece in pieces], axis=1)
    active, power = [], 0.0
    for k in range(n_col):
        mixed = jnp.dot(spread, held[k], preferred_element_type=jnp.float32)
        mixed = jnp.maximum(mixed + bias[pl.ds(k, 1), :], 0.0)
        power = power + jnp.sum(mixed * mixed, axis=1, keepdims=True)
        active.append(mixed)
    scale = lax.rsqrt(power * (1.0 / channels) + EPS)
    for k in range(n_col):
        scaled = active[k] * scale
        outs[k][...] = scaled.astype(outs[k].dtype)
        stats[pl.ds(2 * k, 1), :] += jnp.sum(scaled, axis=0, keepdims=True)
        stats[pl.ds(2 * k + 1, 1), :] += jnp.sum(scaled * scaled, axis=0, keepdims=True)


def mix_rows(pieces, weights, bias, before):
    n_col, channels, width = weights.shape
    rows = pieces[0].shape[0]
    block = TILE
    spec = lambda w: pl.BlockSpec((block, w), lambda i: (i, 0))
    first = before is None
    out = pl.pallas_call(
        functools.partial(mix_kernel, n_col, len(pieces), channels, first),
        out_shape=[jax.ShapeDtypeStruct((rows, width), jnp.bfloat16)] * n_col
        + [jax.ShapeDtypeStruct((2 * n_col, width), jnp.float32)],
        grid=(rows // block,),
        in_specs=[spec(piece.shape[1]) for piece in pieces] + [VMEM] * (2 if first else 3),
        out_specs=[spec(width)] * n_col + [VMEM],
        compiler_params=grant(10),
        cost_estimate=cost(2 * rows * channels * channels, 4 << 20),
        name="mix_rows",
    )(*pieces, weights, bias, *([] if first else [before]))
    return out[:n_col], out[n_col]


def place_kernel(n_col, per_dest, base, nodes, *refs):
    pieces = refs[:n_col]
    parts = refs[n_col : 2 * n_col] if nodes else ()
    out, put = refs[-2 - bool(nodes)], refs[-1]
    rows = pieces[0].shape[0]
    stores = []
    for k in range(n_col):
        dest = partner(lax.axis_index("col"), k, n_col)
        at = pl.ds(pl.multiple_of((dest * per_dest + base) * TILE, TILE), rows)
        stores.append(pltpu.make_async_copy(pieces[k], out.at[at], put.at[k]))
    for store in stores:
        store.start()
    if nodes:
        total = parts[0][...]
        for part in parts[1:]:
            total = total + part[...]
        total = total / nodes
        mean = total[0:1]
        refs[-2][pl.ds(0, 1), :] = mean
        refs[-2][pl.ds(1, 1), :] = total[1:2] - mean * mean
    for store in stores:
        store.wait()


def place_rows(pieces, out, n_rows, base, parts=(), nodes=0):
    n_col = len(pieces)
    _, width = pieces[0].shape
    per_dest = n_rows // TILE // n_col
    extra = list(parts) + ([] if out is None else [out])
    out_shape = [jax.ShapeDtypeStruct((n_rows, width), jnp.bfloat16)]
    out_specs = [HBM]
    if nodes:
        out_shape.append(jax.ShapeDtypeStruct((2, width), jnp.float32))
        out_specs.append(VMEM)
    return pl.pallas_call(
        functools.partial(place_kernel, n_col, per_dest, base, nodes),
        out_shape=out_shape,
        in_specs=[VMEM] * (n_col + len(parts)) + ([] if out is None else [HBM]),
        out_specs=out_specs,
        scratch_shapes=[pltpu.SemaphoreType.DMA((n_col,))],
        input_output_aliases={} if out is None else {n_col + len(extra) - 1: 0},
        compiler_params=grant(8),
        cost_estimate=cost(1e8, 2 << 20),
        name="place_rows",
    )(*pieces, *extra)


def chunk_plan(per_dest):
    if per_dest < 16:
        return [(0, per_dest)]
    cuts = [per_dest * c // 16 for c in (0, 3, 7, 14, 16)]
    return [(a, b - a) for a, b in zip(cuts, cuts[1:])]


def sharers(n_dom, channels):
    share = 1
    while share < 8 and n_dom % (2 * share) == 0 and channels % (2 * share * PAD) == 0:
        share *= 2
    return share


def swap_stages(share):
    return [1 << b for b in reversed(range(share.bit_length() - 1))]


def on_device(
    features,
    weight,
    out_bias,
    local_index,
    local_count,
    local_vals,
    halo_index,
    halo_count,
    halo_vals,
    send_rows,
    send_count,
):
    n_rows, width = features.shape
    n_dom, n_col = lax.axis_size("dom"), lax.axis_size("col")

    peer = lambda d, k: partner(d, k, n_dom)
    along_dom = lambda x, k: lax.ppermute(x, "dom", [(i, peer(i, k)) for i in range(n_dom)])
    along_col = lambda x, k: lax.ppermute(
        x, "col", [(i, partner(i, k, n_col)) for i in range(n_col)]
    )
    order = list(reversed(range(1, n_col)))

    far = list(reversed(range(1, n_dom)))
    lead, rest = far[:2], far[2:]
    rest = rest[0::2] + rest[1::2]
    rows, first_row, within = storage_order(send_rows[0])
    slots = send_rows.shape[2]
    halves = width // LANES
    vals = (local_vals[0], halo_vals[0])
    per_dest = n_rows // TILE // n_col
    plan = chunk_plan(per_dest)
    ahead = [(n_col, per_dest, base, size) for base, size in plan]
    halo, own_tiles = [], []
    for h in range(halves):
        pieces, table = {}, None
        groups = [g for g in (lead, rest) if g] if h == 0 else [lead + rest]
        for peers in groups:
            load = ahead[:2] if h == 0 and peers is groups[-1] else []
            outgoing, made, block = gather_rows(
                rows, first_row, within, send_count[0], features, h, table, peers, peer,
                slots, vals, load,
            )
            if load:
                blocks = list(block)
            if made:
                table, tiles = made
            for k, piece in zip(peers, outgoing):
                pieces[k] = along_dom(piece, k)
        halo.append(pieces)
        own_tiles.append(tiles)

    share = sharers(n_dom, n_col * width)
    bias_row = out_bias.reshape(1, width)
    mine = weight_part(weight, bias_row, share)
    arrived = {k: along_col(mine, k) for k in order}
    parts = [pack_rows([arrived[k] for k in range(1, n_col)])]
    got = {0: parts[0]}
    for step in swap_stages(share):
        swap = [(i, i ^ step) for i in range(n_dom)]
        for flip in list(got):
            got[flip ^ step] = lax.ppermute(got[flip], "dom", swap)
    weights, bias = join_weights(weight, bias_row, [got[f] for f in range(share)], n_col)

    index_tables = (local_index[0].T, local_count[0], halo_index[0].T, halo_count[0])
    incoming = [[[] for _ in range(n_col)] for _ in plan]
    for h in range(halves):
        received = assemble(far, [halo[h][k] for k in far], n_dom, peer)
        for g, (base, size) in enumerate(plan):
            load = ahead[g + 1] if h == 0 < g < len(plan) - 1 else ()
            groups = [order + [0]]
            if g == h == 0 and n_col > 2:
                groups = [order[:1], order[1:] + [0]]
            sums, moved = {}, {}
            for ks in groups:
                made, block = tile_sums(
                    index_tables, received, own_tiles[h], blocks[g], vals, per_dest, base,
                    load, ks,
                )
                sums.update(made)
                blocks += block
                moved.update({k: along_col(made[k], k) for k in ks if k})
            for k in range(n_col):
                incoming[g][k].append(moved[k] if k else sums[0])

    stats = None
    returned = []
    for pieces in incoming:
        done, stats = mix_rows(sum(pieces, []), weights, bias, stats)
        moved = {k: along_col(done[k], -k) for k in order}
        returned.append([done[0]] + [moved[k] for k in range(1, n_col)])

    over_dom = lax.all_gather(stats, "dom", axis=0)
    over_dom = over_dom.sum(axis=0)
    totals = [over_dom[:2]]
    for k in range(1, n_col):
        totals.append(along_col(over_dom[2 * k : 2 * k + 2], -k))

    out = None
    for g, ((base, _), pieces) in enumerate(zip(plan, returned)):
        if g < len(plan) - 1:
            (out,) = place_rows(pieces, out, n_rows, base)
        else:
            out, channel_stats = place_rows(
                pieces, out, n_rows, base, totals, n_rows * n_dom
            )
    return (out, channel_stats)


def solution(mesh):
    in_specs = (
        P("dom", "col"),
        P(None, "col"),
        P("col"),
        P("dom", None, None),
        P("dom", None),
        P("dom", None, None, None, None),
        P("dom", None, None),
        P("dom", None),
        P("dom", None, None, None, None),
        P("dom", None, None),
        P("dom", None),
    )
    out_specs = (P("dom", "col"), P(None, "col"))
    return jax.shard_map(
        on_device, mesh=mesh, in_specs=in_specs, out_specs=out_specs, check_vma=False
    )
```
